128 devices in a mesh: grp: 2 (over x_lo), dp: 64 (over y, x_hi, z, core).
Axes of the slice: x: 4 (x_hi: 2, x_lo: 2; x = x_hi * 2 + x_lo), y: 4, z: 4, core: 2. Of those that a mesh axis runs over, the one named last changes fastest.
Arguments:
- teacher_in: bfloat16 [32768, 1664], P('dp'), may hold values from -6 to 6
- teacher_gain: float32 [1664], replicated, may hold values from 0.5 to 1.5
- teacher_up: bfloat16 [1664, 4096], P('dp', 'grp'), may hold values from -0.15625 to 0.15625
- teacher_down: bfloat16 [1664, 4096], P('dp', 'grp'), may hold values from -0.09375 to 0.09375
- student_in: bfloat16 [32768, 768], P('dp'), may hold values from -6 to 6
- student_gain: float32 [768], replicated, may hold values from 0.5 to 1.5
- student_up: bfloat16 [768, 1536], P(None, ('grp', 'dp')), may hold values from -0.21875 to 0.21875
- student_down: bfloat16 [1536, 768], P(('grp', 'dp')), may hold values from -0.15625 to 0.15625
- student_head: bfloat16 [768, 1664], P(None, ('grp', 'dp')), may hold values from -0.21875 to 0.21875
- student_proj: bfloat16 [768, 512], P(None, ('grp', 'dp')), may hold values from -1 to 1
- word_table: bfloat16 [49408, 512], P(('grp', 'dp')), may hold values from -6 to 6
- caption_ids: int32 [128, 77], replicated, may hold values from 0 to 49407
- positive: int32 [128], replicated, may hold values from 0 to 127, each once
Outputs:
- loss: float32 [], replicated
- grad_up: float32 [768, 1536], P(None, ('grp', 'dp'))
- grad_down: float32 [1536, 768], P(('grp', 'dp'))
- grad_head: float32 [768, 1664], P(None, ('grp', 'dp'))
- grad_proj: float32 [768, 512], P(None, ('grp', 'dp'))
The draws below stay inside these ranges and needn't reach their ends.
Inputs may be any that keep to these rules, and one draw needn't show every extreme that they name: Each caption is the positive of exactly one image.
All inputs are finite; a program needn't handle non-finite values.
Results may differ from the reference program's by a relative error of at most 0.0065.
Values may be sent and summed in bfloat16 or wider, within the bound.
A program may use at most 128 MiB of HBM per device.

```python
import math
import jax
import jax.numpy as jnp
import numpy as np
from jax import lax

DT = 1664
HT = 4096
DS = 768
HS = 1536
DE = 512
VOCAB = 49408
CAP_LEN = 77
PATCHES = 256
IMAGES = 128
CAPTIONS = 128
N_GRP = 2
N_DP = 64


def draw_student_in(key, part):
    noise_key = jax.random.fold_in(key, 1103)
    values = jax.random.normal(noise_key, (IMAGES * PATCHES, DS), jnp.float32)
    return jnp.clip(values, -6.0, 6.0).astype(jnp.bfloat16)


def draw_student_proj(key, part):
    noise_key = jax.random.fold_in(key, 2207)
    values = jax.random.normal(noise_key, (DS, DE), jnp.float32) / jnp.sqrt(jnp.float32(DS))
    return jnp.clip(values, -1.0, 1.0).astype(jnp.bfloat16)


def draw_word_table(key, part):
    noise_key = jax.random.fold_in(key, 3301)
    values = jax.random.normal(noise_key, (VOCAB, DE), jnp.float32)
    return jnp.clip(values, -6.0, 6.0).astype(jnp.bfloat16)


def place_ends(values, key, low, top_value):
    longest = values.shape.index(max(values.shape))
    spots = []
    for shift in (0, 1):
        where = [jax.random.randint(jax.random.fold_in(key, axis), (), 0, length) for axis, length in enumerate(values.shape)]
        where[longest] = (where[longest] + shift) % values.shape[longest]
        spots.append(tuple(where))
    return values.at[spots[0]].set(low).at[spots[1]].set(top_value)


def levels(rng, shape, cuts, low, high):
    level, own = 1.0, jax.random.fold_in(rng, 6)
    for axis_at, blocks in cuts:
        heights = jnp.exp(jax.random.uniform(jax.random.fold_in(own, axis_at), (blocks,), jnp.float32, low / len(cuts), high / len(cuts)))
        level = level * jnp.repeat(heights, shape[axis_at] // blocks).reshape([-1 if axis == axis_at else 1 for axis in range(len(shape))])
    return level


def rank_bounds(number_of, slope):
    portions = [(1 << 20) // math.isqrt(rank ** slope) + 1 for rank in range(1, number_of + 1)]
    scale = 1 + sum(portions) // (1 << 30)
    return np.cumsum(np.array([max(1, weight // scale) for weight in portions]))


def ranked(key, dims, number_of, skew):
    table = rank_bounds(number_of, skew)
    pick = jax.random.randint(jax.random.fold_in(key, 1), dims, 0, int(table[number_of - 1]))
    rank = jnp.searchsorted(jnp.asarray(table, jnp.int32), pick, side="right")
    return jax.random.permutation(jax.random.fold_in(key, 2), number_of)[rank].astype(jnp.int32)


def gaussian(key, shape, scale, limit, cuts=(), held_as=jnp.bfloat16):
    loudness = levels(key, shape, cuts, -0.22, 0.18) if cuts else 1.0
    values = jax.random.normal(key, shape, jnp.float32) * scale * loudness
    return jnp.minimum(jnp.maximum(values, -limit), limit).astype(held_as)


def setup_inputs(seed: int = 0) -> dict:
    key_list = jax.random.split(jax.random.key(seed), 14)
    return {
        "teacher_in": gaussian(key_list[0], (IMAGES * PATCHES, DT), 1.0, 6.0, ((0, 64),)),
        "teacher_gain": jnp.clip(1.0 + 0.1 * jax.random.normal(key_list[1], (DT,), jnp.float32), 0.5, 1.5),
        "teacher_up": gaussian(key_list[2], (DT, HT), DT ** -0.5, 0.15625, ((0, 64), (1, 2))),
        "teacher_down": gaussian(key_list[3], (DT, HT), HT ** -0.5, 0.09375, ((0, 64), (1, 2))),
        "student_in": draw_student_in(jax.random.fold_in(key_list[13], 71), 0),
        "student_gain": jnp.clip(1.0 + 0.1 * jax.random.normal(key_list[5], (DS,), jnp.float32), 0.5, 1.5),
        "student_up": gaussian(key_list[6], (DS, HS), DS ** -0.5, 0.21875, ((1, 128),)),
        "student_down": gaussian(key_list[7], (HS, DS), HS ** -0.5, 0.15625, ((0, 128),)),
        "student_head": gaussian(key_list[8], (DS, DT), DS ** -0.5, 0.21875, ((1, 128),)),
        "student_proj": draw_student_proj(jax.random.fold_in(key_list[13], 71), 0),
        "word_table": draw_word_table(jax.random.fold_in(key_list[13], 71), 0),
        "caption_ids": place_ends(ranked(key_list[11], (CAPTIONS, CAP_LEN), VOCAB, 2), jax.random.fold_in(key_list[11], 3), 0, VOCAB - 1).astype(jnp.int32),
        "positive": jax.random.permutation(key_list[12], IMAGES).astype(jnp.int32),
    }


def normalize_rows(values, gain):
    center = values - lax.optimization_barrier(jnp.mean(values, -1, keepdims=True))
    spread = lax.optimization_barrier(jnp.mean(center * center, -1, keepdims=True))
    return center * lax.rsqrt(spread + 1e-05) * gain

def gelu_tanh(values):
    return jax.nn.gelu(values, approximate=True)

def unit_rows(values):
    return values / jnp.sqrt(lax.optimization_barrier(jnp.sum(values * values, -1, keepdims=True)) + 1e-06)

def reference(teacher_in, teacher_gain, teacher_up, teacher_down, student_in, student_gain, student_up, student_down, student_head, student_proj, word_table, caption_ids, positive):
    half_units = HT // N_GRP
    contract = (((1,), (1,)), ((), ()))

    def teacher_block(rows):
        normed = normalize_rows(rows.astype(jnp.float32), teacher_gain).astype(jnp.bfloat16)
        hidden = jnp.dot(normed, teacher_up, preferred_element_type=jnp.float32)
        active = gelu_tanh(hidden).astype(jnp.bfloat16)
        branch = jnp.zeros((rows.shape[0], DT), jnp.float32)
        for group in range(N_GRP):
            part = lax.dot_general(active[:, group * half_units:(group + 1) * half_units], teacher_down[:, group * half_units:(group + 1) * half_units], contract, preferred_element_type=jnp.float32)
            rounded = lax.optimization_barrier(part.astype(jnp.bfloat16))
            branch = branch + rounded.astype(jnp.float32)
        return rows.astype(jnp.float32) + branch
    target = lax.map(teacher_block, teacher_in.reshape(N_DP, -1, DT)).reshape(-1, DT)
    student_rows = student_in.astype(jnp.float32)
    student_normed = normalize_rows(student_rows, student_gain).astype(jnp.bfloat16)
    gate_out = jnp.dot(student_normed, student_up, preferred_element_type=jnp.float32)
    student_act = gelu_tanh(gate_out).astype(jnp.bfloat16)
    student_out = student_rows + jnp.dot(student_act, student_down, preferred_element_type=jnp.float32)
    student_rounded = student_out.astype(jnp.bfloat16)
    diff = jnp.dot(student_rounded, student_head, preferred_element_type=jnp.float32) - target
    feature_total = jnp.sum(diff * diff) / DT
    pooled = (lax.optimization_barrier(jnp.sum(student_out.reshape(IMAGES, PATCHES, DS), 1)) / PATCHES).astype(jnp.bfloat16)
    projected = jnp.dot(pooled, student_proj, preferred_element_type=jnp.float32)
    proj_norm = jnp.sqrt(lax.optimization_barrier(jnp.sum(projected * projected, -1, keepdims=True)) + 1e-06)
    image_emb = projected / proj_norm
    caption_sum = lax.optimization_barrier(jnp.sum(word_table[caption_ids].astype(jnp.float32), 1)) / CAP_LEN
    caption_emb = unit_rows(caption_sum)
    scores = 100.0 * jnp.dot(image_emb, caption_emb.T, precision=lax.Precision.HIGHEST)
    match = (positive[:, None] == jnp.arange(CAPTIONS, dtype=jnp.int32)[None, :]).astype(jnp.float32)
    contrast_total = jnp.sum(jax.nn.logsumexp(scores, 1)) + jnp.sum(jax.nn.logsumexp(scores, 0)) - 2.0 * jnp.sum(match * scores)
    loss = (feature_total + contrast_total) / (IMAGES * PATCHES)
    grad_scores = jax.nn.softmax(scores, 1) + jax.nn.softmax(scores, 0) - 2.0 * match
    grad_image = 100.0 * jnp.dot(grad_scores, caption_emb, precision=lax.Precision.HIGHEST)
    grad_projected = ((grad_image - image_emb * lax.optimization_barrier(jnp.sum(image_emb * grad_image, -1, keepdims=True))) / proj_norm).astype(jnp.bfloat16)
    grad_proj = jnp.dot(pooled.T, grad_projected, preferred_element_type=jnp.float32)
    grad_pooled = jnp.dot(grad_projected, student_proj.T, preferred_element_type=jnp.float32)
    grad_pred = (2.0 * diff / DT).astype(jnp.bfloat16)
    grad_head = jnp.dot(student_rounded.T, grad_pred, preferred_element_type=jnp.float32)
    grad_out = jnp.dot(grad_pred, student_head.T, preferred_element_type=jnp.float32)
    grad_out = (grad_out.reshape(IMAGES, PATCHES, DS) + (grad_pooled / PATCHES)[:, None, :]).reshape(-1, DS).astype(jnp.bfloat16)
    grad_down = jnp.dot(student_act.T, grad_out, preferred_element_type=jnp.float32)
    grad_act = jnp.dot(grad_out, student_down.T, preferred_element_type=jnp.float32)
    grad_gate = jax.vjp(gelu_tanh, gate_out)[1](grad_act)[0].astype(jnp.bfloat16)
    grad_up = jnp.dot(student_normed.T, grad_gate, preferred_element_type=jnp.float32)
    return (loss, grad_up, grad_down, grad_head, grad_proj)
```

```python
import jax
import jax.numpy as jnp
from jax import lax
from jax.experimental import pallas as pl
from jax.experimental.pallas import tpu as pltpu
from jax.sharding import PartitionSpec as P

CAP_LEN = 77
PATCHES = 256
BLK = 16
MESH = pl.DeviceIdType.MESH
ANY = pl.BlockSpec(memory_space=pl.ANY)
VM = pl.BlockSpec(memory_space=pltpu.VMEM)


def coords():
    grp = lax.axis_index("grp")
    dp = lax.axis_index("dp")
    x_hi = (dp // 8) % 2
    return {
        "x": 2 * x_hi + grp,
        "y": dp // 16,
        "z": (dp // 2) % 4,
        "core": dp % 2,
    }


def device(at):
    return (at["x"] % 2, at["y"] * 16 + (at["x"] // 2) * 8 + at["z"] * 2 + at["core"])


def shifted(me, axis, step):
    if axis == "core":
        return {**me, "core": 1 - me["core"]}
    return {**me, axis: (me[axis] + step) % 4}


def enter(me, axes=("x", "y", "z"), steps=(1, 2, 3)):
    barrier = pltpu.get_barrier_semaphore()
    peers = [shifted(me, "core", 1)]
    for axis in axes:
        for step in steps:
            peers.append(shifted(me, axis, step))
    for peer in peers:
        pl.semaphore_signal(barrier, inc=1, device_id=device(peer), device_id_type=MESH)
    pl.semaphore_wait(barrier, len(peers))


class Copies:
    def __init__(self, send, recv):
        self.send, self.recv, self.count, self.open = send, recv, 0, []

    def start(self, src, dst, peer):
        copy = pltpu.make_async_remote_copy(
            src_ref=src,
            dst_ref=dst,
            send_sem=self.send.at[self.count],
            recv_sem=self.recv.at[self.count],
            device_id=device(peer),
            device_id_type=MESH,
        )
        self.count += 1
        copy.start()
        self.open.append(copy)
        return copy

    def finish(self):
        for copy in self.open:
            copy.wait_send()


def pick(ref, at, tail=()):
    x = at.get("x")
    whole = slice(None)
    index = (
        whole if x is None else x % 2,
        at.get("y", whole),
        whole if x is None else x // 2,
        at.get("z", whole),
    )
    if "core" in at:
        index += (at["core"],)
    return ref.at[index + tail]


def half(ref, side):
    size = ref.shape[0] // 2
    return ref.at[pl.ds(side * size, size)]


def weight_gather(ins, outs, send, recv, local_sem):
    me = coords()
    enter(me)
    copies = Copies(send, recv)
    sibling = shifted(me, "core", 1)
    locals_ = []
    for i in range(6):
        own = pick_out(outs[i], me, i < 2)
        copy = pltpu.make_async_copy(ins[i], own, local_sem.at[i])
        copy.start()
        locals_.append(copy)

    def push(pushes, view):
        pushes.append(copies.start(view, view, sibling))

    def chain(i, order):
        teacher = i < 2
        out = outs[i]
        pushes = []
        pushes.append(copies.start(ins[i], pick_out(out, me, teacher), sibling))
        held = dict(me)
        first = True
        for axis in order:
            if axis == "xh":
                other = shifted(me, "x", 2)
                copy = copies.start(ins[i], pick_out(out, me, True), other)
                yield
                copy.wait_recv()
                push(pushes, pick_out(out, other, True))
                locals_[i].wait()
                first = False
                held.pop("x")
                continue
            up, down, far = (shifted(me, axis, s) for s in (1, 3, 2))
            block = pick_out(out, held, teacher)
            source = ins[i] if first else block
            right = copies.start(source, block, up)
            left = copies.start(source, block, down)
            yield
            right.wait_recv()
            from_down = pick_out(out, {**held, axis: down[axis]}, teacher)
            right2 = copies.start(half(from_down, 0), half(from_down, 0), up)
            push(pushes, from_down)
            left.wait_recv()
            from_up = pick_out(out, {**held, axis: up[axis]}, teacher)
            left2 = copies.start(half(from_up, 1), half(from_up, 1), down)
            push(pushes, from_up)
            if first:
                locals_[i].wait()
                first = False
            yield
            right2.wait_recv()
            left2.wait_recv()
            push(pushes, pick_out(out, {**held, axis: far[axis]}, teacher))
            held.pop(axis)
        yield
        for copy in pushes:
            copy.wait_recv()

    chains = [
        chain(2, ("y", "z", "x")),
        chain(3, ("z", "y", "x")),
        chain(4, ("y", "z", "x")),
        chain(5, ("z", "y", "x")),
        chain(0, ("xh", "y", "z")),
        chain(1, ("xh", "z", "y")),
    ]
    while chains:
        alive = []
        for one in chains:
            try:
                next(one)
                alive.append(one)
            except StopIteration:
                pass
        chains = alive
    copies.finish()


def pick_out(ref, at, teacher):
    if not teacher:
        return pick(ref, at)
    whole = slice(None)
    x = at.get("x")
    return ref.at[
        (
            at.get("y", whole),
            whole if x is None else x // 2,
            at.get("z", whole),
            at["core"],
        )
    ]


def weight_kernel(*refs):
    ins, outs = refs[:6], refs[6:12]
    weight_gather(ins, outs, *refs[12:])


def gather_weights(parts):
    outs = []
    for i, part in enumerate(parts):
        lead = (4, 2, 4, 2) if i < 2 else (2, 4, 2, 4, 2)
        outs.append(jax.ShapeDtypeStruct(lead + part.shape, part.dtype))
    return pl.pallas_call(
        weight_kernel,
        out_shape=outs,
        in_specs=[ANY] * 6,
        out_specs=[ANY] * 6,
        scratch_shapes=[
            pltpu.SemaphoreType.DMA((122,)),
            pltpu.SemaphoreType.DMA((122,)),
            pltpu.SemaphoreType.DMA((6,)),
        ],
        compiler_params=pltpu.CompilerParams(collective_id=1, has_side_effects=True),
        name="gather_weights",
    )(*parts)


def caption_kernel(p_ref, out_ref, other, at_x, at_y, at_z, send, recv):
    me = coords()
    enter(me)
    copies = Copies(send, recv)
    copy = copies.start(p_ref, other, shifted(me, "core", 1))
    copy.wait_recv()
    other[...] = other[...] + p_ref[...]

    def exchange(axis, source, slots):
        waits = []
        for step in (2, 1, 3):
            peer = shifted(me, axis, step)
            waits.append(copies.start(source.at[peer[axis]], slots.at[me[axis]], peer))
        slots[me[axis]] = source[me[axis]]
        for copy in waits:
            copy.wait_recv()
        return (slots[0] + slots[1]) + (slots[2] + slots[3])

    sum_x = exchange("x", other, at_x)
    at_x2 = at_x.at[4]
    at_x2[...] = sum_x
    sum_y = exchange("y", at_x2, at_y)
    at_y2 = at_y.at[4]
    at_y2[...] = sum_y
    sum_z = exchange("z", at_y2, at_z)
    own = out_ref.at[me["x"], me["y"], me["z"]]
    own[...] = sum_z

    def spread(axis, view):
        waits = []
        for step in (2, 1, 3):
            waits.append(copies.start(view, view, shifted(me, axis, step)))
        for copy in waits:
            copy.wait_recv()

    spread("z", own)
    spread("y", out_ref.at[me["x"], me["y"]])
    spread("x", out_ref.at[me["x"]])
    copies.finish()


def sum_captions(partial):
    shape = (4, 4, 4, 8, 128)
    tiles = partial.reshape(16, 8, 4, 128).transpose(0, 2, 1, 3).reshape(shape)
    out = pl.pallas_call(
        caption_kernel,
        out_shape=jax.ShapeDtypeStruct(shape, jnp.float32),
        in_specs=[VM],
        out_specs=VM,
        scratch_shapes=[
            pltpu.VMEM(shape, jnp.float32),
            pltpu.VMEM((5, 4, 4, 8, 128), jnp.float32),
            pltpu.VMEM((5, 4, 8, 128), jnp.float32),
            pltpu.VMEM((4, 8, 128), jnp.float32),
            pltpu.SemaphoreType.DMA((19,)),
            pltpu.SemaphoreType.DMA((19,)),
        ],
        compiler_params=pltpu.CompilerParams(collective_id=2, has_side_effects=True),
        name="sum_captions",
    )(tiles)
    return out.reshape(16, 4, 8, 128).transpose(0, 2, 1, 3).reshape(128, 512)


def image_kernel(p_ref, out_ref, send, recv):
    me = coords()
    enter(me)
    copies = Copies(send, recv)
    pick(out_ref, me)[...] = p_ref[...]
    held = dict(me)
    first = True
    for axis in ("core", "z", "y", "x"):
        waits = []
        view = pick(out_ref, held)
        for step in (1,) if axis == "core" else (2, 1, 3):
            waits.append(copies.start(p_ref if first else view, view, shifted(me, axis, step)))
        first = False
        for copy in waits:
            copy.wait_recv()
        held.pop(axis)
    copies.finish()


def gather_images(pooled):
    tile = jnp.pad(pooled.reshape(6, 128), ((0, 10), (0, 0)))
    shape = (2, 4, 2, 4, 2, 16, 128)
    out = pl.pallas_call(
        image_kernel,
        out_shape=jax.ShapeDtypeStruct(shape, pooled.dtype),
        in_specs=[VM],
        out_specs=VM,
        scratch_shapes=[
            pltpu.SemaphoreType.DMA((10,)),
            pltpu.SemaphoreType.DMA((10,)),
        ],
        compiler_params=pltpu.CompilerParams(collective_id=3, has_side_effects=True),
        name="gather_images",
    )(tile)
    return out.reshape(128, 16, 128)[:, :6].reshape(128, 768)


ORDERS = (("x", "y", "z"), ("y", "z", "x"), ("z", "x", "y"))


def dims_of(axes):
    dims = []
    if "x" in axes:
        dims.append(2)
    if "y" in axes:
        dims.append(4)
    if "x" in axes:
        dims.append(2)
    if "z" in axes:
        dims.append(4)
    return tuple(dims)


def rest_of(order, phase):
    return [a for a in ("x", "y", "z") if a not in order[: phase + 1]]


def half_shape(order, phase):
    shape = dims_of(rest_of(order, phase)) + (BLK, 768)
    if len(shape) == 2:
        return (BLK, 384)
    return (shape[0] // 2,) + shape[1:]


def split(ref, side):
    if len(ref.shape) == 2:
        return ref.at[:, pl.ds(side * 384, 384)]
    return half(ref, side)


def add_into(dst, srcs, out=None):
    lead = dst.shape[:-2]
    total = 1
    for size in lead:
        total *= size

    def one(index):
        value = dst[index].astype(jnp.float32)
        for src in srcs:
            value = value + src[index].astype(jnp.float32)
        dst[index] = value.astype(dst.dtype)

    if total == 1:
        one((0,) * len(lead) + (slice(None), slice(None)))
        return

    def body(n, carry):
        index = []
        rest = n
        for size in reversed(lead):
            index.append(rest % size)
            rest = rest // size
        one(tuple(reversed(index)))
        return carry

    lax.fori_loop(0, total, body, 0)


def scatter_kernel(*refs):
    grads, s_ref = refs[0:3], refs[3]
    outs, s_out = refs[4:7], refs[7]
    accs = refs[8:11]
    hold = refs[11:29]
    s_slots, send, recv = refs[29], refs[30], refs[31]
    first = lambda t, p: hold[(t * 3 + p) * 2]
    second = lambda t, p: hold[(t * 3 + p) * 2 + 1]
    me = coords()
    enter(me)
    copies = Copies(send, recv)
    sibling = shifted(me, "core", 1)
    opening = []
    for t in range(3):
        opening.append(copies.start(grads[t].at[:, :, :, :, sibling["core"]], accs[t], sibling))
    s_wait = [copies.start(s_ref, s_slots.at[0, me["core"]], sibling)]
    s_slots[0, me["core"]] = s_ref[...]
    pending = [None] * 3
    held = [dict() for _ in range(3)]

    def open_phase(t, phase):
        axis = ORDERS[t][phase]
        far = shifted(me, axis, 2)
        view = pick(accs[t], {**held[t], axis: far[axis]})
        up, down = shifted(me, axis, 1), shifted(me, axis, 3)
        return (
            copies.start(split(view, 0), first(t, phase).at[0], up),
            copies.start(split(view, 1), first(t, phase).at[1], down),
        )

    for t in range(3):
        opening[t].wait_recv()
        add_into(accs[t], [grads[t].at[:, :, :, :, me["core"]]])
        pending[t] = open_phase(t, 0)
    for copy in s_wait:
        copy.wait_recv()
    s_value = s_slots[0, 0] + s_slots[0, 1]
    for phase in range(3):
        s_axis = ("x", "y", "z")[phase]
        s_slots[phase + 1, me[s_axis]] = s_value
        s_wait = []
        for step in (1, 2, 3):
            s_mine = s_slots.at[phase + 1, me[s_axis]]
            s_wait.append(copies.start(s_mine, s_mine, shifted(me, s_axis, step)))
        for t in range(3):
            axis = ORDERS[t][phase]
            up, down = shifted(me, axis, 1), shifted(me, axis, 3)
            to_up = pick(accs[t], {**held[t], axis: up[axis]})
            to_down = pick(accs[t], {**held[t], axis: down[axis]})
            pending[t][0].wait_recv()
            add_into(split(to_up, 0), [first(t, phase).at[0]])
            a = copies.start(to_up, second(t, phase).at[0], up)
            pending[t][1].wait_recv()
            add_into(split(to_down, 1), [first(t, phase).at[1]])
            b = copies.start(to_down, second(t, phase).at[1], down)
            pending[t] = (a, b)
        for t in range(3):
            axis = ORDERS[t][phase]
            pending[t][0].wait_recv()
            pending[t][1].wait_recv()
            held[t][axis] = me[axis]
            mine = pick(accs[t], held[t])
            if phase < 2:
                add_into(mine, [second(t, phase).at[0], second(t, phase).at[1]])
                pending[t] = open_phase(t, phase + 1)
            else:
                value = mine[...].astype(jnp.float32) + second(t, phase)[0].astype(jnp.float32)
                value = value + second(t, phase)[1].astype(jnp.float32)
                outs[t][...] = value[: outs[t].shape[0]]
        for copy in s_wait:
            copy.wait_recv()
        s_value = (s_slots[phase + 1, 0] + s_slots[phase + 1, 1]) + (
            s_slots[phase + 1, 2] + s_slots[phase + 1, 3]
        )
    s_out[...] = s_value
    copies.finish()


def scatter_grads(grads, rows, scalar):
    lead = (2, 4, 2, 4, 2, BLK, 768)
    grads = [g.reshape(lead) for g in grads]
    tile = jnp.full((8, 128), scalar, jnp.float32)
    scratch = [pltpu.VMEM((2, 4, 2, 4, BLK, 768), jnp.bfloat16) for _ in range(3)]
    for t in range(3):
        for phase in range(3):
            scratch.append(pltpu.VMEM((2,) + half_shape(ORDERS[t], phase), jnp.bfloat16))
            scratch.append(
                pltpu.VMEM((2,) + dims_of(rest_of(ORDERS[t], phase)) + (BLK, 768), jnp.bfloat16)
            )
    scratch += [
        pltpu.VMEM((4, 4, 8, 128), jnp.float32),
        pltpu.SemaphoreType.DMA((49,)),
        pltpu.SemaphoreType.DMA((49,)),
    ]
    return pl.pallas_call(
        scatter_kernel,
        out_shape=[jax.ShapeDtypeStruct((r, 768), jnp.float32) for r in rows]
        + [jax.ShapeDtypeStruct((8, 128), jnp.float32)],
        in_specs=[VM] * 4,
        out_specs=[VM] * 4,
        scratch_shapes=scratch,
        compiler_params=pltpu.CompilerParams(
            collective_id=4, has_side_effects=True, vmem_limit_bytes=48 * 1024 * 1024
        ),
        name="scatter_grads",
    )(*grads, tile)


def gelu_tanh(values):
    return jax.nn.gelu(values, approximate=True)


def pad_blocks(values, size, axis):
    shape = values.shape
    blocks = shape[axis] // size
    cut = values.reshape(shape[:axis] + (blocks, size) + shape[axis + 1 :])
    pads = [(0, 0)] * cut.ndim
    pads[axis + 1] = (0, BLK - size)
    return jnp.pad(cut, pads).reshape(shape[:axis] + (blocks * BLK,) + shape[axis + 1 :])


def unit_rows(values):
    return values / jnp.sqrt(jnp.sum(values * values, -1, keepdims=True) + 1e-06)


def dot(a, b, da, db):
    return lax.dot_general(a, b, (((da,), (db,)), ((), ())), preferred_element_type=jnp.float32)


def local(
    teacher_in,
    teacher_gain,
    teacher_up,
    teacher_down,
    student_in,
    student_gain,
    student_up,
    student_down,
    student_head,
    student_proj,
    word_table,
    caption_ids,
    positive,
):
    grp_index = lax.axis_index("grp")
    dp_index = lax.axis_index("dp")
    n_grp = lax.axis_size("grp")
    n_dp = lax.axis_size("dp")
    shard = grp_index * n_dp + dp_index
    width = teacher_in.shape[1]
    feat = width // (n_grp * n_dp)
    hid = student_up.shape[1]
    own_rows = teacher_in.shape[0] // n_grp

    proj_cols = student_proj.shape[1]
    parts = [
        pad_blocks(teacher_up, feat, 0),
        pad_blocks(teacher_down, feat, 0),
        pad_blocks(student_up.T, hid, 0),
        pad_blocks(student_down, hid, 0),
        pad_blocks(student_head.T, feat, 0),
        jnp.pad(student_proj.T, ((0, BLK - proj_cols), (0, 0))),
    ]
    t_up, t_down, s_up, s_down, s_head, s_proj = gather_weights(parts)
    t_up = t_up.reshape(-1, t_up.shape[-1])
    t_down = t_down.reshape(-1, t_down.shape[-1])
    s_up, s_down, s_head = (v.reshape(-1, v.shape[-1]) for v in (s_up, s_down, s_head))
    s_proj = s_proj.reshape(-1, BLK, s_proj.shape[-1])[:, :proj_cols]
    s_proj = s_proj.reshape(-1, s_proj.shape[-1])

    vocab_dev = word_table.shape[0]
    vocab_codes = shard * vocab_dev + jnp.arange(vocab_dev, dtype=jnp.int32)
    counts = jnp.sum(
        caption_ids[:, :, None] == vocab_codes[None, None, :], 1, dtype=jnp.float32
    ).astype(jnp.bfloat16)
    partial_words = jnp.dot(counts, word_table, preferred_element_type=jnp.float32) / CAP_LEN
    caption_all = unit_rows(sum_captions(partial_words))

    wide = t_up.shape[0]
    place = jnp.arange(width, dtype=jnp.int32)
    place = place // feat * BLK + place % feat
    spread_map = (place[:, None] == jnp.arange(wide, dtype=jnp.int32)[None, :]).astype(jnp.bfloat16)
    teacher_wide = dot(teacher_in, spread_map, 1, 0).astype(jnp.bfloat16)
    gain_wide = pad_blocks(teacher_gain, feat, 0)
    real = (jnp.arange(wide, dtype=jnp.int32) % BLK < feat)[None, :]
    values = teacher_wide.astype(jnp.float32)
    mean = jnp.sum(values, -1, keepdims=True) / width
    center = jnp.where(real, values - mean, 0.0)
    variance = jnp.sum(center * center, -1, keepdims=True) / width
    teacher_normed = (center * lax.rsqrt(variance + 1e-05) * gain_wide).astype(jnp.bfloat16)
    teacher_act = gelu_tanh(dot(teacher_normed, t_up, 1, 0)).astype(jnp.bfloat16)
    branch = dot(teacher_act, t_down, 1, 1).astype(jnp.bfloat16)
    branch_own = lax.dynamic_slice_in_dim(branch, grp_index * own_rows, own_rows, 0)
    branch_far = lax.dynamic_slice_in_dim(branch, (1 - grp_index) * own_rows, own_rows, 0)
    branch_got = lax.ppermute(branch_far, "grp", [(0, 1), (1, 0)])
    teacher_own = lax.dynamic_slice_in_dim(teacher_wide, grp_index * own_rows, own_rows, 0)

    rows = lax.dynamic_slice_in_dim(student_in, grp_index * own_rows, own_rows, 0).astype(
        jnp.float32
    )
    center = rows - jnp.mean(rows, -1, keepdims=True)
    variance = jnp.mean(center * center, -1, keepdims=True)
    normed = (center * lax.rsqrt(variance + 1e-05) * student_gain).astype(jnp.bfloat16)
    gate_out = dot(normed, s_up, 1, 1)
    act = gelu_tanh(gate_out).astype(jnp.bfloat16)
    student_out = rows + dot(act, s_down, 1, 0)
    rounded = student_out.astype(jnp.bfloat16)
    pooled = (jnp.sum(student_out, 0, keepdims=True) / PATCHES).astype(jnp.bfloat16)

    pooled_all = gather_images(pooled)
    projected = dot(pooled_all, s_proj, 1, 1)
    proj_norm = jnp.sqrt(jnp.sum(projected * projected, -1, keepdims=True) + 1e-06)
    image_emb = projected / proj_norm
    scores = 100.0 * jnp.dot(image_emb, caption_all.T, precision=lax.Precision.HIGHEST)
    target_of = positive.reshape(n_dp, n_grp).T.reshape(-1)
    match = (target_of[:, None] == jnp.arange(scores.shape[1], dtype=jnp.int32)[None, :]).astype(
        jnp.float32
    )
    contrast = (
        jnp.sum(jax.nn.logsumexp(scores, 1))
        + jnp.sum(jax.nn.logsumexp(scores, 0))
        - 2.0 * jnp.sum(match * scores)
    )
    grad_scores = jax.nn.softmax(scores, 1) + jax.nn.softmax(scores, 0) - 2.0 * match
    grad_image = 100.0 * jnp.dot(grad_scores, caption_all, precision=lax.Precision.HIGHEST)
    grad_projected = (
        (grad_image - image_emb * jnp.sum(image_emb * grad_image, -1, keepdims=True)) / proj_norm
    ).astype(jnp.bfloat16)
    grad_columns = lax.dynamic_slice_in_dim(grad_projected, shard * proj_cols, proj_cols, 1)
    grad_proj = dot(grad_columns, pooled_all, 0, 0).T
    grad_projected_own = lax.dynamic_slice_in_dim(grad_projected, shard, 1, 0)
    grad_pooled = dot(grad_projected_own, s_proj, 1, 0)

    target = teacher_own.astype(jnp.float32) + (
        branch_own.astype(jnp.float32) + branch_got.astype(jnp.float32)
    )
    diff = dot(rounded, s_head, 1, 1) - target
    feature_part = jnp.sum(diff * diff) / width
    grad_pred = (2.0 * diff / width).astype(jnp.bfloat16)
    head_part = dot(grad_pred, rounded, 0, 0).astype(jnp.bfloat16)
    grad_out = (dot(grad_pred, s_head, 1, 0) + grad_pooled / PATCHES).astype(jnp.bfloat16)
    down_part = dot(act, grad_out, 0, 0).astype(jnp.bfloat16)
    grad_act = dot(grad_out, s_down, 1, 1)
    grad_gate = jax.vjp(gelu_tanh, gate_out)[1](grad_act)[0].astype(jnp.bfloat16)
    up_part = dot(grad_gate, normed, 0, 0).astype(jnp.bfloat16)
    grad_up, grad_down, grad_head, feature = scatter_grads(
        (up_part, down_part, head_part), (hid, hid, feat), feature_part
    )
    loss = (feature[0, 0] + contrast) / (positive.shape[0] * PATCHES)
    return (loss, grad_up.T, grad_down, grad_head.T, grad_proj)


def solution(mesh):
    placed = (
        P("dp", None),
        P(),
        P("dp", "grp"),
        P("dp", "grp"),
        P("dp", None),
        P(),
        P(None, ("grp", "dp")),
        P(("grp", "dp"), None),
        P(None, ("grp", "dp")),
        P(None, ("grp", "dp")),
        P(("grp", "dp"), None),
        P(),
        P(),
    )
    return jax.shard_map(
        local,
        mesh=mesh,
        in_specs=placed,
        out_specs=(
            P(),
            P(None, ("grp", "dp")),
            P(("grp", "dp"), None),
            P(None, ("grp", "dp")),
            P(None, ("grp", "dp")),
        ),
        check_vma=False,
    )
```

```python
import jax
import jax.numpy as jnp
from jax import lax
from jax.experimental import pallas as pl
from jax.experimental.pallas import tpu as pltpu
from jax.sharding import PartitionSpec as P

CAP_LEN = 77
PATCHES = 256
BLK = 16
MESH = pl.DeviceIdType.MESH
ANY = pl.BlockSpec(memory_space=pl.ANY)
VM = pl.BlockSpec(memory_space=pltpu.VMEM)


def coords():
    grp = lax.axis_index("grp")
    dp = lax.axis_index("dp")
    x_hi = (dp // 8) % 2
    return {
        "x": 2 * x_hi + grp,
        "y": dp // 16,
        "z": (dp // 2) % 4,
        "core": dp % 2,
    }


def device(at):
    return (at["x"] % 2, at["y"] * 16 + (at["x"] // 2) * 8 + at["z"] * 2 + at["core"])


def shifted(me, axis, step):
    if axis == "core":
        return {**me, "core": 1 - me["core"]}
    return {**me, axis: (me[axis] + step) % 4}


def enter(me, axes=("x", "y", "z"), steps=(1, 2, 3)):
    barrier = pltpu.get_barrier_semaphore()
    peers = [shifted(me, "core", 1)]
    for axis in axes:
        for step in steps:
            peers.append(shifted(me, axis, step))
    for peer in peers:
        pl.semaphore_signal(barrier, inc=1, device_id=device(peer), device_id_type=MESH)
    pl.semaphore_wait(barrier, len(peers))


class Copies:
    def __init__(self, send, recv):
        self.send, self.recv, self.count, self.open = send, recv, 0, []

    def start(self, src, dst, peer):
        copy = pltpu.make_async_remote_copy(
            src_ref=src,
            dst_ref=dst,
            send_sem=self.send.at[self.count],
            recv_sem=self.recv.at[self.count],
            device_id=device(peer),
            device_id_type=MESH,
        )
        self.count += 1
        copy.start()
        self.open.append(copy)
        return copy

    def finish(self):
        for copy in self.open:
            copy.wait_send()


def pick(ref, at, tail=()):
    x = at.get("x")
    whole = slice(None)
    index = (
        whole if x is None else x % 2,
        at.get("y", whole),
        whole if x is None else x // 2,
        at.get("z", whole),
    )
    if "core" in at:
        index += (at["core"],)
    return ref.at[index + tail]


def half(ref, side):
    if len(ref.shape) > 2:
        size = ref.shape[0] // 2
        return ref.at[pl.ds(side * size, size)]
    lanes = ref.shape[1] // 128
    cut = lanes // 2 * 128
    if side == 0:
        return ref.at[:, pl.ds(0, cut)]
    return ref.at[:, pl.ds(cut, ref.shape[1] - cut)]


def pick_teacher(ref, at, tail=()):
    whole = slice(None)
    index = (
        at.get("y", whole),
        at["x"] // 2,
        at.get("z", whole),
        at["core"],
    )
    return ref.at[index + tail]


def ring(copies, me, sibling, view, order, held, pushes):
    for axis in order:
        up, down, far = (shifted(me, axis, s) for s in (1, 3, 2))
        block = view(held)
        right = copies.start(block, block, up)
        left = copies.start(block, block, down)
        yield
        right.wait_recv()
        from_down = view({**held, axis: down[axis]})
        right2 = copies.start(half(from_down, 0), half(from_down, 0), up)
        pushes.append(copies.start(from_down, from_down, sibling))
        left.wait_recv()
        from_up = view({**held, axis: up[axis]})
        left2 = copies.start(half(from_up, 1), half(from_up, 1), down)
        pushes.append(copies.start(from_up, from_up, sibling))
        yield
        right2.wait_recv()
        left2.wait_recv()
        from_far = view({**held, axis: far[axis]})
        pushes.append(copies.start(from_far, from_far, sibling))
        held.pop(axis)


def student_chain(copies, me, sibling, ref, order):
    view = lambda at: pick(ref, at)
    own = view(me)
    pushes = [copies.start(own, own, sibling)]
    yield from ring(copies, me, sibling, view, order, dict(me), pushes)
    yield
    for copy in pushes:
        copy.wait_recv()


def teacher_chain(copies, me, sibling, ref, part, order, other):
    tail = (pl.ds(part * BLK, BLK),)
    view = lambda at: pick_teacher(ref, at, tail)
    pushes = []
    held = dict(me)
    if other:
        far = shifted(me, "x", 2)
        copy = copies.start(view(me), view(me), far)
        yield
        copy.wait_recv()
        held = dict(far)
    block = view(held)
    pushes.append(copies.start(block, block, sibling))
    yield from ring(copies, me, sibling, view, order, held, pushes)
    yield
    for copy in pushes:
        copy.wait_recv()


def caption_chain(copies, me, sibling, p_ref, out_ref, other, at_x, at_y, at_z):
    copy = copies.start(p_ref, other, sibling)
    yield
    copy.wait_recv()
    other[...] = other[...] + p_ref[...]

    def exchange(axis, source, slots):
        waits = []
        for step in (2, 1, 3):
            peer = shifted(me, axis, step)
            waits.append(copies.start(source.at[peer[axis]], slots.at[me[axis]], peer))
        slots[me[axis]] = source[me[axis]]
        return waits

    def total(waits, slots):
        for copy in waits:
            copy.wait_recv()
        return (slots[0] + slots[1]) + (slots[2] + slots[3])

    def spread(axis, view):
        return [copies.start(view, view, shifted(me, axis, step)) for step in (2, 1, 3)]

    waits = exchange("x", other, at_x)
    yield
    at_x[4] = total(waits, at_x)
    waits = exchange("y", at_x.at[4], at_y)
    yield
    at_y[4] = total(waits, at_y)
    waits = exchange("z", at_y.at[4], at_z)
    yield
    own = out_ref.at[me["x"], me["y"], me["z"]]
    own[...] = total(waits, at_z)
    for axis, view in (
        ("z", own),
        ("y", out_ref.at[me["x"], me["y"]]),
        ("x", out_ref.at[me["x"]]),
    ):
        waits = spread(axis, view)
        yield
        for copy in waits:
            copy.wait_recv()


def rows_padded(values, rows):
    short = rows - values.shape[0]
    if short == 0:
        return values
    return jnp.concatenate([values, jnp.zeros((short, values.shape[1]), values.dtype)], 0)


def weight_kernel(
    t_up, t_down, up, down, head, proj, words,
    o_up, o_down, o_pack, o_head, o_proj, o_words,
    other, at_x, at_y, at_z, send, recv,
):
    me = coords()
    sibling = shifted(me, "core", 1)
    feat = head.shape[0]
    f32 = jnp.float32
    pick(o_pack, me)[...] = jnp.concatenate(
        [up[...].astype(f32), down[...].astype(f32)], 0
    ).astype(o_pack.dtype)
    pick(o_head, me)[...] = rows_padded(head[...].astype(f32), BLK).astype(o_head.dtype)
    wide = proj[...].astype(f32)
    cut = wide.shape[1] // 2
    pick(o_proj, me)[...] = jnp.concatenate([wide[:, :cut], wide[:, cut:]], 0).astype(o_proj.dtype)
    for source, out in ((t_up, o_up), (t_down, o_down)):
        values = source[...].astype(f32)
        for part in range(2):
            cut = values[part * feat : (part + 1) * feat]
            pick_teacher(out, me, (pl.ds(part * BLK, BLK),))[...] = rows_padded(cut, BLK).astype(
                out.dtype
            )
    enter(me)
    copies = Copies(send, recv)
    pack = [
        student_chain(copies, me, sibling, o_pack, ("y", "z", "x")),
        student_chain(copies, me, sibling, o_head, ("z", "y", "x")),
        student_chain(copies, me, sibling, o_proj, ("z", "y", "x")),
    ]
    caps = [caption_chain(copies, me, sibling, words, o_words, other, at_x, at_y, at_z)]

    def teacher(ref, other_x):
        return [
            teacher_chain(copies, me, sibling, ref, 0, ("y", "z"), other_x),
            teacher_chain(copies, me, sibling, ref, 1, ("z", "y"), other_x),
        ]

    ua, da = teacher(o_up, False), teacher(o_down, False)
    ub, db = teacher(o_up, True), teacher(o_down, True)
    order = [pack, caps, ua, ub, da, db]
    order += [pack, caps, ua, pack, caps, da, pack, caps, ua, pack, caps, da]
    order += [ub, db, caps, ua, da, ub, db, caps, ua, da, ub, db, caps, pack]
    order += [ua, da, ub, db, pack] * 8 + [caps] * 8
    for group in order:
        for one in group:
            next(one, None)
    copies.finish()


N_COPIES = 22 * 3 + 19 + 4 * 15 + 4 * 16


def gather_weights(t_up, t_down, up, down, head, proj, words):
    dtype = t_up.dtype
    width = up.shape[1]
    whole = (2, 4, 2, 4, 2)
    tiles = (4, 4, 4, 8, 128)
    shapes = [
        (4, 2, 4, 2, 2 * BLK, t_up.shape[1]),
        (4, 2, 4, 2, 2 * BLK, t_up.shape[1]),
        whole + (up.shape[0] + down.shape[0], width),
        whole + (BLK, width),
        whole + (2 * proj.shape[0], width // 2),
    ]
    out = pl.pallas_call(
        weight_kernel,
        out_shape=[jax.ShapeDtypeStruct(s, dtype) for s in shapes]
        + [jax.ShapeDtypeStruct(tiles, jnp.float32)],
        in_specs=[VM] * 7,
        out_specs=[VM] * 6,
        scratch_shapes=[
            pltpu.VMEM(tiles, jnp.float32),
            pltpu.VMEM((5, 4, 4, 8, 128), jnp.float32),
            pltpu.VMEM((5, 4, 8, 128), jnp.float32),
            pltpu.VMEM((4, 8, 128), jnp.float32),
            pltpu.SemaphoreType.DMA((N_COPIES,)),
            pltpu.SemaphoreType.DMA((N_COPIES,)),
        ],
        compiler_params=pltpu.CompilerParams(
            collective_id=1, has_side_effects=True, vmem_limit_bytes=40 * 1024 * 1024
        ),
        name="gather_weights",
    )(
        t_up, t_down, up, down, head, proj,
        words.reshape(16, 8, 4, 128).transpose(0, 2, 1, 3).reshape(tiles),
    )
    words = out[5].reshape(16, 4, 8, 128).transpose(0, 2, 1, 3).reshape(128, 512)
    return list(out[:5]) + [words]


def image_kernel(p_ref, out_ref, send, recv):
    me = coords()
    enter(me)
    copies = Copies(send, recv)
    pick(out_ref, me)[...] = p_ref[...]
    held = dict(me)
    first = True
    for axis in ("core", "z", "y", "x"):
        waits = []
        view = pick(out_ref, held)
        for step in (1,) if axis == "core" else (2, 1, 3):
            waits.append(copies.start(p_ref if first else view, view, shifted(me, axis, step)))
        first = False
        for copy in waits:
            copy.wait_recv()
        held.pop(axis)
    copies.finish()


def gather_images(pooled):
    tile = jnp.pad(pooled.reshape(6, 128), ((0, 10), (0, 0)))
    shape = (2, 4, 2, 4, 2, 16, 128)
    out = pl.pallas_call(
        image_kernel,
        out_shape=jax.ShapeDtypeStruct(shape, pooled.dtype),
        in_specs=[VM],
        out_specs=VM,
        scratch_shapes=[
            pltpu.SemaphoreType.DMA((10,)),
            pltpu.SemaphoreType.DMA((10,)),
        ],
        compiler_params=pltpu.CompilerParams(collective_id=3, has_side_effects=True),
        name="gather_images",
    )(tile)
    return out.reshape(128, 16, 128)[:, :6].reshape(128, 768)


ORDERS = (("x", "y", "z"), ("y", "z", "x"), ("z", "x", "y"))
COLS = 256


def dims_of(axes):
    dims = []
    if "x" in axes:
        dims.append(2)
    if "y" in axes:
        dims.append(4)
    if "x" in axes:
        dims.append(2)
    if "z" in axes:
        dims.append(4)
    return tuple(dims)


def rest_of(order, phase):
    return [a for a in ("x", "y", "z") if a not in order[: phase + 1]]


def half_shape(order, phase, rows):
    shape = dims_of(rest_of(order, phase)) + (rows, COLS)
    if len(shape) == 2:
        return (rows, COLS // 2)
    return (shape[0] // 2,) + shape[1:]


def add_into(dst, srcs):
    lead = dst.shape[:-2]
    total = 1
    for size in lead:
        total *= size

    def one(index):
        value = dst[index].astype(jnp.float32)
        for src in srcs:
            value = value + src[index].astype(jnp.float32)
        dst[index] = value.astype(dst.dtype)

    if total == 1:
        one((0,) * len(lead) + (slice(None), slice(None)))
        return

    def body(n, carry):
        index = []
        rest = n
        for size in reversed(lead):
            index.append(rest % size)
            rest = rest // size
        one(tuple(reversed(index)))
        return carry

    lax.fori_loop(0, total, body, 0)


def rows_of(view, first, count, cols=None):
    lead = (slice(None),) * (len(view.shape) - 2)
    return view.at[lead + (pl.ds(first, count), slice(None) if cols is None else cols)]


def scatter_kernel(pack, head, s_ref, o_up, o_down, o_head, s_out, *refs):
    accs = refs[0:3]
    hold = refs[3:21]
    s_slots, send, recv = refs[21:]
    first = lambda t, p: hold[(t * 3 + p) * 2]
    second = lambda t, p: hold[(t * 3 + p) * 2 + 1]
    n_pack, n_head = pack.shape[-2], head.shape[-2]
    me = coords()
    enter(me)
    copies = Copies(send, recv)
    sibling = shifted(me, "core", 1)

    def sources(t, at):
        cols = pl.ds(t * COLS, COLS)
        return ((0, rows_of(pick(pack, at), 0, n_pack, cols)), (n_pack, rows_of(pick(head, at), 0, n_head, cols)))

    opening = {}
    for step in (2, 1, 3, 0):
        for t in range(3):
            axis = ORDERS[t][0]
            at = {axis: shifted(me, axis, step)[axis]}
            target = pick(accs[t], at)
            opening[t, step] = [
                copies.start(src, rows_of(target, row, src.shape[-2]), sibling)
                for row, src in sources(t, {**at, "core": sibling["core"]})
            ]
    s_wait = [copies.start(s_ref, s_slots.at[0, me["core"]], sibling)]
    s_slots[0, me["core"]] = s_ref[...]
    pending = [None] * 3
    held = [dict() for _ in range(3)]

    def opened(t, step):
        axis = ORDERS[t][0]
        at = {axis: shifted(me, axis, step)[axis]}
        for copy in opening[t, step]:
            copy.wait_recv()
        target = pick(accs[t], at)
        for row, src in sources(t, {**at, "core": me["core"]}):
            add_into(rows_of(target, row, src.shape[-2]), [src])

    def open_phase(t, phase):
        axis = ORDERS[t][phase]
        far = shifted(me, axis, 2)
        view = pick(accs[t], {**held[t], axis: far[axis]})
        up, down = shifted(me, axis, 1), shifted(me, axis, 3)
        return (
            copies.start(half(view, 0), first(t, phase).at[0], up),
            copies.start(half(view, 1), first(t, phase).at[1], down),
        )

    for t in range(3):
        opened(t, 2)
        pending[t] = open_phase(t, 0)
    for step in (1, 3, 0):
        for t in range(3):
            opened(t, step)
    for copy in s_wait:
        copy.wait_recv()
    s_value = s_slots[0, 0] + s_slots[0, 1]
    for phase in range(3):
        s_axis = ("x", "y", "z")[phase]
        s_slots[phase + 1, me[s_axis]] = s_value
        s_wait = []
        for step in (1, 2, 3):
            s_mine = s_slots.at[phase + 1, me[s_axis]]
            s_wait.append(copies.start(s_mine, s_mine, shifted(me, s_axis, step)))
        for t in range(3):
            axis = ORDERS[t][phase]
            up, down = shifted(me, axis, 1), shifted(me, axis, 3)
            to_up = pick(accs[t], {**held[t], axis: up[axis]})
            to_down = pick(accs[t], {**held[t], axis: down[axis]})
            pending[t][0].wait_recv()
            add_into(half(to_up, 0), [first(t, phase).at[0]])
            a = copies.start(to_up, second(t, phase).at[0], up)
            pending[t][1].wait_recv()
            add_into(half(to_down, 1), [first(t, phase).at[1]])
            b = copies.start(to_down, second(t, phase).at[1], down)
            pending[t] = (a, b)
        for t in range(3):
            axis = ORDERS[t][phase]
            pending[t][0].wait_recv()
            pending[t][1].wait_recv()
            held[t][axis] = me[axis]
            mine = pick(accs[t], held[t])
            if phase < 2:
                add_into(mine, [second(t, phase).at[0], second(t, phase).at[1]])
                pending[t] = open_phase(t, phase + 1)
            else:
                value = mine[...].astype(jnp.float32) + second(t, phase)[0].astype(jnp.float32)
                value = value + second(t, phase)[1].astype(jnp.float32)
                cols = pl.ds(t * COLS, COLS)
                hid = o_up.shape[0]
                o_up[:, cols] = value[:hid]
                o_down[:, cols] = value[hid:n_pack]
                o_head[:, cols] = value[n_pack : n_pack + o_head.shape[0]]
        for copy in s_wait:
            copy.wait_recv()
        s_value = (s_slots[phase + 1, 0] + s_slots[phase + 1, 1]) + (
            s_slots[phase + 1, 2] + s_slots[phase + 1, 3]
        )
    s_out[...] = s_value
    copies.finish()


def scatter_grads(pack, head, hid, feat, scalar):
    lead = (2, 4, 2, 4, 2)
    width = pack.shape[1]
    pack = pack.reshape(lead + (2 * hid, width))
    head = head.reshape(lead + (BLK, width))
    rows = 2 * hid + BLK
    tile = jnp.full((8, 128), scalar, jnp.float32)
    scratch = [pltpu.VMEM((2, 4, 2, 4, rows, COLS), jnp.bfloat16) for _ in range(3)]
    for t in range(3):
        for phase in range(3):
            scratch.append(pltpu.VMEM((2,) + half_shape(ORDERS[t], phase, rows), jnp.bfloat16))
            scratch.append(
                pltpu.VMEM((2,) + dims_of(rest_of(ORDERS[t], phase)) + (rows, COLS), jnp.bfloat16)
            )
    scratch += [
        pltpu.VMEM((4, 4, 8, 128), jnp.float32),
        pltpu.SemaphoreType.DMA((70,)),
        pltpu.SemaphoreType.DMA((70,)),
    ]
    return pl.pallas_call(
        scatter_kernel,
        out_shape=[jax.ShapeDtypeStruct((r, width), jnp.float32) for r in (hid, hid, feat)]
        + [jax.ShapeDtypeStruct((8, 128), jnp.float32)],
        in_specs=[VM] * 3,
        out_specs=[VM] * 4,
        scratch_shapes=scratch,
        compiler_params=pltpu.CompilerParams(
            collective_id=4, has_side_effects=True, vmem_limit_bytes=48 * 1024 * 1024
        ),
        name="scatter_grads",
    )(pack, head, tile)


def gelu_tanh(values):
    return jax.nn.gelu(values, approximate=True)


def pad_blocks(values, size, axis):
    shape = values.shape
    blocks = shape[axis] // size
    cut = values.reshape(shape[:axis] + (blocks, size) + shape[axis + 1 :])
    pads = [(0, 0)] * cut.ndim
    pads[axis + 1] = (0, BLK - size)
    return jnp.pad(cut, pads).reshape(shape[:axis] + (blocks * BLK,) + shape[axis + 1 :])


def unit_rows(values):
    return values / jnp.sqrt(jnp.sum(values * values, -1, keepdims=True) + 1e-06)


def dot(a, b, da, db):
    return lax.dot_general(a, b, (((da,), (db,)), ((), ())), preferred_element_type=jnp.float32)


def local(
    teacher_in,
    teacher_gain,
    teacher_up,
    teacher_down,
    student_in,
    student_gain,
    student_up,
    student_down,
    student_head,
    student_proj,
    word_table,
    caption_ids,
    positive,
):
    grp_index = lax.axis_index("grp")
    dp_index = lax.axis_index("dp")
    n_grp = lax.axis_size("grp")
    n_dp = lax.axis_size("dp")
    shard = grp_index * n_dp + dp_index
    width = teacher_in.shape[1]
    feat = width // (n_grp * n_dp)
    hid = student_up.shape[1]
    own_rows = teacher_in.shape[0] // n_grp

    proj_cols = student_proj.shape[1]

    vocab_dev = word_table.shape[0]
    vocab_codes = shard * vocab_dev + jnp.arange(vocab_dev, dtype=jnp.int32)
    counts = jnp.sum(
        caption_ids[:, :, None] == vocab_codes[None, None, :], 1, dtype=jnp.float32
    ).astype(jnp.bfloat16)
    partial_words = jnp.dot(counts, word_table, preferred_element_type=jnp.float32) / CAP_LEN

    t_up, t_down, pack, s_head, s_proj, words = gather_weights(
        teacher_up,
        teacher_down,
        student_up.T,
        student_down,
        student_head.T,
        student_proj.T,
        partial_words,
    )
    caption_all = unit_rows(words)
    t_up = t_up.reshape(-1, t_up.shape[-1])
    t_down = t_down.reshape(-1, t_down.shape[-1])
    pack = pack.reshape(-1, pack.shape[-1])
    s_head = s_head.reshape(-1, s_head.shape[-1])
    s_proj = s_proj.reshape(-1, 2, proj_cols, s_proj.shape[-1])
    s_proj = jnp.concatenate([s_proj[:, 0], s_proj[:, 1]], -1)
    s_proj = s_proj.reshape(-1, s_proj.shape[-1])

    rows = lax.dynamic_slice_in_dim(student_in, grp_index * own_rows, own_rows, 0).astype(
        jnp.float32
    )
    center = rows - jnp.mean(rows, -1, keepdims=True)
    variance = jnp.mean(center * center, -1, keepdims=True)
    normed = (center * lax.rsqrt(variance + 1e-05) * student_gain).astype(jnp.bfloat16)
    is_up = (jnp.arange(pack.shape[0], dtype=jnp.int32) % (2 * hid) < hid)[None, :]
    gate_out = dot(normed, pack, 1, 1)
    act = jnp.where(is_up, gelu_tanh(gate_out), 0.0).astype(jnp.bfloat16)
    act = jnp.roll(act, hid, 1)
    student_out = rows + dot(act, pack, 1, 0)
    rounded = student_out.astype(jnp.bfloat16)
    pooled = (jnp.sum(student_out, 0, keepdims=True) / PATCHES).astype(jnp.bfloat16)
    pooled_all = gather_images(pooled)

    wide = t_up.shape[0]
    place = jnp.arange(width, dtype=jnp.int32)
    place = place // feat * BLK + place % feat
    spread_map = (place[:, None] == jnp.arange(wide, dtype=jnp.int32)[None, :]).astype(jnp.bfloat16)
    teacher_wide = dot(teacher_in, spread_map, 1, 0).astype(jnp.bfloat16)
    gain_wide = pad_blocks(teacher_gain, feat, 0)
    real = (jnp.arange(wide, dtype=jnp.int32) % BLK < feat)[None, :]

    def teacher(values):
        values = values.astype(jnp.float32)
        mean = jnp.sum(values, -1, keepdims=True) / width
        center = jnp.where(real, values - mean, 0.0)
        variance = jnp.sum(center * center, -1, keepdims=True) / width
        teacher_normed = (center * lax.rsqrt(variance + 1e-05) * gain_wide).astype(jnp.bfloat16)
        teacher_act = gelu_tanh(dot(teacher_normed, t_up, 1, 0)).astype(jnp.bfloat16)
        return dot(teacher_act, t_down, 1, 1).astype(jnp.bfloat16)

    teacher_own = lax.dynamic_slice_in_dim(teacher_wide, grp_index * own_rows, own_rows, 0)
    teacher_far = lax.dynamic_slice_in_dim(teacher_wide, (1 - grp_index) * own_rows, own_rows, 0)
    teacher_far, pooled_all = lax.optimization_barrier((teacher_far, pooled_all))
    branch_far = teacher(teacher_far)
    branch_got = lax.ppermute(branch_far, "grp", [(0, 1), (1, 0)])
    teacher_own, branch_far = lax.optimization_barrier((teacher_own, branch_far))
    branch_own = teacher(teacher_own)

    projected = dot(pooled_all, s_proj, 1, 1)
    proj_norm = jnp.sqrt(jnp.sum(projected * projected, -1, keepdims=True) + 1e-06)
    image_emb = projected / proj_norm
    scores = 100.0 * jnp.dot(image_emb, caption_all.T, precision=lax.Precision.HIGHEST)
    target_of = positive.reshape(n_dp, n_grp).T.reshape(-1)
    match = (target_of[:, None] == jnp.arange(scores.shape[1], dtype=jnp.int32)[None, :]).astype(
        jnp.float32
    )
    contrast = (
        jnp.sum(jax.nn.logsumexp(scores, 1))
        + jnp.sum(jax.nn.logsumexp(scores, 0))
        - 2.0 * jnp.sum(match * scores)
    )
    grad_scores = jax.nn.softmax(scores, 1) + jax.nn.softmax(scores, 0) - 2.0 * match
    grad_image = 100.0 * jnp.dot(grad_scores, caption_all, precision=lax.Precision.HIGHEST)
    grad_projected = (
        (grad_image - image_emb * jnp.sum(image_emb * grad_image, -1, keepdims=True)) / proj_norm
    ).astype(jnp.bfloat16)
    grad_columns = lax.dynamic_slice_in_dim(grad_projected, shard * proj_cols, proj_cols, 1)
    grad_proj = dot(grad_columns, pooled_all, 0, 0).T
    grad_projected_own = lax.dynamic_slice_in_dim(grad_projected, shard, 1, 0)
    grad_pooled = dot(grad_projected_own, s_proj, 1, 0)

    target = teacher_own.astype(jnp.float32) + (
        branch_own.astype(jnp.float32) + branch_got.astype(jnp.float32)
    )
    diff = dot(rounded, s_head, 1, 1) - target
    feature_part = jnp.sum(diff * diff) / width
    grad_pred = (2.0 * diff / width).astype(jnp.bfloat16)
    head_part = dot(grad_pred, rounded, 0, 0).astype(jnp.bfloat16)
    grad_out = (dot(grad_pred, s_head, 1, 0) + grad_pooled / PATCHES).astype(jnp.bfloat16)
    grad_act = jnp.roll(dot(grad_out, pack, 1, 1), -hid, 1)
    grad_gate = jax.vjp(gelu_tanh, gate_out)[1](grad_act)[0]
    grad_gate = jnp.where(is_up, grad_gate, 0.0).astype(jnp.bfloat16)
    pack_part = dot(
        jnp.concatenate([grad_gate, act], 0), jnp.concatenate([normed, grad_out], 0), 0, 0
    ).astype(jnp.bfloat16)
    grad_up, grad_down, grad_head, feature = scatter_grads(
        pack_part, head_part, hid, feat, feature_part
    )
    loss = (feature[0, 0] + contrast) / (positive.shape[0] * PATCHES)
    return (loss, grad_up.T, grad_down, grad_head.T, grad_proj)


def solution(mesh):
    placed = (
        P("dp", None),
        P(),
        P("dp", "grp"),
        P("dp", "grp"),
        P("dp", None),
        P(),
        P(None, ("grp", "dp")),
        P(("grp", "dp"), None),
        P(None, ("grp", "dp")),
        P(None, ("grp", "dp")),
        P(("grp", "dp"), None),
        P(),
        P(),
    )
    return jax.shard_map(
        local,
        mesh=mesh,
        in_specs=placed,
        out_specs=(
            P(),
            P(None, ("grp", "dp")),
            P(("grp", "dp"), None),
            P(None, ("grp", "dp")),
            P(None, ("grp", "dp")),
        ),
        check_vma=False,
    )
```

```python
import jax
import jax.numpy as jnp
from jax import lax
from jax.experimental import pallas as pl
from jax.experimental.pallas import tpu as pltpu
from jax.sharding import PartitionSpec as P

CAP_LEN = 77
PATCHES = 256
BLK = 16
MESH = pl.DeviceIdType.MESH
ANY = pl.BlockSpec(memory_space=pl.ANY)
VM = pl.BlockSpec(memory_space=pltpu.VMEM)


def coords():
    grp = lax.axis_index("grp")
    dp = lax.axis_index("dp")
    x_hi = (dp // 8) % 2
    return {
        "x": 2 * x_hi + grp,
        "y": dp // 16,
        "z": (dp // 2) % 4,
        "core": dp % 2,
    }


def device(at):
    return (at["x"] % 2, at["y"] * 16 + (at["x"] // 2) * 8 + at["z"] * 2 + at["core"])


def shifted(me, axis, step):
    if axis == "core":
        return {**me, "core": 1 - me["core"]}
    return {**me, axis: (me[axis] + step) % 4}


def enter(me, axes=("x", "y", "z"), steps=(1, 2, 3)):
    barrier = pltpu.get_barrier_semaphore()
    peers = [shifted(me, "core", 1)]
    for axis in axes:
        for step in steps:
            peers.append(shifted(me, axis, step))
    for peer in peers:
        pl.semaphore_signal(barrier, inc=1, device_id=device(peer), device_id_type=MESH)
    pl.semaphore_wait(barrier, len(peers))


class Copies:
    def __init__(self, send, recv):
        self.send, self.recv, self.count, self.open = send, recv, 0, []

    def start(self, src, dst, peer):
        copy = pltpu.make_async_remote_copy(
            src_ref=src,
            dst_ref=dst,
            send_sem=self.send.at[self.count],
            recv_sem=self.recv.at[self.count],
            device_id=device(peer),
            device_id_type=MESH,
        )
        self.count += 1
        copy.start()
        self.open.append(copy)
        return copy

    def finish(self):
        for copy in self.open:
            copy.wait_send()


def pick(ref, at, tail=()):
    x = at.get("x")
    whole = slice(None)
    index = (
        whole if x is None else x % 2,
        at.get("y", whole),
        whole if x is None else x // 2,
        at.get("z", whole),
    )
    if "core" in at:
        index += (at["core"],)
    return ref.at[index + tail]


def half(ref, side):
    if len(ref.shape) > 2:
        size = ref.shape[0] // 2
        return ref.at[pl.ds(side * size, size)]
    lanes = ref.shape[1] // 128
    cut = lanes // 2 * 128
    if side == 0:
        return ref.at[:, pl.ds(0, cut)]
    return ref.at[:, pl.ds(cut, ref.shape[1] - cut)]


def pick_teacher(ref, at, tail=()):
    whole = slice(None)
    index = (
        at.get("y", whole),
        at["x"] // 2,
        at.get("z", whole),
        at["core"],
    )
    return ref.at[index + tail]


def ring(copies, me, sibling, view, order, held, pushes):
    for axis in order:
        up, down, far = (shifted(me, axis, s) for s in (1, 3, 2))
        block = view(held)
        right = copies.start(block, block, up)
        left = copies.start(block, block, down)
        yield
        right.wait_recv()
        from_down = view({**held, axis: down[axis]})
        right2 = copies.start(half(from_down, 0), half(from_down, 0), up)
        pushes.append(copies.start(from_down, from_down, sibling))
        left.wait_recv()
        from_up = view({**held, axis: up[axis]})
        left2 = copies.start(half(from_up, 1), half(from_up, 1), down)
        pushes.append(copies.start(from_up, from_up, sibling))
        yield
        right2.wait_recv()
        left2.wait_recv()
        from_far = view({**held, axis: far[axis]})
        pushes.append(copies.start(from_far, from_far, sibling))
        held.pop(axis)


def student_chain(copies, me, sibling, ref, order):
    view = lambda at: pick(ref, at)
    own = view(me)
    pushes = [copies.start(own, own, sibling)]
    yield from ring(copies, me, sibling, view, order, dict(me), pushes)
    yield
    for copy in pushes:
        copy.wait_recv()


def teacher_chain(copies, me, sibling, ref, part, order, other):
    tail = (pl.ds(part * BLK, BLK),)
    view = lambda at: pick_teacher(ref, at, tail)
    pushes = []
    held = dict(me)
    if other:
        far = shifted(me, "x", 2)
        copy = copies.start(view(me), view(me), far)
        yield
        copy.wait_recv()
        held = dict(far)
    block = view(held)
    pushes.append(copies.start(block, block, sibling))
    yield from ring(copies, me, sibling, view, order, held, pushes)
    yield
    for copy in pushes:
        copy.wait_recv()


def caption_chain(copies, me, sibling, p_ref, out_ref, other, at_x, at_y, at_z):
    copy = copies.start(p_ref, other, sibling)
    yield
    copy.wait_recv()
    other[...] = other[...] + p_ref[...]

    def exchange(axis, source, slots):
        waits = []
        for step in (2, 1, 3):
            peer = shifted(me, axis, step)
            waits.append(copies.start(source.at[peer[axis]], slots.at[me[axis]], peer))
        slots[me[axis]] = source[me[axis]]
        return waits

    def total(waits, slots):
        for copy in waits:
            copy.wait_recv()
        return (slots[0] + slots[1]) + (slots[2] + slots[3])

    def spread(axis, view):
        return [copies.start(view, view, shifted(me, axis, step)) for step in (2, 1, 3)]

    waits = exchange("x", other, at_x)
    yield
    at_x[4] = total(waits, at_x)
    waits = exchange("y", at_x.at[4], at_y)
    yield
    at_y[4] = total(waits, at_y)
    waits = exchange("z", at_y.at[4], at_z)
    yield
    own = out_ref.at[me["x"], me["y"], me["z"]]
    own[...] = total(waits, at_z)
    for axis, view in (
        ("z", own),
        ("y", out_ref.at[me["x"], me["y"]]),
        ("x", out_ref.at[me["x"]]),
    ):
        waits = spread(axis, view)
        yield
        for copy in waits:
            copy.wait_recv()


def rows_padded(values, rows):
    short = rows - values.shape[0]
    if short == 0:
        return values
    return jnp.concatenate([values, jnp.zeros((short, values.shape[1]), values.dtype)], 0)


def image_chain(copies, me, out):
    held = dict(me)
    for axis in ("core", "z", "y", "x"):
        view = pick(out, held)
        steps = (1,) if axis == "core" else (2, 1, 3)
        waits = [copies.start(view, view, shifted(me, axis, step)) for step in steps]
        yield
        for copy in waits:
            copy.wait_recv()
        held.pop(axis)


def norm_rows(values, gain):
    center = values - jnp.mean(values, -1, keepdims=True)
    variance = jnp.mean(center * center, -1, keepdims=True)
    return (center * lax.rsqrt(variance + 1e-05) * gain).astype(jnp.bfloat16)


ORDER = (
    "PHQKUuvVeEnnnPHQnuUnvPHQ",
    "KuUVvePHQEuUVvdDePHQ",
    "KEUuVdUuvDVeEKdPvDVvV",
    "hehHEhhQKhdhhDhePEdePK",
    "sDHsEsQdssDsHsQsK",
)


def forward_kernel(
    t_up, t_down, up, down, head, proj, words, t_in, t_gain, s_in, s_gain,
    o_pack, o_head, o_proj, o_words, o_images, o_gate, o_act, o_normed, o_rounded, o_branch, o_wide,
    g_up, g_down, t_dense, t_normed, t_act, s_acc, other, at_x, at_y, at_z, send, recv,
):
    me = coords()
    grp = me["x"] % 2
    sibling = shifted(me, "core", 1)
    feat, hid = head.shape[0], up.shape[0]
    f32, bf16 = jnp.float32, jnp.bfloat16
    pick(o_pack, me)[...] = jnp.concatenate([up[...].astype(f32), down[...].astype(f32)], 0).astype(
        bf16
    )
    pick(o_head, me)[...] = rows_padded(head[...].astype(f32), BLK).astype(bf16)
    wide = proj[...].astype(f32)
    cut = wide.shape[1] // 2
    pick(o_proj, me)[...] = jnp.concatenate([wide[:, :cut], wide[:, cut:]], 0).astype(bf16)
    for source, out in ((t_up, g_up), (t_down, g_down)):
        values = source[...].astype(f32)
        for part in range(2):
            cut = values[part * feat : (part + 1) * feat]
            pick_teacher(out, me, (pl.ds(part * BLK, BLK),))[...] = rows_padded(cut, BLK).astype(
                bf16
            )
    enter(me)
    copies = Copies(send, recv)

    def teacher(ref, part, other_x):
        order = ("y", "z") if part == 0 else ("z", "y")
        return teacher_chain(copies, me, sibling, ref, part, order, other_x)

    chains = {
        "P": student_chain(copies, me, sibling, o_pack, ("y", "z", "x")),
        "H": student_chain(copies, me, sibling, o_head, ("z", "y", "x")),
        "Q": student_chain(copies, me, sibling, o_proj, ("z", "y", "x")),
        "K": caption_chain(copies, me, sibling, words, o_words, other, at_x, at_y, at_z),
    }
    for part in range(2):
        chains["uU"[part]] = teacher(g_up, part, False)
        chains["vV"[part]] = teacher(g_up, part, True)
        chains["dD"[part]] = teacher(g_down, part, False)
        chains["eE"[part]] = teacher(g_down, part, True)

    own_rows = o_gate.shape[0]
    own = pl.ds(pl.multiple_of(grp * own_rows, own_rows), own_rows)
    step = 256
    span = step // BLK * feat

    def student_norm():
        o_normed[...] = norm_rows(s_in[own, :].astype(f32), s_gain[...])

    def teacher_norm():
        def body(r, carry):
            rows = pl.ds(pl.multiple_of(r * 64, 64), 64)
            t_dense[rows, :] = norm_rows(t_in[rows, :].astype(f32), t_gain[...])
            return carry

        lax.fori_loop(0, t_in.shape[0] // 64, body, 0)

    def spread(j):
        base = span * j // 128 * 128
        size = -(-(span * j + span - base) // 128) * 128
        row = lax.broadcasted_iota(jnp.int32, (size, step), 0) + base
        col = lax.broadcasted_iota(jnp.int32, (size, step), 1)
        place = span * j + col // BLK * feat + col % BLK
        chosen = jnp.where((row == place) & (col % BLK < feat), 1.0, 0.0).astype(bf16)
        window = pl.ds(base, size)
        cols = pl.ds(j * step, step)
        t_normed[:, cols] = dot(t_dense[:, window], chosen, 1, 0).astype(bf16)
        o_wide[:, cols] = dot(t_in[own, window], chosen, 1, 0).astype(bf16)

    def hidden(j):
        cols = pl.ds(j * step, step)
        weights = g_up[:, :, :, :, :, cols].reshape(-1, step)
        t_act[:, cols] = gelu_tanh(dot(t_normed[...], weights, 1, 0)).astype(bf16)

    def branch(y):
        weights = g_down[y].reshape(-1, g_down.shape[-1])
        size = weights.shape[0]
        o_branch[:, pl.ds(y * size, size)] = dot(t_act[...], weights, 1, 1).astype(bf16)

    def student(n):
        weights = o_pack[n // 4, n % 4].reshape(-1, o_pack.shape[-1])
        size = weights.shape[0]
        cols = pl.ds(n * size, size)
        gate = dot(o_normed[...], weights, 1, 1)
        o_gate[:, cols] = gate
        is_up = lax.broadcasted_iota(jnp.int32, gate.shape, 1) % (2 * hid) < hid
        act = pltpu.roll(jnp.where(is_up, gelu_tanh(gate), 0.0), hid, 1).astype(bf16)
        o_act[:, cols] = act
        part = dot(act, weights, 1, 0)
        s_acc[...] = part + (s_in[own, :].astype(f32) if n == 0 else s_acc[...])

    def student_end():
        value = s_acc[...]
        o_rounded[...] = value.astype(bf16)
        pooled = jnp.sum(value, 0, keepdims=True) / PATCHES
        lanes = [pooled[:, i * 128 : (i + 1) * 128] for i in range(pooled.shape[1] // 128)]
        tile = rows_padded(jnp.concatenate(lanes, 0), 16)
        pick(o_images, me)[...] = tile.astype(bf16)

    work = {
        "n": [student_norm, teacher_norm]
        + [lambda k=k: [spread(j) for j in range(k, k + 3) if j < 8] for k in (0, 3, 6)],
        "h": [lambda j=j: hidden(j) for j in range(8)],
        "s": [lambda n=n: student(n) for n in range(8)],
    }
    for line in ORDER:
        for name in line:
            if name in work:
                work[name].pop(0)()
            else:
                next(chains[name], None)
    student_end()
    chains["I"] = image_chain(copies, me, o_images)
    for y in range(4):
        next(chains["I"], None)
        branch(y)
    for turn in range(8):
        for one in chains.values():
            next(one, None)
    copies.finish()


N_COPIES = 22 * 3 + 19 + 4 * 15 + 4 * 16 + 10


def forward(t_up, t_down, up, down, head, proj, words, t_in, t_gain, s_in, s_gain, own_rows):
    dtype = t_up.dtype
    width = up.shape[1]
    whole = (2, 4, 2, 4, 2)
    tiles = (4, 4, 4, 8, 128)
    rows = t_in.shape[0]
    gathered = (4, 2, 4, 2, 2 * BLK, t_up.shape[1])
    wide = 64 * 2 * BLK
    packed = 128 * (up.shape[0] + down.shape[0])
    shapes = [
        (whole + (up.shape[0] + down.shape[0], width), dtype),
        (whole + (BLK, width), dtype),
        (whole + (2 * proj.shape[0], width // 2), dtype),
        (tiles, jnp.float32),
        (whole + (16, 128), dtype),
        ((own_rows, packed), jnp.float32),
        ((own_rows, packed), dtype),
        ((own_rows, width), dtype),
        ((own_rows, width), dtype),
        ((rows, wide), dtype),
        ((own_rows, wide), dtype),
    ]
    out = pl.pallas_call(
        forward_kernel,
        out_shape=[jax.ShapeDtypeStruct(*s) for s in shapes],
        in_specs=[VM] * 11,
        out_specs=[VM] * 11,
        scratch_shapes=[
            pltpu.VMEM(gathered, dtype),
            pltpu.VMEM(gathered, dtype),
            pltpu.VMEM(t_in.shape, dtype),
            pltpu.VMEM((rows, wide), dtype),
            pltpu.VMEM((rows, t_up.shape[1]), dtype),
            pltpu.VMEM((own_rows, width), jnp.float32),
            pltpu.VMEM(tiles, jnp.float32),
            pltpu.VMEM((5, 4, 4, 8, 128), jnp.float32),
            pltpu.VMEM((5, 4, 8, 128), jnp.float32),
            pltpu.VMEM((4, 8, 128), jnp.float32),
            pltpu.SemaphoreType.DMA((N_COPIES,)),
            pltpu.SemaphoreType.DMA((N_COPIES,)),
        ],
        compiler_params=pltpu.CompilerParams(
            collective_id=1, has_side_effects=True, vmem_limit_bytes=56 * 1024 * 1024
        ),
        name="forward",
    )(
        t_up, t_down, up, down, head, proj,
        words.reshape(16, 8, 4, 128).transpose(0, 2, 1, 3).reshape(tiles),
        t_in, t_gain.reshape(1, -1), s_in, s_gain.reshape(1, -1),
    )
    out = list(out)
    out[3] = out[3].reshape(16, 4, 8, 128).transpose(0, 2, 1, 3).reshape(128, 512)
    out[4] = out[4].reshape(128, 16, 128)[:, : width // 128].reshape(128, width)
    return out


ORDERS = (("x", "y", "z"), ("y", "z", "x"), ("z", "x", "y"))
COLS = 256


def dims_of(axes):
    dims = []
    if "x" in axes:
        dims.append(2)
    if "y" in axes:
        dims.append(4)
    if "x" in axes:
        dims.append(2)
    if "z" in axes:
        dims.append(4)
    return tuple(dims)


def rest_of(order, phase):
    return [a for a in ("x", "y", "z") if a not in order[: phase + 1]]


def half_shape(order, phase, rows):
    shape = dims_of(rest_of(order, phase)) + (rows, COLS)
    if len(shape) == 2:
        return (rows, COLS // 2)
    return (shape[0] // 2,) + shape[1:]


def add_into(dst, srcs):
    lead = dst.shape[:-2]
    total = 1
    for size in lead:
        total *= size

    def one(index):
        value = dst[index].astype(jnp.float32)
        for src in srcs:
            value = value + src[index].astype(jnp.float32)
        dst[index] = value.astype(dst.dtype)

    if total == 1:
        one((0,) * len(lead) + (slice(None), slice(None)))
        return

    def body(n, carry):
        index = []
        rest = n
        for size in reversed(lead):
            index.append(rest % size)
            rest = rest // size
        one(tuple(reversed(index)))
        return carry

    lax.fori_loop(0, total, body, 0)


def rows_of(view, first, count, cols=None):
    lead = (slice(None),) * (len(view.shape) - 2)
    return view.at[lead + (pl.ds(first, count), slice(None) if cols is None else cols)]


def scatter_kernel(pack, head, s_ref, o_up, o_down, o_head, s_out, *refs):
    accs = refs[0:3]
    hold = refs[3:21]
    s_slots, send, recv = refs[21:]
    first = lambda t, p: hold[(t * 3 + p) * 2]
    second = lambda t, p: hold[(t * 3 + p) * 2 + 1]
    n_pack, n_head = pack.shape[-2], head.shape[-2]
    me = coords()
    enter(me)
    copies = Copies(send, recv)
    sibling = shifted(me, "core", 1)

    def sources(t, at):
        cols = pl.ds(t * COLS, COLS)
        return ((0, rows_of(pick(pack, at), 0, n_pack, cols)), (n_pack, rows_of(pick(head, at), 0, n_head, cols)))

    opening = {}
    for step in (2, 1, 3, 0):
        for t in range(3):
            axis = ORDERS[t][0]
            at = {axis: shifted(me, axis, step)[axis]}
            target = pick(accs[t], at)
            opening[t, step] = [
                copies.start(src, rows_of(target, row, src.shape[-2]), sibling)
                for row, src in sources(t, {**at, "core": sibling["core"]})
            ]
    s_wait = [copies.start(s_ref, s_slots.at[0, me["core"]], sibling)]
    s_slots[0, me["core"]] = s_ref[...]
    pending = [None] * 3
    held = [dict() for _ in range(3)]

    def opened(t, step):
        axis = ORDERS[t][0]
        at = {axis: shifted(me, axis, step)[axis]}
        for copy in opening[t, step]:
            copy.wait_recv()
        target = pick(accs[t], at)
        for row, src in sources(t, {**at, "core": me["core"]}):
            add_into(rows_of(target, row, src.shape[-2]), [src])

    def open_phase(t, phase):
        axis = ORDERS[t][phase]
        far = shifted(me, axis, 2)
        view = pick(accs[t], {**held[t], axis: far[axis]})
        up, down = shifted(me, axis, 1), shifted(me, axis, 3)
        return (
            copies.start(half(view, 0), first(t, phase).at[0], up),
            copies.start(half(view, 1), first(t, phase).at[1], down),
        )

    for t in range(3):
        opened(t, 2)
        pending[t] = open_phase(t, 0)
    for step in (1, 3, 0):
        for t in range(3):
            opened(t, step)
    for copy in s_wait:
        copy.wait_recv()
    s_value = s_slots[0, 0] + s_slots[0, 1]
    for phase in range(3):
        s_axis = ("x", "y", "z")[phase]
        s_slots[phase + 1, me[s_axis]] = s_value
        s_wait = []
        for step in (1, 2, 3):
            s_mine = s_slots.at[phase + 1, me[s_axis]]
            s_wait.append(copies.start(s_mine, s_mine, shifted(me, s_axis, step)))
        for t in range(3):
            axis = ORDERS[t][phase]
            up, down = shifted(me, axis, 1), shifted(me, axis, 3)
            to_up = pick(accs[t], {**held[t], axis: up[axis]})
            to_down = pick(accs[t], {**held[t], axis: down[axis]})
            pending[t][0].wait_recv()
            add_into(half(to_up, 0), [first(t, phase).at[0]])
            a = copies.start(to_up, second(t, phase).at[0], up)
            pending[t][1].wait_recv()
            add_into(half(to_down, 1), [first(t, phase).at[1]])
            b = copies.start(to_down, second(t, phase).at[1], down)
            pending[t] = (a, b)
        for t in range(3):
            axis = ORDERS[t][phase]
            pending[t][0].wait_recv()
            pending[t][1].wait_recv()
            held[t][axis] = me[axis]
            mine = pick(accs[t], held[t])
            if phase < 2:
                add_into(mine, [second(t, phase).at[0], second(t, phase).at[1]])
                pending[t] = open_phase(t, phase + 1)
            else:
                value = mine[...].astype(jnp.float32) + second(t, phase)[0].astype(jnp.float32)
                value = value + second(t, phase)[1].astype(jnp.float32)
                cols = pl.ds(t * COLS, COLS)
                hid = o_up.shape[0]
                o_up[:, cols] = value[:hid]
                o_down[:, cols] = value[hid:n_pack]
                o_head[:, cols] = value[n_pack : n_pack + o_head.shape[0]]
        for copy in s_wait:
            copy.wait_recv()
        s_value = (s_slots[phase + 1, 0] + s_slots[phase + 1, 1]) + (
            s_slots[phase + 1, 2] + s_slots[phase + 1, 3]
        )
    s_out[...] = s_value
    copies.finish()


def scatter_grads(pack, head, hid, feat, scalar):
    lead = (2, 4, 2, 4, 2)
    width = pack.shape[1]
    pack = pack.reshape(lead + (2 * hid, width))
    head = head.reshape(lead + (BLK, width))
    rows = 2 * hid + BLK
    tile = jnp.full((8, 128), scalar, jnp.float32)
    scratch = [pltpu.VMEM((2, 4, 2, 4, rows, COLS), jnp.bfloat16) for _ in range(3)]
    for t in range(3):
        for phase in range(3):
            scratch.append(pltpu.VMEM((2,) + half_shape(ORDERS[t], phase, rows), jnp.bfloat16))
            scratch.append(
                pltpu.VMEM((2,) + dims_of(rest_of(ORDERS[t], phase)) + (rows, COLS), jnp.bfloat16)
            )
    scratch += [
        pltpu.VMEM((4, 4, 8, 128), jnp.float32),
        pltpu.SemaphoreType.DMA((70,)),
        pltpu.SemaphoreType.DMA((70,)),
    ]
    return pl.pallas_call(
        scatter_kernel,
        out_shape=[jax.ShapeDtypeStruct((r, width), jnp.float32) for r in (hid, hid, feat)]
        + [jax.ShapeDtypeStruct((8, 128), jnp.float32)],
        in_specs=[VM] * 3,
        out_specs=[VM] * 4,
        scratch_shapes=scratch,
        compiler_params=pltpu.CompilerParams(
            collective_id=4, has_side_effects=True, vmem_limit_bytes=48 * 1024 * 1024
        ),
        name="scatter_grads",
    )(pack, head, tile)


def gelu_tanh(values):
    return jax.nn.gelu(values, approximate=True)


def unit_rows(values):
    return values / jnp.sqrt(jnp.sum(values * values, -1, keepdims=True) + 1e-06)


def dot(a, b, da, db):
    return lax.dot_general(a, b, (((da,), (db,)), ((), ())), preferred_element_type=jnp.float32)


def local(
    teacher_in,
    teacher_gain,
    teacher_up,
    teacher_down,
    student_in,
    student_gain,
    student_up,
    student_down,
    student_head,
    student_proj,
    word_table,
    caption_ids,
    positive,
):
    grp_index = lax.axis_index("grp")
    dp_index = lax.axis_index("dp")
    n_grp = lax.axis_size("grp")
    n_dp = lax.axis_size("dp")
    shard = grp_index * n_dp + dp_index
    width = teacher_in.shape[1]
    feat = width // (n_grp * n_dp)
    hid = student_up.shape[1]
    own_rows = teacher_in.shape[0] // n_grp

    proj_cols = student_proj.shape[1]

    vocab_dev = word_table.shape[0]
    vocab_codes = shard * vocab_dev + jnp.arange(vocab_dev, dtype=jnp.int32)
    counts = jnp.sum(
        caption_ids[:, :, None] == vocab_codes[None, None, :], 1, dtype=jnp.float32
    ).astype(jnp.bfloat16)
    partial_words = jnp.dot(counts, word_table, preferred_element_type=jnp.float32) / CAP_LEN

    (
        pack, s_head, s_proj, words, pooled_all,
        gate_out, act, normed, rounded, branch, teacher_own,
    ) = forward(
        teacher_up,
        teacher_down,
        student_up.T,
        student_down,
        student_head.T,
        student_proj.T,
        partial_words,
        teacher_in,
        teacher_gain,
        student_in,
        student_gain,
        own_rows,
    )
    caption_all = unit_rows(words)
    pack = pack.reshape(-1, pack.shape[-1])
    s_head = s_head.reshape(-1, s_head.shape[-1])
    s_proj = s_proj.reshape(-1, 2, proj_cols, s_proj.shape[-1])
    s_proj = jnp.concatenate([s_proj[:, 0], s_proj[:, 1]], -1)
    s_proj = s_proj.reshape(-1, s_proj.shape[-1])
    is_up = (jnp.arange(pack.shape[0], dtype=jnp.int32) % (2 * hid) < hid)[None, :]
    branch_far = lax.dynamic_slice_in_dim(branch, (1 - grp_index) * own_rows, own_rows, 0)
    branch_got = lax.ppermute(branch_far, "grp", [(0, 1), (1, 0)])
    branch_own = lax.dynamic_slice_in_dim(branch, grp_index * own_rows, own_rows, 0)

    projected = dot(pooled_all, s_proj, 1, 1)
    proj_norm = jnp.sqrt(jnp.sum(projected * projected, -1, keepdims=True) + 1e-06)
    image_emb = projected / proj_norm
    scores = 100.0 * jnp.dot(image_emb, caption_all.T, precision=lax.Precision.HIGHEST)
    target_of = positive.reshape(n_dp, n_grp).T.reshape(-1)
    match = (target_of[:, None] == jnp.arange(scores.shape[1], dtype=jnp.int32)[None, :]).astype(
        jnp.float32
    )
    contrast = (
        jnp.sum(jax.nn.logsumexp(scores, 1))
        + jnp.sum(jax.nn.logsumexp(scores, 0))
        - 2.0 * jnp.sum(match * scores)
    )
    grad_scores = jax.nn.softmax(scores, 1) + jax.nn.softmax(scores, 0) - 2.0 * match
    grad_image = 100.0 * jnp.dot(grad_scores, caption_all, precision=lax.Precision.HIGHEST)
    grad_projected = (
        (grad_image - image_emb * jnp.sum(image_emb * grad_image, -1, keepdims=True)) / proj_norm
    ).astype(jnp.bfloat16)
    grad_columns = lax.dynamic_slice_in_dim(grad_projected, shard * proj_cols, proj_cols, 1)
    grad_proj = dot(grad_columns, pooled_all, 0, 0).T
    grad_projected_own = lax.dynamic_slice_in_dim(grad_projected, shard, 1, 0)
    grad_pooled = dot(grad_projected_own, s_proj, 1, 0)

    target = teacher_own.astype(jnp.float32) + (
        branch_own.astype(jnp.float32) + branch_got.astype(jnp.float32)
    )
    diff = dot(rounded, s_head, 1, 1) - target
    feature_part = jnp.sum(diff * diff) / width
    grad_pred = (2.0 * diff / width).astype(jnp.bfloat16)
    head_part = dot(grad_pred, rounded, 0, 0).astype(jnp.bfloat16)
    grad_out = (dot(grad_pred, s_head, 1, 0) + grad_pooled / PATCHES).astype(jnp.bfloat16)
    grad_act = jnp.roll(dot(grad_out, pack, 1, 1), -hid, 1)
    grad_gate = jax.vjp(gelu_tanh, gate_out)[1](grad_act)[0]
    grad_gate = jnp.where(is_up, grad_gate, 0.0).astype(jnp.bfloat16)
    pack_part = dot(
        jnp.concatenate([grad_gate, act], 0), jnp.concatenate([normed, grad_out], 0), 0, 0
    ).astype(jnp.bfloat16)
    grad_up, grad_down, grad_head, feature = scatter_grads(
        pack_part, head_part, hid, feat, feature_part
    )
    loss = (feature[0, 0] + contrast) / (positive.shape[0] * PATCHES)
    return (loss, grad_up.T, grad_down, grad_head.T, grad_proj)


def solution(mesh):
    placed = (
        P("dp", None),
        P(),
        P("dp", "grp"),
        P("dp", "grp"),
        P("dp", None),
        P(),
        P(None, ("grp", "dp")),
        P(("grp", "dp"), None),
        P(None, ("grp", "dp")),
        P(None, ("grp", "dp")),
        P(("grp", "dp"), None),
        P(),
        P(),
    )
    return jax.shard_map(
        local,
        mesh=mesh,
        in_specs=placed,
        out_specs=(
            P(),
            P(None, ("grp", "dp")),
            P(("grp", "dp"), None),
            P(None, ("grp", "dp")),
            P(None, ("grp", "dp")),
        ),
        check_vma=False,
    )
```

```python
import jax
import jax.numpy as jnp
from jax import lax
from jax.experimental import pallas as pl
from jax.experimental.pallas import tpu as pltpu
from jax.sharding import PartitionSpec as P

CAP_LEN = 77
PATCHES = 256
BLK = 16
MESH = pl.DeviceIdType.MESH
VM = pl.BlockSpec(memory_space=pltpu.VMEM)


def coords():
    grp = lax.axis_index("grp")
    dp = lax.axis_index("dp")
    x_hi = (dp // 8) % 2
    return {
        "x": 2 * x_hi + grp,
        "y": dp // 16,
        "z": (dp // 2) % 4,
        "core": dp % 2,
    }


def device(at):
    return (at["x"] % 2, at["y"] * 16 + (at["x"] // 2) * 8 + at["z"] * 2 + at["core"])


def shifted(me, axis, step):
    if axis == "core":
        return {**me, "core": 1 - me["core"]}
    return {**me, axis: (me[axis] + step) % 4}


def enter(me, axes=("x", "y", "z"), steps=(1, 2, 3)):
    barrier = pltpu.get_barrier_semaphore()
    peers = [shifted(me, "core", 1)]
    for axis in axes:
        for step in steps:
            peers.append(shifted(me, axis, step))
    for peer in peers:
        pl.semaphore_signal(barrier, inc=1, device_id=device(peer), device_id_type=MESH)
    pl.semaphore_wait(barrier, len(peers))


class Copies:
    def __init__(self, send, recv):
        self.send, self.recv, self.count, self.open = send, recv, 0, []

    def start(self, src, dst, peer):
        copy = pltpu.make_async_remote_copy(
            src_ref=src,
            dst_ref=dst,
            send_sem=self.send.at[self.count],
            recv_sem=self.recv.at[self.count],
            device_id=device(peer),
            device_id_type=MESH,
        )
        self.count += 1
        copy.start()
        self.open.append(copy)
        return copy

    def finish(self):
        for copy in self.open:
            copy.wait_send()


def pick(ref, at, tail=()):
    x = at.get("x")
    whole = slice(None)
    index = (
        whole if x is None else x % 2,
        at.get("y", whole),
        whole if x is None else x // 2,
        at.get("z", whole),
    )
    if "core" in at:
        index += (at["core"],)
    return ref.at[index + tail]


def half(ref, side):
    if len(ref.shape) > 2:
        size = ref.shape[0] // 2
        return ref.at[pl.ds(side * size, size)]
    lanes = ref.shape[1] // 128
    cut = lanes // 2 * 128
    if side == 0:
        return ref.at[:, pl.ds(0, cut)]
    return ref.at[:, pl.ds(cut, ref.shape[1] - cut)]


def pick_teacher(ref, at, tail=()):
    whole = slice(None)
    index = (
        at.get("y", whole),
        at["x"] // 2,
        at.get("z", whole),
        at["core"],
    )
    return ref.at[index + tail]


def ring(copies, me, sibling, view, order, held, pushes):
    for axis in order:
        up, down, far = (shifted(me, axis, s) for s in (1, 3, 2))
        block = view(held)
        right = copies.start(block, block, up)
        left = copies.start(block, block, down)
        yield
        right.wait_recv()
        from_down = view({**held, axis: down[axis]})
        right2 = copies.start(half(from_down, 0), half(from_down, 0), up)
        pushes.append(copies.start(from_down, from_down, sibling))
        left.wait_recv()
        from_up = view({**held, axis: up[axis]})
        left2 = copies.start(half(from_up, 1), half(from_up, 1), down)
        pushes.append(copies.start(from_up, from_up, sibling))
        yield
        right2.wait_recv()
        left2.wait_recv()
        from_far = view({**held, axis: far[axis]})
        pushes.append(copies.start(from_far, from_far, sibling))
        held.pop(axis)


def student_chain(copies, me, sibling, ref, order):
    view = lambda at: pick(ref, at)
    own = view(me)
    pushes = [copies.start(own, own, sibling)]
    yield from ring(copies, me, sibling, view, order, dict(me), pushes)
    yield
    for copy in pushes:
        copy.wait_recv()


def teacher_chain(copies, me, sibling, ref, part, order, other):
    tail = (pl.ds(part * BLK, BLK),)
    view = lambda at: pick_teacher(ref, at, tail)
    pushes = []
    held = dict(me)
    if other:
        far = shifted(me, "x", 2)
        copy = copies.start(view(me), view(me), far)
        yield
        copy.wait_recv()
        held = dict(far)
    block = view(held)
    pushes.append(copies.start(block, block, sibling))
    yield from ring(copies, me, sibling, view, order, held, pushes)
    yield
    for copy in pushes:
        copy.wait_recv()


def caption_chain(copies, me, sibling, p_ref, out_ref, other, at_x, at_y, at_z):
    copy = copies.start(p_ref, other, sibling)
    yield
    copy.wait_recv()
    other[...] = other[...] + p_ref[...]

    def exchange(axis, source, slots):
        waits = []
        for step in (2, 1, 3):
            peer = shifted(me, axis, step)
            waits.append(copies.start(source.at[peer[axis]], slots.at[me[axis]], peer))
        slots[me[axis]] = source[me[axis]]
        return waits

    def total(waits, slots):
        for copy in waits:
            copy.wait_recv()
        return (slots[0] + slots[1]) + (slots[2] + slots[3])

    def spread(axis, view):
        return [copies.start(view, view, shifted(me, axis, step)) for step in (2, 1, 3)]

    waits = exchange("x", other, at_x)
    yield
    at_x[4] = total(waits, at_x)
    waits = exchange("y", at_x.at[4], at_y)
    yield
    at_y[4] = total(waits, at_y)
    waits = exchange("z", at_y.at[4], at_z)
    yield
    own = out_ref.at[me["x"], me["y"], me["z"]]
    own[...] = total(waits, at_z)
    for axis, view in (
        ("z", own),
        ("y", out_ref.at[me["x"], me["y"]]),
        ("x", out_ref.at[me["x"]]),
    ):
        waits = spread(axis, view)
        yield
        for copy in waits:
            copy.wait_recv()


def rows_padded(values, rows):
    short = rows - values.shape[0]
    if short == 0:
        return values
    return jnp.concatenate([values, jnp.zeros((short, values.shape[1]), values.dtype)], 0)


def image_chain(copies, me, out):
    held = dict(me)
    for axis in ("core", "x", "z", "y"):
        view = pick(out, held)
        steps = (1,) if axis == "core" else (2, 1, 3)
        waits = [copies.start(view, view, shifted(me, axis, step)) for step in steps]
        yield
        for copy in waits:
            copy.wait_recv()
        held.pop(axis)


def norm_rows(values, gain):
    center = values - jnp.mean(values, -1, keepdims=True)
    variance = jnp.mean(center * center, -1, keepdims=True)
    return (center * lax.rsqrt(variance + 1e-05) * gain).astype(jnp.bfloat16)


ORDERS = (("x", "y", "z"), ("y", "z", "x"), ("z", "x", "y"))
COLS = 256


def dims_of(axes):
    dims = []
    if "x" in axes:
        dims.append(2)
    if "y" in axes:
        dims.append(4)
    if "x" in axes:
        dims.append(2)
    if "z" in axes:
        dims.append(4)
    return tuple(dims)


def rest_of(order, phase):
    return [a for a in ("x", "y", "z") if a not in order[: phase + 1]]


def half_shape(order, phase, rows):
    shape = dims_of(rest_of(order, phase)) + (rows, COLS)
    if len(shape) == 2:
        return (rows, COLS // 2)
    return (shape[0] // 2,) + shape[1:]


def add_into(dst, srcs):
    lead = dst.shape[:-2]
    total = 1
    for size in lead:
        total *= size

    def one(index):
        value = dst[index].astype(jnp.float32)
        for src in srcs:
            value = value + src[index].astype(jnp.float32)
        dst[index] = value.astype(dst.dtype)

    if total == 1:
        one((0,) * len(lead) + (slice(None), slice(None)))
        return

    def body(n, carry):
        index = []
        rest = n
        for size in reversed(lead):
            index.append(rest % size)
            rest = rest // size
        one(tuple(reversed(index)))
        return carry

    lax.fori_loop(0, total, body, 0)


def rows_of(view, first, count, cols=None):
    lead = (slice(None),) * (len(view.shape) - 2)
    return view.at[lead + (pl.ds(first, count), slice(None) if cols is None else cols)]


class Scatter:
    def __init__(self, copies, me, sibling, pack, head, accs, hold):
        self.copies, self.me, self.sibling = copies, me, sibling
        self.pack, self.head, self.accs, self.hold = pack, head, accs, hold
        self.opening = {}

    def first(self, t, phase):
        return self.hold[(t * 3 + phase) * 2]

    def second(self, t, phase):
        return self.hold[(t * 3 + phase) * 2 + 1]

    def source(self, which, t, at):
        ref = self.head if which else self.pack
        return rows_of(pick(ref, at), 0, ref.shape[-2], pl.ds(t * COLS, COLS))

    def place(self, which, t, at):
        n_pack = self.pack.shape[-2]
        first, count = (n_pack, self.head.shape[-2]) if which else (0, n_pack)
        return rows_of(pick(self.accs[t], at), first, count)

    def at(self, t, step):
        axis = ORDERS[t][0]
        return {axis: shifted(self.me, axis, step)[axis]}

    def push(self, which):
        for step in (2, 1, 3, 0):
            for t in range(3):
                at = self.at(t, step)
                self.opening[which, t, step] = self.copies.start(
                    self.source(which, t, {**at, "core": self.sibling["core"]}),
                    self.place(which, t, at),
                    self.sibling,
                )

    def opened(self, t, step):
        at = self.at(t, step)
        for which in range(2):
            self.opening[which, t, step].wait_recv()
            add_into(
                self.place(which, t, at),
                [self.source(which, t, {**at, "core": self.me["core"]})],
            )

    def open_phase(self, t, phase, held):
        axis = ORDERS[t][phase]
        far = shifted(self.me, axis, 2)
        view = pick(self.accs[t], {**held, axis: far[axis]})
        up, down = shifted(self.me, axis, 1), shifted(self.me, axis, 3)
        return (
            self.copies.start(half(view, 0), self.first(t, phase).at[0], up),
            self.copies.start(half(view, 1), self.first(t, phase).at[1], down),
        )

    def finish(self, s_ref, s_slots, o_up, o_down, o_head):
        copies, me, accs = self.copies, self.me, self.accs
        n_pack = self.pack.shape[-2]
        s_wait = [copies.start(s_ref, s_slots.at[0, me["core"]], self.sibling)]
        s_slots[0, me["core"]] = s_ref[...]
        pending = [None] * 3
        held = [dict() for _ in range(3)]
        for t in range(3):
            self.opened(t, 2)
            pending[t] = self.open_phase(t, 0, held[t])
        for step in (1, 3, 0):
            for t in range(3):
                self.opened(t, step)
        for copy in s_wait:
            copy.wait_recv()
        s_value = s_slots[0, 0] + s_slots[0, 1]
        for phase in range(3):
            s_axis = ("x", "y", "z")[phase]
            s_slots[phase + 1, me[s_axis]] = s_value
            s_wait = []
            for step in (1, 2, 3):
                s_mine = s_slots.at[phase + 1, me[s_axis]]
                s_wait.append(copies.start(s_mine, s_mine, shifted(me, s_axis, step)))
            for t in range(3):
                axis = ORDERS[t][phase]
                up, down = shifted(me, axis, 1), shifted(me, axis, 3)
                to_up = pick(accs[t], {**held[t], axis: up[axis]})
                to_down = pick(accs[t], {**held[t], axis: down[axis]})
                pending[t][0].wait_recv()
                add_into(half(to_up, 0), [self.first(t, phase).at[0]])
                a = copies.start(to_up, self.second(t, phase).at[0], up)
                pending[t][1].wait_recv()
                add_into(half(to_down, 1), [self.first(t, phase).at[1]])
                b = copies.start(to_down, self.second(t, phase).at[1], down)
                pending[t] = (a, b)
            for t in range(3):
                axis = ORDERS[t][phase]
                pending[t][0].wait_recv()
                pending[t][1].wait_recv()
                held[t][axis] = me[axis]
                mine = pick(accs[t], held[t])
                got = self.second(t, phase)
                if phase < 2:
                    add_into(mine, [got.at[0], got.at[1]])
                    pending[t] = self.open_phase(t, phase + 1, held[t])
                else:
                    value = mine[...].astype(jnp.float32) + got[0].astype(jnp.float32)
                    value = value + got[1].astype(jnp.float32)
                    cols = pl.ds(t * COLS, COLS)
                    hid = o_up.shape[0]
                    o_up[:, cols] = value[:hid]
                    o_down[:, cols] = value[hid:n_pack]
                    o_head[:, cols] = value[n_pack : n_pack + o_head.shape[0]]
            for copy in s_wait:
                copy.wait_recv()
            s_value = (s_slots[phase + 1, 0] + s_slots[phase + 1, 1]) + (
                s_slots[phase + 1, 2] + s_slots[phase + 1, 3]
            )
        return s_value


def gelu_tanh(values):
    return jax.nn.gelu(values, approximate=True)


def dot(a, b, da, db):
    return lax.dot_general(a, b, (((da,), (db,)), ((), ())), preferred_element_type=jnp.float32)


def exact(a, b, da, db):
    return lax.dot_general(
        a, b, (((da,), (db,)), ((), ())),
        precision=lax.Precision.HIGHEST, preferred_element_type=jnp.float32,
    )


ORDER = (
    "PHQuKUvVDdnnPHKQnuUnPHQvdDnKuUeEVHQPveEuKUVPvEeuUVDdeKuUvEV",
    "PHQdDePKEvVPssdssvsVssKDsSIehdhhIHDEehhhhhE",
)


def step_kernel(
    t_up, t_down, up, down, head, proj, words, t_in, t_gain, s_in, s_gain, target_of,
    o_up, o_down, o_head, o_proj, o_loss,
    g_up, g_down, g_pack, g_head, g_proj, captions, images, gates, acts, normed, rounded, wide,
    far, near, got, t_normed, t_act, s_acc, grad_out, grad_img, d_pack, d_head, f_tile,
    other, at_x, at_y, at_z, s_slots, send, recv, *stores
):
    accs, hold = stores[:3], stores[3:]
    me = coords()
    grp = me["x"] % 2
    shard = grp * 64 + me["y"] * 16 + me["x"] // 2 * 8 + me["z"] * 2 + me["core"]
    sibling = shifted(me, "core", 1)
    feat, hid = head.shape[0], up.shape[0]
    width = t_in.shape[1]
    f32, bf16 = jnp.float32, jnp.bfloat16
    iota = lambda shape, axis: lax.broadcasted_iota(jnp.int32, shape, axis)

    pick(g_pack, me)[...] = jnp.concatenate([up[...].astype(f32), down[...].astype(f32)], 0).astype(
        bf16
    )
    pick(g_head, me)[...] = rows_padded(head[...].astype(f32), BLK).astype(bf16)
    values = proj[...].astype(f32)
    cut = values.shape[1] // 2
    pick(g_proj, me)[...] = jnp.concatenate([values[:, :cut], values[:, cut:]], 0).astype(bf16)
    for source, out in ((t_up, g_up), (t_down, g_down)):
        values = source[...].astype(f32)
        for part in range(2):
            cut = values[part * feat : (part + 1) * feat]
            pick_teacher(out, me, (pl.ds(part * BLK, BLK),))[...] = rows_padded(cut, BLK).astype(
                bf16
            )
    enter(me)
    copies = Copies(send, recv)

    def teacher(ref, part, other_x):
        order = ("y", "z") if part == 0 else ("z", "y")
        return teacher_chain(copies, me, sibling, ref, part, order, other_x)

    chains = {
        "P": student_chain(copies, me, sibling, g_pack, ("y", "z", "x")),
        "H": student_chain(copies, me, sibling, g_head, ("z", "y", "x")),
        "Q": student_chain(copies, me, sibling, g_proj, ("z", "y", "x")),
        "K": caption_chain(copies, me, sibling, words, captions, other, at_x, at_y, at_z),
        "I": image_chain(copies, me, images),
    }
    for part in range(2):
        chains["uU"[part]] = teacher(g_up, part, False)
        chains["vV"[part]] = teacher(g_up, part, True)
        chains["dD"[part]] = teacher(g_down, part, False)
        chains["eE"[part]] = teacher(g_down, part, True)

    own_rows = gates.shape[0]
    own = pl.ds(pl.multiple_of(grp * own_rows, own_rows), own_rows)
    partner_rows = pl.ds(pl.multiple_of((1 - grp) * own_rows, own_rows), own_rows)
    step = 256
    span = step // BLK * feat

    def student_norm():
        normed[...] = norm_rows(s_in[own, :].astype(f32), s_gain[...])

    def teacher_norm():
        def body(r, carry):
            rows = pl.ds(pl.multiple_of(r * 64, 64), 64)
            t_act[rows, pl.ds(0, width)] = norm_rows(t_in[rows, :].astype(f32), t_gain[...])
            return carry

        lax.fori_loop(0, t_in.shape[0] // 64, body, 0)

    def spread(j):
        base = span * j // 128 * 128
        size = -(-(span * j + span - base) // 128) * 128
        row = iota((size, step), 0) + base
        col = iota((size, step), 1)
        place = span * j + col // BLK * feat + col % BLK
        chosen = jnp.where((row == place) & (col % BLK < feat), 1.0, 0.0).astype(bf16)
        window = pl.ds(base, size)
        cols = pl.ds(j * step, step)
        t_normed[:, cols] = dot(t_act[:, window], chosen, 1, 0).astype(bf16)
        wide[:, cols] = dot(t_in[own, window], chosen, 1, 0).astype(bf16)

    def hidden(j):
        cols = pl.ds(j * step, step)
        weights = g_up[:, :, :, :, :, cols].reshape(-1, step)
        t_act[:, cols] = gelu_tanh(dot(t_normed[...], weights, 1, 0)).astype(bf16)

    def branch(y, rows, out):
        weights = g_down[y].reshape(-1, g_down.shape[-1])
        out[y] = dot(t_act[rows, :], weights, 1, 1).astype(bf16)

    def ups(shape):
        return iota(shape, 1) % (2 * hid) < hid

    def student(n):
        weights = g_pack[n // 4, n % 4].reshape(-1, g_pack.shape[-1])
        size = weights.shape[0]
        cols = pl.ds(n * size, size)
        gate = dot(normed[...], weights, 1, 1)
        gates[:, cols] = gate
        act = jnp.where(ups(gate.shape), gelu_tanh(gate), 0.0)
        act = pltpu.roll(act, hid, 1).astype(bf16)
        acts[:, cols] = act
        part = dot(act, weights, 1, 0)
        s_acc[...] = part + (s_in[own, :].astype(f32) if n == 0 else s_acc[...])

    def student_end():
        value = s_acc[...]
        rounded[...] = value.astype(bf16)
        pooled = jnp.sum(value, 0, keepdims=True) / PATCHES
        lanes = [pooled[:, i * 128 : (i + 1) * 128] for i in range(pooled.shape[1] // 128)]
        tile = rows_padded(jnp.concatenate(lanes, 0), 8)
        pick(images, me)[...] = tile.astype(bf16).astype(f32)

    work = {
        "n": [student_norm, teacher_norm]
        + [lambda k=k: [spread(j) for j in range(k, k + 3) if j < 8] for k in (0, 3, 6)],
        "h": [lambda j=j: hidden(j) for j in range(8)],
        "s": [lambda n=n: student(n) for n in range(8)],
        "S": [student_end],
    }
    for line in ORDER:
        for name in line:
            if name in work:
                work[name].pop(0)()
            else:
                next(chains[name], None)

    partner = {**me, "x": me["x"] + 1 - 2 * grp}
    exchange = []
    for y in range(4):
        branch(y, partner_rows, far)
        exchange.append(copies.start(far.at[y], got.at[y], partner))
    next(chains["I"], None)
    branch(0, own, near)
    branch(1, own, near)
    next(chains["I"], None)
    branch(2, own, near)
    branch(3, own, near)
    for turn in range(8):
        for one in chains.values():
            next(one, None)

    n_img = 128
    cols_dev = o_proj.shape[0]
    flat = images.reshape(n_img * 8, 128)
    pooled = [flat[pl.ds(i, n_img, stride=8), :] for i in range(g_proj.shape[-1] * 2 // 128)]
    pooled = jnp.concatenate(pooled, 1).astype(bf16)
    proj_all = g_proj[...].reshape(n_img * 8, g_proj.shape[-1])
    cut = g_proj.shape[-1]
    n_emb = proj_all.shape[0]
    low = dot(pooled[:, :cut], proj_all, 1, 1)
    high = dot(pooled[:, cut:], proj_all, 1, 1)
    real = iota(low.shape, 1) % 8 < cols_dev
    projected = jnp.where(real, low + pltpu.roll(high, n_emb - cols_dev, 1), 0.0)
    proj_norm = jnp.sqrt(jnp.sum(projected * projected, -1, keepdims=True) + 1e-06)
    image_emb = projected / proj_norm
    parts = [captions[:, :, z].reshape(n_img, 128) for z in range(4)]
    squares = sum(jnp.sum(part * part, -1, keepdims=True) for part in parts)
    size = 128 // cols_dev * 8
    row, col = iota((128, size), 0), iota((128, size), 1)
    chosen = jnp.where((row == col // 8 * cols_dev + col % 8) & (col % 8 < cols_dev), 1.0, 0.0)
    caption_all = jnp.concatenate([exact(part, chosen, 1, 0) for part in parts], 1)
    caption_all = caption_all / jnp.sqrt(squares + 1e-06)
    scores = 100.0 * exact(image_emb, caption_all, 1, 1)
    match = jnp.where(iota(scores.shape, 1) == target_of[...], 1.0, 0.0)

    def soft(axis):
        top = jnp.max(scores, axis, keepdims=True)
        powers = jnp.exp(scores - top)
        total = jnp.sum(powers, axis, keepdims=True)
        return jnp.sum(top + jnp.log(total)), powers / total

    log_rows, soft_rows = soft(1)
    log_cols, soft_cols = soft(0)
    contrast = log_rows + log_cols - 2.0 * jnp.sum(match * scores)
    grad_scores = soft_rows + soft_cols - 2.0 * match
    grad_image = 100.0 * exact(grad_scores, caption_all, 1, 0)
    inner = jnp.sum(image_emb * grad_image, -1, keepdims=True)
    grad_projected = ((grad_image - image_emb * inner) / proj_norm).astype(bf16)
    grad_img[...] = grad_projected.astype(f32)
    row, col = iota((n_emb, 128), 0), iota((n_emb, 128), 1)
    chosen = jnp.where((row == 8 * shard + col) & (col < cols_dev), 1.0, 0.0).astype(bf16)
    columns = dot(grad_projected, chosen, 1, 0).astype(bf16)
    o_proj[...] = dot(columns, pooled, 0, 0)[:cols_dev]
    mine = jnp.broadcast_to(grad_img[pl.ds(shard, 1), :], (8, n_emb))
    grad_low = dot(mine.astype(bf16), proj_all, 1, 0)
    grad_high = dot(pltpu.roll(mine, cols_dev, 1).astype(bf16), proj_all, 1, 0)
    grad_pooled = jnp.concatenate([grad_low, grad_high], 1)[:1]

    s_acc[...] = jnp.zeros_like(s_acc)
    f_tile[...] = jnp.zeros_like(f_tile)

    def head_block(n, carry):
        weights = g_head[n // 4, n % 4].reshape(step, -1)
        cols = pl.ds(pl.multiple_of(n * step, step), step)
        lanes = pl.ds(pl.multiple_of(n % 2 * step, step), step)
        pred = dot(rounded[...], weights, 1, 1)
        added = near[n // 2, :, lanes].astype(f32) + got[n // 2, :, lanes].astype(f32)
        diff = pred - (wide[:, cols].astype(f32) + added)
        f_tile[...] = f_tile[...] + jnp.sum(diff * diff)
        grad_pred = (2.0 * diff / width).astype(bf16)
        d_head[n // 4, n % 4] = (
            dot(grad_pred, rounded[...], 0, 0).astype(bf16).reshape(d_head.shape[2:])
        )
        s_acc[...] = s_acc[...] + dot(grad_pred, weights, 1, 0)
        return carry

    for y in range(4):
        exchange[y].wait_recv()
        lax.fori_loop(2 * y, 2 * y + 2, head_block, 0)

    scatter = Scatter(copies, me, sibling, d_pack, d_head, accs, hold)
    scatter.push(1)
    grad_out[...] = (s_acc[...] + grad_pooled / PATCHES).astype(bf16)

    def pack_block(n, carry):
        weights = g_pack[n // 4, n % 4].reshape(-1, g_pack.shape[-1])
        size = weights.shape[0]
        cols = pl.ds(pl.multiple_of(n * size, 128), size)
        grad_act = pltpu.roll(dot(grad_out[...], weights, 1, 1), size - hid, 1)
        grad_gate = jax.vjp(gelu_tanh, gates[:, cols])[1](grad_act)[0]
        grad_gate = jnp.where(ups(grad_gate.shape), grad_gate, 0.0).astype(bf16)
        total = dot(grad_gate, normed[...], 0, 0) + dot(acts[:, cols], grad_out[...], 0, 0)
        d_pack[n // 4, n % 4] = total.astype(bf16).reshape(d_pack.shape[2:])
        return carry

    lax.fori_loop(0, 8, pack_block, 0)
    scatter.push(0)
    f_tile[...] = f_tile[...] / width
    total = scatter.finish(f_tile, s_slots, o_up, o_down, o_head)
    o_loss[...] = (total + contrast) / (n_img * PATCHES)
    copies.finish()


N_COPIES = 22 * 3 + 19 + 4 * 15 + 4 * 16 + 10 + 4 + 70


def run_step(t_up, t_down, up, down, head, proj, words, t_in, t_gain, s_in, s_gain, target_of):
    bf16, f32 = t_up.dtype, jnp.float32
    rows, width = t_in.shape[0], up.shape[1]
    own_rows = rows // 2
    hid, feat = up.shape[0], head.shape[0]
    whole = (2, 4, 2, 4, 2)
    tiles = (4, 4, 4, 8, 128)
    teacher = (4, 2, 4, 2, 2 * BLK, t_up.shape[1])
    n_wide = 128 * BLK
    n_pack = 128 * 2 * hid
    vmem = pltpu.VMEM
    scratch = [
        vmem(teacher, bf16),
        vmem(teacher, bf16),
        vmem(whole + (2 * hid, width), bf16),
        vmem(whole + (BLK, width), bf16),
        vmem(whole + (2 * proj.shape[0], width // 2), bf16),
        vmem(tiles, f32),
        vmem(whole + (8, 128), f32),
        vmem((own_rows, n_pack), f32),
        vmem((own_rows, n_pack), bf16),
        vmem((own_rows, width), bf16),
        vmem((own_rows, width), bf16),
        vmem((own_rows, n_wide), bf16),
        vmem((4, own_rows, n_wide // 4), bf16),
        vmem((4, own_rows, n_wide // 4), bf16),
        vmem((4, own_rows, n_wide // 4), bf16),
        vmem((rows, n_wide), bf16),
        vmem((rows, t_up.shape[1]), bf16),
        vmem((own_rows, width), f32),
        vmem((own_rows, width), bf16),
        vmem((128, 128 * 8), f32),
        vmem(whole + (2 * hid, width), bf16),
        vmem(whole + (BLK, width), bf16),
        vmem((8, 128), f32),
        vmem(tiles, f32),
        vmem((5, 4, 4, 8, 128), f32),
        vmem((5, 4, 8, 128), f32),
        vmem((4, 8, 128), f32),
        vmem((4, 4, 8, 128), f32),
        pltpu.SemaphoreType.DMA((N_COPIES,)),
        pltpu.SemaphoreType.DMA((N_COPIES,)),
    ]
    block = 2 * hid + BLK
    scratch += [vmem((2, 4, 2, 4, block, COLS), bf16) for _ in range(3)]
    for t in range(3):
        for phase in range(3):
            scratch.append(vmem((2,) + half_shape(ORDERS[t], phase, block), bf16))
            scratch.append(vmem((2,) + dims_of(rest_of(ORDERS[t], phase)) + (block, COLS), bf16))
    return pl.pallas_call(
        step_kernel,
        out_shape=[
            jax.ShapeDtypeStruct(s, f32)
            for s in ((hid, width), (hid, width), (feat, width), (proj.shape[0], width), (8, 128))
        ],
        in_specs=[VM] * 12,
        out_specs=[VM] * 5,
        scratch_shapes=scratch,
        compiler_params=pltpu.CompilerParams(
            collective_id=1, has_side_effects=True, vmem_limit_bytes=67043328
        ),
        name="step",
    )(
        t_up, t_down, up, down, head, proj,
        words.reshape(16, 8, 4, 128).transpose(0, 2, 1, 3).reshape(tiles),
        t_in, t_gain.reshape(1, -1), s_in, s_gain.reshape(1, -1), target_of,
    )


def local(
    teacher_in,
    teacher_gain,
    teacher_up,
    teacher_down,
    student_in,
    student_gain,
    student_up,
    student_down,
    student_head,
    student_proj,
    word_table,
    caption_ids,
    positive,
):
    grp_index = lax.axis_index("grp")
    dp_index = lax.axis_index("dp")
    n_grp = lax.axis_size("grp")
    n_dp = lax.axis_size("dp")
    shard = grp_index * n_dp + dp_index
    vocab_dev = word_table.shape[0]
    vocab_codes = shard * vocab_dev + jnp.arange(vocab_dev, dtype=jnp.int32)
    counts = jnp.sum(
        caption_ids[:, :, None] == vocab_codes[None, None, :], 1, dtype=jnp.float32
    ).astype(jnp.bfloat16)
    partial_words = jnp.dot(counts, word_table, preferred_element_type=jnp.float32) / CAP_LEN

    target_of = positive.reshape(n_dp, n_grp).T.reshape(-1, 1)
    grad_up, grad_down, grad_head, grad_proj, loss = run_step(
        teacher_up,
        teacher_down,
        student_up.T,
        student_down,
        student_head.T,
        student_proj.T,
        partial_words,
        teacher_in,
        teacher_gain,
        student_in,
        student_gain,
        target_of,
    )
    return (loss[0, 0], grad_up.T, grad_down, grad_head.T, grad_proj.T)


def solution(mesh):
    placed = (
        P("dp", None),
        P(),
        P("dp", "grp"),
        P("dp", "grp"),
        P("dp", None),
        P(),
        P(None, ("grp", "dp")),
        P(("grp", "dp"), None),
        P(None, ("grp", "dp")),
        P(None, ("grp", "dp")),
        P(("grp", "dp"), None),
        P(),
        P(),
    )
    return jax.shard_map(
        local,
        mesh=mesh,
        in_specs=placed,
        out_specs=(
            P(),
            P(None, ("grp", "dp")),
            P(("grp", "dp"), None),
            P(None, ("grp", "dp")),
            P(None, ("grp", "dp")),
        ),
        check_vma=False,
    )
```

```python
import jax
import jax.numpy as jnp
from jax import lax
from jax.experimental import pallas as pl
from jax.experimental.pallas import tpu as pltpu
from jax.sharding import PartitionSpec as P

CAP_LEN = 77
PATCHES = 256
BLK = 16
MESH = pl.DeviceIdType.MESH
VM = pl.BlockSpec(memory_space=pltpu.VMEM)


def coords():
    grp = lax.axis_index("grp")
    dp = lax.axis_index("dp")
    x_hi = (dp // 8) % 2
    return {
        "x": 2 * x_hi + grp,
        "y": dp // 16,
        "z": (dp // 2) % 4,
        "core": dp % 2,
    }


def device(at):
    return (at["x"] % 2, at["y"] * 16 + (at["x"] // 2) * 8 + at["z"] * 2 + at["core"])


def shifted(me, axis, step):
    if axis == "core":
        return {**me, "core": 1 - me["core"]}
    return {**me, axis: (me[axis] + step) % 4}


def enter(me, axes=("x", "y", "z"), steps=(1, 2, 3)):
    barrier = pltpu.get_barrier_semaphore()
    peers = [shifted(me, "core", 1)]
    for axis in axes:
        for step in steps:
            peers.append(shifted(me, axis, step))
    for peer in peers:
        pl.semaphore_signal(barrier, inc=1, device_id=device(peer), device_id_type=MESH)
    pl.semaphore_wait(barrier, len(peers))


class Copies:
    def __init__(self, send, recv):
        self.send, self.recv, self.count, self.open = send, recv, 0, []

    def start(self, src, dst, peer):
        copy = pltpu.make_async_remote_copy(
            src_ref=src,
            dst_ref=dst,
            send_sem=self.send.at[self.count],
            recv_sem=self.recv.at[self.count],
            device_id=device(peer),
            device_id_type=MESH,
        )
        self.count += 1
        copy.start()
        self.open.append(copy)
        return copy

    def finish(self):
        for copy in self.open:
            copy.wait_send()


def pick(ref, at, tail=()):
    x = at.get("x")
    whole = slice(None)
    index = (
        whole if x is None else x % 2,
        at.get("y", whole),
        whole if x is None else x // 2,
        at.get("z", whole),
    )
    if "core" in at:
        index += (at["core"],)
    return ref.at[index + tail]


def half(ref, side):
    if len(ref.shape) > 2:
        size = ref.shape[0] // 2
        return ref.at[pl.ds(side * size, size)]
    lanes = ref.shape[1] // 128
    cut = lanes // 2 * 128
    if side == 0:
        return ref.at[:, pl.ds(0, cut)]
    return ref.at[:, pl.ds(cut, ref.shape[1] - cut)]


def pick_teacher(ref, at, tail=()):
    whole = slice(None)
    index = (
        at.get("y", whole),
        at["x"] // 2,
        at.get("z", whole),
        at["core"],
    )
    return ref.at[index + tail]


def ring(copies, me, sibling, view, order, held, pushes):
    for axis in order:
        up, down, far = (shifted(me, axis, s) for s in (1, 3, 2))
        block = view(held)
        right = copies.start(block, block, up)
        left = copies.start(block, block, down)
        yield
        right.wait_recv()
        from_down = view({**held, axis: down[axis]})
        right2 = copies.start(half(from_down, 0), half(from_down, 0), up)
        pushes.append(copies.start(from_down, from_down, sibling))
        left.wait_recv()
        from_up = view({**held, axis: up[axis]})
        left2 = copies.start(half(from_up, 1), half(from_up, 1), down)
        pushes.append(copies.start(from_up, from_up, sibling))
        yield
        right2.wait_recv()
        left2.wait_recv()
        from_far = view({**held, axis: far[axis]})
        pushes.append(copies.start(from_far, from_far, sibling))
        held.pop(axis)


def student_chain(copies, me, sibling, ref, order):
    view = lambda at: pick(ref, at)
    own = view(me)
    pushes = [copies.start(own, own, sibling)]
    yield from ring(copies, me, sibling, view, order, dict(me), pushes)
    yield
    for copy in pushes:
        copy.wait_recv()


def teacher_chain(copies, me, sibling, ref, part, order, other):
    tail = (pl.ds(part * BLK, BLK),)
    view = lambda at: pick_teacher(ref, at, tail)
    pushes = []
    held = dict(me)
    if other:
        far = shifted(me, "x", 2)
        copy = copies.start(view(me), view(me), far)
        yield
        copy.wait_recv()
        held = dict(far)
    block = view(held)
    pushes.append(copies.start(block, block, sibling))
    yield from ring(copies, me, sibling, view, order, held, pushes)
    yield
    for copy in pushes:
        copy.wait_recv()


def caption_chain(copies, me, sibling, p_ref, out_ref, other, at_x, at_y, at_z):
    copy = copies.start(p_ref, other, sibling)
    yield
    copy.wait_recv()
    other[...] = other[...] + p_ref[...]

    def exchange(axis, source, slots):
        waits = []
        for step in (2, 1, 3):
            peer = shifted(me, axis, step)
            waits.append(copies.start(source.at[peer[axis]], slots.at[me[axis]], peer))
        slots[me[axis]] = source[me[axis]]
        return waits

    def total(waits, slots):
        for copy in waits:
            copy.wait_recv()
        return (slots[0] + slots[1]) + (slots[2] + slots[3])

    def spread(axis, view):
        return [copies.start(view, view, shifted(me, axis, step)) for step in (2, 1, 3)]

    waits = exchange("x", other, at_x)
    yield
    at_x[4] = total(waits, at_x)
    waits = exchange("y", at_x.at[4], at_y)
    yield
    at_y[4] = total(waits, at_y)
    waits = exchange("z", at_y.at[4], at_z)
    yield
    own = out_ref.at[me["x"], me["y"], me["z"]]
    own[...] = total(waits, at_z)
    for axis, view in (
        ("z", own),
        ("y", out_ref.at[me["x"], me["y"]]),
        ("x", out_ref.at[me["x"]]),
    ):
        waits = spread(axis, view)
        yield
        for copy in waits:
            copy.wait_recv()


def rows_padded(values, rows):
    short = rows - values.shape[0]
    if short == 0:
        return values
    return jnp.concatenate([values, jnp.zeros((short, values.shape[1]), values.dtype)], 0)


def image_chain(copies, me, out):
    held = dict(me)
    for axis in ("core", "x", "z", "y"):
        view = pick(out, held)
        steps = (1,) if axis == "core" else (2, 1, 3)
        waits = [copies.start(view, view, shifted(me, axis, step)) for step in steps]
        yield
        for copy in waits:
            copy.wait_recv()
        held.pop(axis)


def norm_rows(values, gain):
    center = values - jnp.mean(values, -1, keepdims=True)
    variance = jnp.mean(center * center, -1, keepdims=True)
    return (center * lax.rsqrt(variance + 1e-05) * gain).astype(jnp.bfloat16)


ORDERS = (("x", "y", "z"), ("y", "z", "x"), ("z", "x", "y"))
COLS = 256


def dims_of(axes):
    dims = []
    if "x" in axes:
        dims.append(2)
    if "y" in axes:
        dims.append(4)
    if "x" in axes:
        dims.append(2)
    if "z" in axes:
        dims.append(4)
    return tuple(dims)


def rest_of(order, phase):
    return [a for a in ("x", "y", "z") if a not in order[: phase + 1]]


def half_shape(order, phase, rows):
    shape = dims_of(rest_of(order, phase)) + (rows, COLS)
    if len(shape) == 2:
        return (rows, COLS // 2)
    return (shape[0] // 2,) + shape[1:]


def add_into(dst, srcs):
    lead = dst.shape[:-2]
    total = 1
    for size in lead:
        total *= size

    def one(index):
        value = dst[index].astype(jnp.float32)
        for src in srcs:
            value = value + src[index].astype(jnp.float32)
        dst[index] = value.astype(dst.dtype)

    if total == 1:
        one((0,) * len(lead) + (slice(None), slice(None)))
        return

    def body(n, carry):
        index = []
        rest = n
        for size in reversed(lead):
            index.append(rest % size)
            rest = rest // size
        one(tuple(reversed(index)))
        return carry

    lax.fori_loop(0, total, body, 0)


def rows_of(view, first, count, cols=None):
    lead = (slice(None),) * (len(view.shape) - 2)
    return view.at[lead + (pl.ds(first, count), slice(None) if cols is None else cols)]


class Scatter:
    def __init__(self, copies, me, sibling, ref, accs, hold):
        self.copies, self.me, self.sibling = copies, me, sibling
        self.ref, self.accs, self.hold = ref, accs, hold
        self.opening = {}
        self.sums = [None] * 3

    def first(self, t, phase):
        return self.hold[t * 5 + phase * 2]

    def second(self, t, phase):
        return self.hold[t * 5 + (phase * 2 + 1 if phase < 2 else 4)]

    def source(self, t, at):
        return rows_of(pick(self.ref, at), 0, self.ref.shape[-2], pl.ds(t * COLS, COLS))

    def at(self, t, step):
        axis = ORDERS[t][0]
        return {axis: shifted(self.me, axis, step)[axis]}

    def push(self):
        for step in (2, 1, 3, 0):
            for t in range(3):
                at = self.at(t, step)
                self.opening[t, step] = self.copies.start(
                    self.source(t, {**at, "core": self.sibling["core"]}),
                    pick(self.accs[t], at),
                    self.sibling,
                )

    def opened(self, t, step):
        at = self.at(t, step)
        self.opening[t, step].wait_recv()
        add_into(pick(self.accs[t], at), [self.source(t, {**at, "core": self.me["core"]})])

    def open_phase(self, t, phase, held):
        axis = ORDERS[t][phase]
        if phase == 2:
            waits = []
            for step in (2, 1, 3):
                peer = shifted(self.me, axis, step)
                view = pick(self.accs[t], {**held, axis: peer[axis]})
                waits.append(self.copies.start(view, self.second(t, 2).at[step - 1], peer))
            return waits
        far = shifted(self.me, axis, 2)
        view = pick(self.accs[t], {**held, axis: far[axis]})
        up, down = shifted(self.me, axis, 1), shifted(self.me, axis, 3)
        return (
            self.copies.start(half(view, 0), self.first(t, phase).at[0], up),
            self.copies.start(half(view, 1), self.first(t, phase).at[1], down),
        )

    def chain(self):
        me, accs = self.me, self.accs
        pending = [None] * 3
        held = [dict() for _ in range(3)]
        for t in range(3):
            self.opened(t, 2)
            pending[t] = self.open_phase(t, 0, held[t])
        for step in (1, 3, 0):
            for t in range(3):
                self.opened(t, step)
        for phase in range(2):
            yield
            for t in range(3):
                axis = ORDERS[t][phase]
                up, down = shifted(me, axis, 1), shifted(me, axis, 3)
                to_up = pick(accs[t], {**held[t], axis: up[axis]})
                to_down = pick(accs[t], {**held[t], axis: down[axis]})
                pending[t][0].wait_recv()
                add_into(half(to_up, 0), [self.first(t, phase).at[0]])
                a = self.copies.start(to_up, self.second(t, phase).at[0], up)
                pending[t][1].wait_recv()
                add_into(half(to_down, 1), [self.first(t, phase).at[1]])
                b = self.copies.start(to_down, self.second(t, phase).at[1], down)
                pending[t] = (a, b)
            yield
            for t in range(3):
                axis = ORDERS[t][phase]
                pending[t][0].wait_recv()
                pending[t][1].wait_recv()
                held[t][axis] = me[axis]
                got = self.second(t, phase)
                add_into(pick(accs[t], held[t]), [got.at[0], got.at[1]])
                pending[t] = self.open_phase(t, phase + 1, held[t])
        yield
        for t in range(3):
            for copy in pending[t]:
                copy.wait_recv()
            axis = ORDERS[t][2]
            value = pick(accs[t], {**held[t], axis: me[axis]})[...].astype(jnp.float32)
            for slot in range(3):
                value = value + self.second(t, 2)[slot].astype(jnp.float32)
            self.sums[t] = value


def scalar_chain(copies, me, sibling, tile, slots):
    waits = [copies.start(tile, slots.at[0, me["core"]], sibling)]
    slots[0, me["core"]] = tile[...]
    value = None
    for phase, axis in enumerate(("x", "y", "z", None)):
        yield
        for copy in waits:
            copy.wait_recv()
        value = slots[phase, 0] + slots[phase, 1]
        if phase:
            value = value + (slots[phase, 2] + slots[phase, 3])
        if axis is None:
            break
        mine = slots.at[phase + 1, me[axis]]
        mine[...] = value
        waits = [copies.start(mine, mine, shifted(me, axis, step)) for step in (2, 1, 3)]
    slots[4, 0] = value


def gelu_tanh(values):
    return jax.nn.gelu(values, approximate=True)


def dot(a, b, da, db):
    return lax.dot_general(a, b, (((da,), (db,)), ((), ())), preferred_element_type=jnp.float32)


def exact(a, b, da, db):
    return lax.dot_general(
        a, b, (((da,), (db,)), ((), ())),
        precision=lax.Precision.HIGHEST, preferred_element_type=jnp.float32,
    )


ORDER = (
    "PuUVCKvDdHQnnnPnUuDnVdHPQKvUuEeVHvPQEeUuKVHvDdQPeEUuUKuVv",
    "HdEPDQevVKdHvVhEdhhehhKDhhhPDEQePssEssessHsQsSKHQ",
)


def step_kernel(
    t_up, t_down, up, down, head, proj, table, ids, t_in, t_gain, s_in, s_gain, positive,
    o_up, o_down, o_head, o_proj, o_loss,
    g_up, g_down, g_pack, g_head, g_proj, captions, images, gates, acts, normed, rounded, wide,
    far, near, got, t_normed, t_act, s_acc, grad_out, grad_img, d_pack, d_head, f_tile,
    words, other, at_x, at_y, at_z, s_slots, send, recv, *stores
):
    me = coords()
    grp = me["x"] % 2
    shard = grp * 64 + me["y"] * 16 + me["x"] // 2 * 8 + me["z"] * 2 + me["core"]
    sibling = shifted(me, "core", 1)
    feat, hid = head.shape[0], up.shape[0]
    width = t_in.shape[1]
    f32, bf16 = jnp.float32, jnp.bfloat16
    iota = lambda shape, axis: lax.broadcasted_iota(jnp.int32, shape, axis)

    pick(g_pack, me)[...] = jnp.concatenate([up[...].astype(f32), down[...].astype(f32)], 0).astype(
        bf16
    )
    pick(g_head, me)[...] = rows_padded(head[...].astype(f32), BLK).astype(bf16)
    values = proj[...].astype(f32)
    cut = values.shape[1] // 2
    pick(g_proj, me)[...] = jnp.concatenate([values[:, :cut], values[:, cut:]], 0).astype(bf16)
    for source, out in ((t_up, g_up), (t_down, g_down)):
        values = source[...].astype(f32)
        for part in range(2):
            cut = values[part * feat : (part + 1) * feat]
            pick_teacher(out, me, (pl.ds(part * BLK, BLK),))[...] = rows_padded(cut, BLK).astype(
                bf16
            )
    enter(me)
    copies = Copies(send, recv)

    def teacher(ref, part, other_x):
        order = ("y", "z") if part == 0 else ("z", "y")
        return teacher_chain(copies, me, sibling, ref, part, order, other_x)

    chains = {
        "P": student_chain(copies, me, sibling, g_pack, ("y", "z", "x")),
        "H": student_chain(copies, me, sibling, g_head, ("z", "y", "x")),
        "Q": student_chain(copies, me, sibling, g_proj, ("z", "y", "x")),
        "K": caption_chain(copies, me, sibling, words, captions, other, at_x, at_y, at_z),
        "I": image_chain(copies, me, images),
    }
    for part in range(2):
        chains["uU"[part]] = teacher(g_up, part, False)
        chains["vV"[part]] = teacher(g_up, part, True)
        chains["dD"[part]] = teacher(g_down, part, False)
        chains["eE"[part]] = teacher(g_down, part, True)

    own_rows = gates.shape[0]
    own = pl.ds(pl.multiple_of(grp * own_rows, own_rows), own_rows)
    partner_rows = pl.ds(pl.multiple_of((1 - grp) * own_rows, own_rows), own_rows)
    step = 256
    span = step // BLK * feat

    def count_words():
        vocab = table.shape[0]
        code = iota((vocab, ids.shape[1]), 0) + shard * vocab

        def body(j, counts):
            return counts + jnp.where(code == ids[pl.ds(j, 1), :], 1.0, 0.0)

        counts = lax.fori_loop(0, ids.shape[0], body, jnp.zeros(code.shape, f32))
        sums = dot(counts.astype(bf16), table[...], 0, 0) / CAP_LEN
        for z in range(4):
            words[:, :, z] = sums[:, z * 128 : (z + 1) * 128].reshape(4, 4, 8, 128)

    def student_norm():
        normed[...] = norm_rows(s_in[own, :].astype(f32), s_gain[...].reshape(1, -1))

    def teacher_norm():
        def body(r, carry):
            rows = pl.ds(pl.multiple_of(r * 64, 64), 64)
            t_act[rows, pl.ds(0, width)] = norm_rows(t_in[rows, :].astype(f32), t_gain[...].reshape(1, -1))
            return carry

        lax.fori_loop(0, t_in.shape[0] // 64, body, 0)

    def spread(j):
        base = span * j // 128 * 128
        size = -(-(span * j + span - base) // 128) * 128
        row = iota((size, step), 0) + base
        col = iota((size, step), 1)
        place = span * j + col // BLK * feat + col % BLK
        chosen = jnp.where((row == place) & (col % BLK < feat), 1.0, 0.0).astype(bf16)
        window = pl.ds(base, size)
        cols = pl.ds(j * step, step)
        t_normed[:, cols] = dot(t_act[:, window], chosen, 1, 0).astype(bf16)
        wide[:, cols] = dot(t_in[own, window], chosen, 1, 0).astype(bf16)

    def hidden(j):
        cols = pl.ds(j * step, step)
        weights = g_up[:, :, :, :, :, cols].reshape(-1, step)
        t_act[:, cols] = gelu_tanh(dot(t_normed[...], weights, 1, 0)).astype(bf16)

    def branch(y, rows, out):
        weights = g_down[y].reshape(-1, g_down.shape[-1])
        out[y] = dot(t_act[rows, :], weights, 1, 1).astype(bf16)

    def ups(shape):
        return iota(shape, 1) % (2 * hid) < hid

    def student(n):
        weights = g_pack[n // 4, n % 4].reshape(-1, g_pack.shape[-1])
        size = weights.shape[0]
        cols = pl.ds(n * size, size)
        gate = dot(normed[...], weights, 1, 1)
        gates[:, cols] = gate
        act = jnp.where(ups(gate.shape), gelu_tanh(gate), 0.0)
        act = pltpu.roll(act, hid, 1).astype(bf16)
        acts[:, cols] = act
        part = dot(act, weights, 1, 0)
        s_acc[...] = part + (s_in[own, :].astype(f32) if n == 0 else s_acc[...])

    def student_end():
        value = s_acc[...]
        rounded[...] = value.astype(bf16)
        pooled = jnp.sum(value, 0, keepdims=True) / PATCHES
        lanes = [pooled[:, i * 128 : (i + 1) * 128] for i in range(pooled.shape[1] // 128)]
        tile = rows_padded(jnp.concatenate(lanes, 0), 8)
        pick(images, me)[...] = tile.astype(bf16).astype(f32)

    work = {
        "C": [count_words],
        "n": [student_norm, teacher_norm]
        + [lambda k=k: [spread(j) for j in range(k, k + 3) if j < 8] for k in (0, 3, 6)],
        "h": [lambda j=j: hidden(j) for j in range(8)],
        "s": [lambda n=n: student(n) for n in range(8)],
        "S": [student_end],
    }
    for line in ORDER:
        for name in line:
            if name in work:
                work[name].pop(0)()
            else:
                next(chains[name], None)

    partner = {**me, "x": me["x"] + 1 - 2 * grp}
    exchange = []
    next(chains["I"], None)
    branch(0, partner_rows, far)
    branch(1, partner_rows, far)
    next(chains["I"], None)
    for y in range(4):
        if y > 1:
            branch(y, partner_rows, far)
        exchange.append(copies.start(far.at[y], got.at[y], partner))
    branch(0, own, near)
    branch(1, own, near)
    next(chains["I"], None)
    branch(2, own, near)
    branch(3, own, near)
    images_left = chains.pop("I")
    for turn in range(8):
        for one in chains.values():
            next(one, None)
    next(images_left, None)

    s_acc[...] = jnp.zeros_like(s_acc)
    f_tile[...] = jnp.zeros_like(f_tile)

    def head_block(n, carry):
        weights = g_head[n // 4, n % 4].reshape(step, -1)
        cols = pl.ds(pl.multiple_of(n * step, step), step)
        lanes = pl.ds(pl.multiple_of(n % 2 * step, step), step)
        pred = dot(rounded[...], weights, 1, 1)
        added = near[n // 2, :, lanes].astype(f32) + got[n // 2, :, lanes].astype(f32)
        diff = pred - (wide[:, cols].astype(f32) + added)
        f_tile[...] = f_tile[...] + jnp.sum(diff * diff)
        grad_pred = (2.0 * diff / width).astype(bf16)
        d_head[n // 4, n % 4] = (
            dot(grad_pred, rounded[...], 0, 0).astype(bf16).reshape(d_head.shape[2:])
        )
        s_acc[...] = s_acc[...] + dot(grad_pred, weights, 1, 0)
        return carry

    def head_blocks(y):
        exchange[y].wait_recv()
        lax.fori_loop(2 * y, 2 * y + 2, head_block, 0)

    head_blocks(0)
    head_blocks(1)
    next(images_left, None)

    n_img = 128
    cols_dev = o_proj.shape[0]
    flat = images.reshape(n_img * 8, 128)
    pooled = [flat[pl.ds(i, n_img, stride=8), :] for i in range(g_proj.shape[-1] * 2 // 128)]
    pooled = jnp.concatenate(pooled, 1).astype(bf16)
    proj_all = g_proj[...].reshape(n_img * 8, g_proj.shape[-1])
    cut = g_proj.shape[-1]
    n_emb = proj_all.shape[0]
    low = dot(pooled[:, :cut], proj_all, 1, 1)
    high = dot(pooled[:, cut:], proj_all, 1, 1)
    real = iota(low.shape, 1) % 8 < cols_dev
    projected = jnp.where(real, low + pltpu.roll(high, n_emb - cols_dev, 1), 0.0)
    proj_norm = jnp.sqrt(jnp.sum(projected * projected, -1, keepdims=True) + 1e-06)
    image_emb = projected / proj_norm
    parts = [captions[:, :, z].reshape(n_img, 128) for z in range(4)]
    squares = sum(jnp.sum(part * part, -1, keepdims=True) for part in parts)
    size = 128 // cols_dev * 8
    row, col = iota((128, size), 0), iota((128, size), 1)
    chosen = jnp.where((row == col // 8 * cols_dev + col % 8) & (col % 8 < cols_dev), 1.0, 0.0)
    caption_all = jnp.concatenate([exact(part, chosen, 1, 0) for part in parts], 1)
    caption_all = caption_all / jnp.sqrt(squares + 1e-06)
    scores = 100.0 * exact(image_emb, caption_all, 1, 1)
    target = jnp.broadcast_to(positive[...].reshape(1, -1), (n_img, n_img))
    match = jnp.where(iota(target.shape, 0) == target, 1.0, 0.0).astype(bf16)
    row = iota(target.shape, 0)
    chosen = jnp.where(iota(target.shape, 1) == row % 64 * 2 + row // 64, 1.0, 0.0).astype(bf16)
    match = dot(chosen, match, 1, 1)

    def soft(axis):
        top = jnp.max(scores, axis, keepdims=True)
        powers = jnp.exp(scores - top)
        total = jnp.sum(powers, axis, keepdims=True)
        return jnp.sum(top + jnp.log(total)), powers / total

    log_rows, soft_rows = soft(1)
    log_cols, soft_cols = soft(0)
    contrast = log_rows + log_cols - 2.0 * jnp.sum(match * scores)
    grad_scores = soft_rows + soft_cols - 2.0 * match
    grad_image = 100.0 * exact(grad_scores, caption_all, 1, 0)
    inner = jnp.sum(image_emb * grad_image, -1, keepdims=True)
    grad_projected = ((grad_image - image_emb * inner) / proj_norm).astype(bf16)
    grad_img[...] = grad_projected.astype(f32)
    row, col = iota((n_emb, 128), 0), iota((n_emb, 128), 1)
    chosen = jnp.where((row == 8 * shard + col) & (col < cols_dev), 1.0, 0.0).astype(bf16)
    columns = dot(grad_projected, chosen, 1, 0).astype(bf16)
    o_proj[...] = dot(columns, pooled, 0, 0)[:cols_dev]
    mine = jnp.broadcast_to(grad_img[pl.ds(shard, 1), :], (8, n_emb))
    grad_low = dot(mine.astype(bf16), proj_all, 1, 0)
    grad_high = dot(pltpu.roll(mine, cols_dev, 1).astype(bf16), proj_all, 1, 0)
    grad_pooled = jnp.concatenate([grad_low, grad_high], 1)[:1]

    head_blocks(2)
    head_blocks(3)
    n_store = len(stores) // 2
    head_sums = Scatter(copies, me, sibling, d_head, stores[:3], stores[3:n_store])
    pack_sums = Scatter(copies, me, sibling, d_pack, stores[n_store : n_store + 3], stores[n_store + 3 :])
    head_sums.push()
    f_tile[...] = f_tile[...] / width
    ends = [head_sums.chain(), scalar_chain(copies, me, sibling, f_tile, s_slots)]
    grad_out[...] = (s_acc[...] + grad_pooled / PATCHES).astype(bf16)

    def pack_block(n, carry):
        weights = g_pack[n // 4, n % 4].reshape(-1, g_pack.shape[-1])
        size = weights.shape[0]
        cols = pl.ds(pl.multiple_of(n * size, 128), size)
        grad_act = pltpu.roll(dot(grad_out[...], weights, 1, 1), size - hid, 1)
        grad_gate = jax.vjp(gelu_tanh, gates[:, cols])[1](grad_act)[0]
        grad_gate = jnp.where(ups(grad_gate.shape), grad_gate, 0.0).astype(bf16)
        total = dot(grad_gate, normed[...], 0, 0) + dot(acts[:, cols], grad_out[...], 0, 0)
        d_pack[n // 4, n % 4] = total.astype(bf16).reshape(d_pack.shape[2:])
        return carry

    for part in range(4):
        lax.fori_loop(2 * part, 2 * part + 2, pack_block, 0)
        for one in ends:
            next(one, None)
    pack_sums.push()
    ends.append(pack_sums.chain())
    for turn in range(8):
        for one in ends:
            next(one, None)
    for t in range(3):
        cols = pl.ds(t * COLS, COLS)
        o_up[:, cols] = pack_sums.sums[t][:hid]
        o_down[:, cols] = pack_sums.sums[t][hid:]
        o_head[:, cols] = head_sums.sums[t][:feat]
    o_loss[...] = (s_slots[4, 0] + contrast) / (n_img * PATCHES)
    copies.finish()


N_COPIES = 22 * 3 + 19 + 4 * 15 + 4 * 16 + 10 + 4 + 10 + 2 * 45


def run_step(t_up, t_down, up, down, head, proj, table, ids, t_in, t_gain, s_in, s_gain, positive):
    bf16, f32 = t_up.dtype, jnp.float32
    rows, width = t_in.shape[0], up.shape[1]
    own_rows = rows // 2
    hid, feat = up.shape[0], head.shape[0]
    whole = (2, 4, 2, 4, 2)
    tiles = (4, 4, 4, 8, 128)
    teacher = (4, 2, 4, 2, 2 * BLK, t_up.shape[1])
    n_wide = 128 * BLK
    n_pack = 128 * 2 * hid
    vmem = pltpu.VMEM
    scratch = [
        vmem(teacher, bf16),
        vmem(teacher, bf16),
        vmem(whole + (2 * hid, width), bf16),
        vmem(whole + (BLK, width), bf16),
        vmem(whole + (2 * proj.shape[0], width // 2), bf16),
        vmem(tiles, f32),
        vmem(whole + (8, 128), f32),
        vmem((own_rows, n_pack), f32),
        vmem((own_rows, n_pack), bf16),
        vmem((own_rows, width), bf16),
        vmem((own_rows, width), bf16),
        vmem((own_rows, n_wide), bf16),
        vmem((4, own_rows, n_wide // 4), bf16),
        vmem((4, own_rows, n_wide // 4), bf16),
        vmem((4, own_rows, n_wide // 4), bf16),
        vmem((rows, n_wide), bf16),
        vmem((rows, t_up.shape[1]), bf16),
        vmem((own_rows, width), f32),
        vmem((own_rows, width), bf16),
        vmem((128, 128 * 8), f32),
        vmem(whole + (2 * hid, width), bf16),
        vmem(whole + (BLK, width), bf16),
        vmem((8, 128), f32),
        vmem(tiles, f32),
        vmem(tiles, f32),
        vmem((5, 4, 4, 8, 128), f32),
        vmem((5, 4, 8, 128), f32),
        vmem((4, 8, 128), f32),
        vmem((5, 4, 8, 128), f32),
        pltpu.SemaphoreType.DMA((N_COPIES,)),
        pltpu.SemaphoreType.DMA((N_COPIES,)),
    ]
    for block in (BLK, 2 * hid):
        scratch += [vmem((2, 4, 2, 4, block, COLS), bf16) for _ in range(3)]
        for order in ORDERS:
            for phase in range(2):
                rest = dims_of(rest_of(order, phase)) + (block, COLS)
                scratch.append(vmem((2,) + half_shape(order, phase, block), bf16))
                scratch.append(vmem((2,) + rest, bf16))
            scratch.append(vmem((3, block, COLS), bf16))
    shapes = [(hid, width), (hid, width), (feat, width), (proj.shape[0], width), (8, 128)]
    shapes = [jax.ShapeDtypeStruct(shape, f32) for shape in shapes]
    out = pl.pallas_call(
        step_kernel,
        out_shape=shapes,
        in_specs=[VM] * 13,
        out_specs=[VM] * 5,
        scratch_shapes=scratch,
        compiler_params=pltpu.CompilerParams(
            collective_id=1, has_side_effects=True, vmem_limit_bytes=67043328
        ),
        name="step",
    )(t_up, t_down, up, down, head, proj, table, ids, t_in, t_gain, s_in, s_gain, positive)
    return pl.pallas_call(
        write_kernel,
        out_shape=shapes[:4] + [jax.ShapeDtypeStruct((1, 1), f32)],
        in_specs=[VM] * 5,
        out_specs=[VM] * 4 + [pl.BlockSpec(memory_space=pltpu.SMEM)],
        name="write",
    )(*out)


def write_kernel(*refs):
    for source, out in zip(refs[:4], refs[5:9]):
        out[...] = source[...]
    refs[9][0, 0] = jnp.max(refs[4][...])


def local(
    teacher_in,
    teacher_gain,
    teacher_up,
    teacher_down,
    student_in,
    student_gain,
    student_up,
    student_down,
    student_head,
    student_proj,
    word_table,
    caption_ids,
    positive,
):
    grad_up, grad_down, grad_head, grad_proj, loss = run_step(
        teacher_up,
        teacher_down,
        student_up.T,
        student_down,
        student_head.T,
        student_proj.T,
        word_table,
        caption_ids.T,
        teacher_in,
        teacher_gain,
        student_in,
        student_gain,
        positive,
    )
    return (loss[0, 0], grad_up.T, grad_down, grad_head.T, grad_proj.T)


def solution(mesh):
    placed = (
        P("dp", None),
        P(),
        P("dp", "grp"),
        P("dp", "grp"),
        P("dp", None),
        P(),
        P(None, ("grp", "dp")),
        P(("grp", "dp"), None),
        P(None, ("grp", "dp")),
        P(None, ("grp", "dp")),
        P(("grp", "dp"), None),
        P(),
        P(),
    )
    return jax.shard_map(
        local,
        mesh=mesh,
        in_specs=placed,
        out_specs=(
            P(),
            P(None, ("grp", "dp")),
            P(("grp", "dp"), None),
            P(None, ("grp", "dp")),
            P(None, ("grp", "dp")),
        ),
        check_vma=False,
    )
```

```python
import jax
import jax.numpy as jnp
from jax import lax
from jax.experimental import pallas as pl
from jax.experimental.pallas import tpu as pltpu
from jax.sharding import PartitionSpec as P

CAP_LEN = 77
PATCHES = 256
BLK = 16
MESH = pl.DeviceIdType.MESH
VM = pl.BlockSpec(memory_space=pltpu.VMEM)


def coords():
    grp = lax.axis_index("grp")
    dp = lax.axis_index("dp")
    x_hi = (dp // 8) % 2
    return {
        "x": 2 * x_hi + grp,
        "y": dp // 16,
        "z": (dp // 2) % 4,
        "core": dp % 2,
    }


def device(at):
    return (at["x"] % 2, at["y"] * 16 + (at["x"] // 2) * 8 + at["z"] * 2 + at["core"])


def shifted(me, axis, step):
    if axis == "core":
        return {**me, "core": 1 - me["core"]}
    return {**me, axis: (me[axis] + step) % 4}


def enter(me, axes=("x", "y", "z"), steps=(1, 2, 3)):
    barrier = pltpu.get_barrier_semaphore()
    peers = [shifted(me, "core", 1)]
    for axis in axes:
        for step in steps:
            peers.append(shifted(me, axis, step))
    for peer in peers:
        pl.semaphore_signal(barrier, inc=1, device_id=device(peer), device_id_type=MESH)
    return lambda: pl.semaphore_wait(barrier, len(peers))


class Copies:
    def __init__(self, send, recv):
        self.send, self.recv, self.count, self.open = send, recv, 0, []

    def start(self, src, dst, peer):
        copy = pltpu.make_async_remote_copy(
            src_ref=src,
            dst_ref=dst,
            send_sem=self.send.at[self.count],
            recv_sem=self.recv.at[self.count],
            device_id=device(peer),
            device_id_type=MESH,
        )
        self.count += 1
        copy.start()
        self.open.append(copy)
        return copy

    def finish(self):
        for copy in self.open:
            copy.wait_send()


def pick(ref, at, tail=()):
    x = at.get("x")
    whole = slice(None)
    index = (
        whole if x is None else x % 2,
        at.get("y", whole),
        whole if x is None else x // 2,
        at.get("z", whole),
    )
    if "core" in at:
        index += (at["core"],)
    return ref.at[index + tail]


def half(ref, side):
    if len(ref.shape) > 2:
        size = ref.shape[0] // 2
        return ref.at[pl.ds(side * size, size)]
    lanes = ref.shape[1] // 128
    cut = lanes // 2 * 128
    if side == 0:
        return ref.at[:, pl.ds(0, cut)]
    return ref.at[:, pl.ds(cut, ref.shape[1] - cut)]


def pick_teacher(ref, at, tail=()):
    whole = slice(None)
    index = (
        at.get("y", whole),
        at["x"] // 2,
        at.get("z", whole),
        at["core"],
    )
    return ref.at[index + tail]


def ring(copies, me, sibling, view, order, held, pushes):
    for axis in order:
        up, down, far = (shifted(me, axis, s) for s in (1, 3, 2))
        block = view(held)
        right = copies.start(block, block, up)
        left = copies.start(block, block, down)
        yield
        right.wait_recv()
        from_down = view({**held, axis: down[axis]})
        right2 = copies.start(half(from_down, 0), half(from_down, 0), up)
        pushes.append(copies.start(from_down, from_down, sibling))
        left.wait_recv()
        from_up = view({**held, axis: up[axis]})
        left2 = copies.start(half(from_up, 1), half(from_up, 1), down)
        pushes.append(copies.start(from_up, from_up, sibling))
        yield
        right2.wait_recv()
        left2.wait_recv()
        from_far = view({**held, axis: far[axis]})
        pushes.append(copies.start(from_far, from_far, sibling))
        held.pop(axis)


def student_chain(copies, me, sibling, ref, order):
    view = lambda at: pick(ref, at)
    own = view(me)
    pushes = [copies.start(own, own, sibling)]
    yield from ring(copies, me, sibling, view, order, dict(me), pushes)
    yield
    for copy in pushes:
        copy.wait_recv()


def teacher_chain(copies, me, sibling, ref, part, order, other):
    tail = (pl.ds(part * BLK, BLK),)
    view = lambda at: pick_teacher(ref, at, tail)
    pushes = []
    held = dict(me)
    if other:
        far = shifted(me, "x", 2)
        copy = copies.start(view(me), view(me), far)
        yield
        copy.wait_recv()
        held = dict(far)
    block = view(held)
    pushes.append(copies.start(block, block, sibling))
    yield from ring(copies, me, sibling, view, order, held, pushes)
    yield
    for copy in pushes:
        copy.wait_recv()


def caption_chain(copies, me, sibling, p_ref, out_ref, other, at_x, at_y, at_z):
    copy = copies.start(p_ref, other, sibling)
    yield
    copy.wait_recv()
    other[...] = other[...] + p_ref[...]

    def exchange(axis, source, slots):
        waits = []
        for step in (2, 1, 3):
            peer = shifted(me, axis, step)
            waits.append(copies.start(source.at[peer[axis]], slots.at[me[axis]], peer))
        slots[me[axis]] = source[me[axis]]
        return waits

    def total(waits, slots):
        for copy in waits:
            copy.wait_recv()
        return (slots[0] + slots[1]) + (slots[2] + slots[3])

    def spread(axis, view):
        return [copies.start(view, view, shifted(me, axis, step)) for step in (2, 1, 3)]

    waits = exchange("x", other, at_x)
    yield
    at_x[4] = total(waits, at_x)
    waits = exchange("y", at_x.at[4], at_y)
    yield
    at_y[4] = total(waits, at_y)
    waits = exchange("z", at_y.at[4], at_z)
    yield
    own = out_ref.at[me["x"], me["y"], me["z"]]
    own[...] = total(waits, at_z)
    for axis, view in (
        ("z", own),
        ("y", out_ref.at[me["x"], me["y"]]),
        ("x", out_ref.at[me["x"]]),
    ):
        waits = spread(axis, view)
        yield
        for copy in waits:
            copy.wait_recv()


def rows_padded(values, rows):
    short = rows - values.shape[0]
    if short == 0:
        return values
    return jnp.concatenate([values, jnp.zeros((short, values.shape[1]), values.dtype)], 0)


def image_chain(copies, me, out):
    held = dict(me)
    for axis in ("core", "x", "z", "y"):
        view = pick(out, held)
        steps = (1,) if axis == "core" else (2, 1, 3)
        waits = [copies.start(view, view, shifted(me, axis, step)) for step in steps]
        yield
        for copy in waits:
            copy.wait_recv()
        held.pop(axis)


def norm_rows(values, gain):
    center = values - jnp.mean(values, -1, keepdims=True)
    variance = jnp.mean(center * center, -1, keepdims=True)
    return (center * lax.rsqrt(variance + 1e-05) * gain).astype(jnp.bfloat16)


ORDERS = (("x", "y", "z"), ("y", "z", "x"), ("z", "x", "y"))
COLS = 256


def dims_of(axes):
    dims = []
    if "x" in axes:
        dims.append(2)
    if "y" in axes:
        dims.append(4)
    if "x" in axes:
        dims.append(2)
    if "z" in axes:
        dims.append(4)
    return tuple(dims)


def rest_of(order, phase):
    return [a for a in ("x", "y", "z") if a not in order[: phase + 1]]


def half_shape(order, phase, rows):
    shape = dims_of(rest_of(order, phase)) + (rows, COLS)
    if len(shape) == 2:
        return (rows, COLS // 2)
    return (shape[0] // 2,) + shape[1:]


def add_into(dst, srcs):
    lead = dst.shape[:-3]
    total = 1
    for size in lead:
        total *= size

    def one(index):
        value = dst[index].astype(jnp.float32)
        for src in srcs:
            value = value + src[index].astype(jnp.float32)
        dst[index] = value.astype(dst.dtype)

    if total == 1:
        one((0,) * len(lead) + (Ellipsis,))
        return

    def body(n, carry):
        index = []
        rest = n
        for size in reversed(lead):
            index.append(rest % size)
            rest = rest // size
        one(tuple(reversed(index)))
        return carry

    lax.fori_loop(0, total, body, 0)


def rows_of(view, first, count, cols=None):
    lead = (slice(None),) * (len(view.shape) - 2)
    return view.at[lead + (pl.ds(first, count), slice(None) if cols is None else cols)]


class Scatter:
    def __init__(self, copies, me, sibling, ref, accs, hold):
        self.copies, self.me, self.sibling = copies, me, sibling
        self.ref, self.accs, self.hold = ref, accs, hold
        self.opening = {}
        self.sums = [None] * 3

    def first(self, t):
        return self.hold[t * 4]

    def second(self, t, phase):
        return self.hold[t * 4 + 1 + phase]

    def source(self, t, at):
        return rows_of(pick(self.ref, at), 0, self.ref.shape[-2], pl.ds(t * COLS, COLS))

    def at(self, t, step):
        axis = ORDERS[t][0]
        return {axis: shifted(self.me, axis, step)[axis]}

    def push(self):
        for step in (2, 1, 3, 0):
            for t in range(3):
                at = self.at(t, step)
                self.opening[t, step] = self.copies.start(
                    self.source(t, {**at, "core": self.sibling["core"]}),
                    pick(self.accs[t], at),
                    self.sibling,
                )

    def opened(self, t, step):
        at = self.at(t, step)
        self.opening[t, step].wait_recv()
        add_into(pick(self.accs[t], at), [self.source(t, {**at, "core": self.me["core"]})])

    def open_phase(self, t, phase, held):
        axis = ORDERS[t][phase]
        if phase > 0:
            waits = []
            for step in (2, 1, 3):
                peer = shifted(self.me, axis, step)
                view = pick(self.accs[t], {**held, axis: peer[axis]})
                waits.append(self.copies.start(view, self.second(t, phase).at[step - 1], peer))
            return waits
        far = shifted(self.me, axis, 2)
        view = pick(self.accs[t], {**held, axis: far[axis]})
        up, down = shifted(self.me, axis, 1), shifted(self.me, axis, 3)
        return (
            self.copies.start(half(view, 0), self.first(t).at[0], up),
            self.copies.start(half(view, 1), self.first(t).at[1], down),
        )

    def chain(self):
        me, accs = self.me, self.accs
        pending = [None] * 3
        held = [dict() for _ in range(3)]
        for t in range(3):
            self.opened(t, 2)
            pending[t] = self.open_phase(t, 0, held[t])
        for step in (1, 3, 0):
            for t in range(3):
                self.opened(t, step)
        yield
        for t in range(3):
            axis = ORDERS[t][0]
            up, down = shifted(me, axis, 1), shifted(me, axis, 3)
            to_up = pick(accs[t], {axis: up[axis]})
            to_down = pick(accs[t], {axis: down[axis]})
            pending[t][0].wait_recv()
            add_into(half(to_up, 0), [self.first(t).at[0]])
            a = self.copies.start(to_up, self.second(t, 0).at[0], up)
            pending[t][1].wait_recv()
            add_into(half(to_down, 1), [self.first(t).at[1]])
            b = self.copies.start(to_down, self.second(t, 0).at[1], down)
            pending[t] = (a, b)
        for phase in range(2):
            yield
            for t in range(3):
                axis = ORDERS[t][phase]
                for copy in pending[t]:
                    copy.wait_recv()
                held[t][axis] = me[axis]
                got = self.second(t, phase)
                add_into(pick(accs[t], held[t]), [got.at[i] for i in range(len(pending[t]))])
                pending[t] = self.open_phase(t, phase + 1, held[t])
        yield
        for t in range(3):
            for copy in pending[t]:
                copy.wait_recv()
            axis = ORDERS[t][2]
            value = pick(accs[t], {**held[t], axis: me[axis]})[...].astype(jnp.float32)
            for slot in range(3):
                value = value + self.second(t, 2)[slot].astype(jnp.float32)
            self.sums[t] = value


def scalar_chain(copies, me, sibling, tile, slots):
    waits = [copies.start(tile, slots.at[0, me["core"]], sibling)]
    slots[0, me["core"]] = tile[...]
    value = None
    for phase, axis in enumerate(("x", "y", "z", None)):
        yield
        for copy in waits:
            copy.wait_recv()
        value = slots[phase, 0] + slots[phase, 1]
        if phase:
            value = value + (slots[phase, 2] + slots[phase, 3])
        if axis is None:
            break
        mine = slots.at[phase + 1, me[axis]]
        mine[...] = value
        waits = [copies.start(mine, mine, shifted(me, axis, step)) for step in (2, 1, 3)]
    slots[4, 0] = value


def gelu_tanh(values):
    return jax.nn.gelu(values, approximate=True)


def dot(a, b, da, db):
    return lax.dot_general(a, b, (((da,), (db,)), ((), ())), preferred_element_type=jnp.float32)


def exact(a, b, da, db):
    return lax.dot_general(
        a, b, (((da,), (db,)), ((), ())),
        precision=lax.Precision.HIGHEST, preferred_element_type=jnp.float32,
    )


ORDER = (
    "VHvPDQdEeCKnnnHPuUKnDQVdnHPvuUQVEKHePvUuQVEePvuUKVvEDedu",
    "UPQHuVvKUVEevhhhPhhhQhKhdDPssssEessssKESIedDIHQdDQ",
)


def step_kernel(
    t_up, t_down, up, down, head, proj, table, ids, t_in, t_gain, s_in, s_gain, positive,
    o_up, o_down, o_head, o_proj, o_loss,
    g_up, g_down, g_pack, g_head, g_proj, captions, images, gates, acts, normed, rounded, wide,
    far, near, got, t_normed, t_act, s_acc, grad_out, grad_img, d_pack, d_head, f_tile,
    words, other, at_x, at_y, at_z, s_slots, send, recv, *stores
):
    me = coords()
    grp = me["x"] % 2
    shard = grp * 64 + me["y"] * 16 + me["x"] // 2 * 8 + me["z"] * 2 + me["core"]
    sibling = shifted(me, "core", 1)
    feat, hid = head.shape[0], up.shape[0]
    width = t_in.shape[1]
    f32, bf16 = jnp.float32, jnp.bfloat16
    iota = lambda shape, axis: lax.broadcasted_iota(jnp.int32, shape, axis)

    entered = enter(me)
    pick(g_pack, me)[...] = jnp.concatenate([up[...].astype(f32), down[...].astype(f32)], 0).astype(
        bf16
    )
    pick(g_head, me)[...] = rows_padded(head[...].astype(f32), BLK).astype(bf16)
    values = proj[...].astype(f32)
    cut = values.shape[1] // 2
    pick(g_proj, me)[...] = jnp.concatenate([values[:, :cut], values[:, cut:]], 0).astype(bf16)
    for source, out in ((t_up, g_up), (t_down, g_down)):
        values = source[...].astype(f32)
        for part in range(2):
            cut = values[part * feat : (part + 1) * feat]
            pick_teacher(out, me, (pl.ds(part * BLK, BLK),))[...] = rows_padded(cut, BLK).astype(
                bf16
            )
    entered()
    copies = Copies(send, recv)

    def teacher(ref, part, other_x):
        order = ("y", "z") if part == 0 else ("z", "y")
        return teacher_chain(copies, me, sibling, ref, part, order, other_x)

    chains = {
        "P": student_chain(copies, me, sibling, g_pack, ("y", "z", "x")),
        "H": student_chain(copies, me, sibling, g_head, ("z", "y", "x")),
        "Q": student_chain(copies, me, sibling, g_proj, ("z", "y", "x")),
        "K": caption_chain(copies, me, sibling, words, captions, other, at_x, at_y, at_z),
        "I": image_chain(copies, me, images),
    }
    for part in range(2):
        chains["uU"[part]] = teacher(g_up, part, False)
        chains["vV"[part]] = teacher(g_up, part, True)
        chains["dD"[part]] = teacher(g_down, part, False)
        chains["eE"[part]] = teacher(g_down, part, True)

    own_rows = gates.shape[0]
    own = pl.ds(pl.multiple_of(grp * own_rows, own_rows), own_rows)
    partner_rows = pl.ds(pl.multiple_of((1 - grp) * own_rows, own_rows), own_rows)
    step = 256
    span = step // BLK * feat

    def count_words():
        vocab = table.shape[0]
        code = iota((vocab, ids.shape[1]), 0) + shard * vocab

        def body(j, counts):
            return counts + jnp.where(code == ids[pl.ds(j, 1), :], 1.0, 0.0)

        counts = lax.fori_loop(0, ids.shape[0], body, jnp.zeros(code.shape, f32))
        sums = dot(counts.astype(bf16), table[...], 0, 0) / CAP_LEN
        for z in range(4):
            words[:, :, z] = sums[:, z * 128 : (z + 1) * 128].reshape(4, 4, 8, 128)

    def student_norm():
        normed[...] = norm_rows(s_in[own, :].astype(f32), s_gain[...].reshape(1, -1))

    def teacher_norm():
        def body(r, carry):
            rows = pl.ds(pl.multiple_of(r * 64, 64), 64)
            t_act[rows, pl.ds(0, width)] = norm_rows(t_in[rows, :].astype(f32), t_gain[...].reshape(1, -1))
            return carry

        lax.fori_loop(0, t_in.shape[0] // 64, body, 0)

    def spread(j):
        base = span * j // 128 * 128
        size = -(-(span * j + span - base) // 128) * 128
        row = iota((size, step), 0) + base
        col = iota((size, step), 1)
        place = span * j + col // BLK * feat + col % BLK
        chosen = jnp.where((row == place) & (col % BLK < feat), 1.0, 0.0).astype(bf16)
        window = pl.ds(base, size)
        cols = pl.ds(j * step, step)
        t_normed[:, cols] = dot(t_act[:, window], chosen, 1, 0).astype(bf16)
        wide[:, cols] = dot(t_in[own, window], chosen, 1, 0).astype(bf16)

    def hidden(j):
        cols = pl.ds(j * step, step)
        weights = g_up[:, :, :, :, :, cols].reshape(-1, step)
        t_act[:, cols] = gelu_tanh(dot(t_normed[...], weights, 1, 0)).astype(bf16)

    def branch(y, rows, out):
        weights = g_down[y].reshape(-1, g_down.shape[-1])
        out[y] = dot(t_act[rows, :], weights, 1, 1).astype(bf16)

    def ups(shape):
        return iota(shape, 1) % (2 * hid) < hid

    def student(n):
        weights = g_pack[n // 4, n % 4].reshape(-1, g_pack.shape[-1])
        size = weights.shape[0]
        cols = pl.ds(n * size, size)
        gate = dot(normed[...], weights, 1, 1)
        gates[:, cols] = gate
        act = jnp.where(ups(gate.shape), gelu_tanh(gate), 0.0)
        act = pltpu.roll(act, hid, 1).astype(bf16)
        acts[:, cols] = act
        part = dot(act, weights, 1, 0)
        s_acc[...] = part + (s_in[own, :].astype(f32) if n == 0 else s_acc[...])

    def student_end():
        value = s_acc[...]
        rounded[...] = value.astype(bf16)
        pooled = jnp.sum(value, 0, keepdims=True) / PATCHES
        lanes = [pooled[:, i * 128 : (i + 1) * 128] for i in range(pooled.shape[1] // 128)]
        tile = rows_padded(jnp.concatenate(lanes, 0), 8)
        pick(images, me)[...] = tile.astype(bf16).astype(f32)

    work = {
        "C": [count_words],
        "n": [student_norm, teacher_norm]
        + [lambda k=k: [spread(j) for j in range(k, k + 3) if j < 8] for k in (0, 3, 6)],
        "h": [lambda j=j: hidden(j) for j in range(8)],
        "s": [lambda n=n: student(n) for n in range(8)],
        "S": [student_end],
    }
    for line in ORDER:
        for name in line:
            if name in work:
                work[name].pop(0)()
            else:
                next(chains[name], None)

    partner = {**me, "x": me["x"] + 1 - 2 * grp}
    exchange = []
    for y in range(4):
        branch(y, partner_rows, far)
        exchange.append(copies.start(far.at[y], got.at[y], partner))
    next(chains["I"], None)
    branch(0, own, near)
    branch(1, own, near)
    branch(2, own, near)
    next(chains["I"], None)
    branch(3, own, near)
    images_left = chains.pop("I")
    for turn in range(8):
        for one in chains.values():
            next(one, None)

    s_acc[...] = jnp.zeros_like(s_acc)
    f_tile[...] = jnp.zeros_like(f_tile)

    def head_block(n, carry):
        weights = g_head[n // 4, n % 4].reshape(step, -1)
        cols = pl.ds(pl.multiple_of(n * step, step), step)
        lanes = pl.ds(pl.multiple_of(n % 2 * step, step), step)
        pred = dot(rounded[...], weights, 1, 1)
        added = near[n // 2, :, lanes].astype(f32) + got[n // 2, :, lanes].astype(f32)
        diff = pred - (wide[:, cols].astype(f32) + added)
        f_tile[...] = f_tile[...] + jnp.sum(diff * diff)
        grad_pred = (2.0 * diff / width).astype(bf16)
        d_head[n // 4, n % 4] = (
            dot(grad_pred, rounded[...], 0, 0).astype(bf16).reshape(d_head.shape[2:])
        )
        s_acc[...] = s_acc[...] + dot(grad_pred, weights, 1, 0)
        return carry

    def head_blocks(y):
        exchange[y].wait_recv()
        lax.fori_loop(2 * y, 2 * y + 2, head_block, 0)

    head_blocks(0)
    next(images_left, None)

    n_img = 128
    cols_dev = o_proj.shape[0]
    flat = images.reshape(n_img * 8, 128)
    pooled = [flat[pl.ds(i, n_img, stride=8), :] for i in range(g_proj.shape[-1] * 2 // 128)]
    pooled = jnp.concatenate(pooled, 1).astype(bf16)
    proj_all = g_proj[...].reshape(n_img * 8, g_proj.shape[-1])
    cut = g_proj.shape[-1]
    n_emb = proj_all.shape[0]
    low = dot(pooled[:, :cut], proj_all, 1, 1)
    high = dot(pooled[:, cut:], proj_all, 1, 1)
    real = iota(low.shape, 1) % 8 < cols_dev
    projected = jnp.where(real, low + pltpu.roll(high, n_emb - cols_dev, 1), 0.0)
    proj_norm = jnp.sqrt(jnp.sum(projected * projected, -1, keepdims=True) + 1e-06)
    image_emb = projected / proj_norm
    parts = [captions[:, :, z].reshape(n_img, 128) for z in range(4)]
    squares = sum(jnp.sum(part * part, -1, keepdims=True) for part in parts)
    size = 128 // cols_dev * 8
    row, col = iota((128, size), 0), iota((128, size), 1)
    chosen = jnp.where((row == col // 8 * cols_dev + col % 8) & (col % 8 < cols_dev), 1.0, 0.0)
    caption_all = jnp.concatenate([exact(part, chosen, 1, 0) for part in parts], 1)
    caption_all = caption_all / jnp.sqrt(squares + 1e-06)
    scores = 100.0 * exact(image_emb, caption_all, 1, 1)
    target = jnp.broadcast_to(positive[...].reshape(1, -1), (n_img, n_img))
    match = jnp.where(iota(target.shape, 0) == target, 1.0, 0.0).astype(bf16)
    row = iota(target.shape, 0)
    chosen = jnp.where(iota(target.shape, 1) == row % 64 * 2 + row // 64, 1.0, 0.0).astype(bf16)
    match = dot(chosen, match, 1, 1)

    def soft(axis):
        top = jnp.max(scores, axis, keepdims=True)
        powers = jnp.exp(scores - top)
        total = jnp.sum(powers, axis, keepdims=True)
        return jnp.sum(top + jnp.log(total)), powers / total

    log_rows, soft_rows = soft(1)
    log_cols, soft_cols = soft(0)
    contrast = log_rows + log_cols - 2.0 * jnp.sum(match * scores)
    grad_scores = soft_rows + soft_cols - 2.0 * match
    grad_image = 100.0 * exact(grad_scores, caption_all, 1, 0)
    inner = jnp.sum(image_emb * grad_image, -1, keepdims=True)
    grad_projected = ((grad_image - image_emb * inner) / proj_norm).astype(bf16)
    grad_img[...] = grad_projected.astype(f32)
    row, col = iota((n_emb, 128), 0), iota((n_emb, 128), 1)
    chosen = jnp.where((row == 8 * shard + col) & (col < cols_dev), 1.0, 0.0).astype(bf16)
    columns = dot(grad_projected, chosen, 1, 0).astype(bf16)
    o_proj[...] = dot(columns, pooled, 0, 0)[:cols_dev]
    mine = jnp.broadcast_to(grad_img[pl.ds(shard, 1), :], (8, n_emb))
    grad_low = dot(mine.astype(bf16), proj_all, 1, 0)
    grad_high = dot(pltpu.roll(mine, cols_dev, 1).astype(bf16), proj_all, 1, 0)
    grad_pooled = jnp.concatenate([grad_low, grad_high], 1)[:1]

    for y in range(1, 4):
        head_blocks(y)
    n_store = len(stores) // 2
    head_sums = Scatter(copies, me, sibling, d_head, stores[:3], stores[3:n_store])
    pack_sums = Scatter(copies, me, sibling, d_pack, stores[n_store : n_store + 3], stores[n_store + 3 :])
    head_sums.push()
    f_tile[...] = f_tile[...] / width
    ends = [head_sums.chain(), scalar_chain(copies, me, sibling, f_tile, s_slots)]
    grad_out[...] = (s_acc[...] + grad_pooled / PATCHES).astype(bf16)

    def pack_block(n, carry):
        weights = g_pack[n // 4, n % 4].reshape(-1, g_pack.shape[-1])
        size = weights.shape[0]
        cols = pl.ds(pl.multiple_of(n * size, 128), size)
        grad_act = pltpu.roll(dot(grad_out[...], weights, 1, 1), size - hid, 1)
        grad_gate = jax.vjp(gelu_tanh, gates[:, cols])[1](grad_act)[0]
        grad_gate = jnp.where(ups(grad_gate.shape), grad_gate, 0.0).astype(bf16)
        total = dot(grad_gate, normed[...], 0, 0) + dot(acts[:, cols], grad_out[...], 0, 0)
        d_pack[n // 4, n % 4] = total.astype(bf16).reshape(d_pack.shape[2:])
        return carry

    for part in range(4):
        lax.fori_loop(2 * part, 2 * part + 2, pack_block, 0)
        for one in ends:
            next(one, None)
    pack_sums.push()
    ends.append(pack_sums.chain())
    for turn in range(8):
        for one in ends:
            next(one, None)
    for t in range(3):
        cols = pl.ds(t * COLS, COLS)
        o_up[:, cols] = pack_sums.sums[t][:hid]
        o_down[:, cols] = pack_sums.sums[t][hid:]
        o_head[:, cols] = head_sums.sums[t][:feat]
    o_loss[...] = (s_slots[4, 0] + contrast) / (n_img * PATCHES)
    copies.finish()


N_COPIES = 22 * 3 + 19 + 4 * 15 + 4 * 16 + 10 + 4 + 10 + 2 * 42


def run_step(t_up, t_down, up, down, head, proj, table, ids, t_in, t_gain, s_in, s_gain, positive):
    bf16, f32 = t_up.dtype, jnp.float32
    rows, width = t_in.shape[0], up.shape[1]
    own_rows = rows // 2
    hid, feat = up.shape[0], head.shape[0]
    whole = (2, 4, 2, 4, 2)
    tiles = (4, 4, 4, 8, 128)
    teacher = (4, 2, 4, 2, 2 * BLK, t_up.shape[1])
    n_wide = 128 * BLK
    n_pack = 128 * 2 * hid
    vmem = pltpu.VMEM
    scratch = [
        vmem(teacher, bf16),
        vmem(teacher, bf16),
        vmem(whole + (2 * hid, width), bf16),
        vmem(whole + (BLK, width), bf16),
        vmem(whole + (2 * proj.shape[0], width // 2), bf16),
        vmem(tiles, f32),
        vmem(whole + (8, 128), f32),
        vmem((own_rows, n_pack), f32),
        vmem((own_rows, n_pack), bf16),
        vmem((own_rows, width), bf16),
        vmem((own_rows, width), bf16),
        vmem((own_rows, n_wide), bf16),
        vmem((4, own_rows, n_wide // 4), bf16),
        vmem((4, own_rows, n_wide // 4), bf16),
        vmem((4, own_rows, n_wide // 4), bf16),
        vmem((rows, n_wide), bf16),
        vmem((rows, t_up.shape[1]), bf16),
        vmem((own_rows, width), f32),
        vmem((own_rows, width), bf16),
        vmem((128, 128 * 8), f32),
        vmem(whole + (2 * hid, width), bf16),
        vmem(whole + (BLK, width), bf16),
        vmem((8, 128), f32),
        vmem(tiles, f32),
        vmem(tiles, f32),
        vmem((5, 4, 4, 8, 128), f32),
        vmem((5, 4, 8, 128), f32),
        vmem((4, 8, 128), f32),
        vmem((5, 4, 8, 128), f32),
        pltpu.SemaphoreType.DMA((N_COPIES,)),
        pltpu.SemaphoreType.DMA((N_COPIES,)),
    ]
    for block in (BLK, 2 * hid):
        scratch += [vmem((2, 4, 2, 4, block, COLS), bf16) for _ in range(3)]
        for order in ORDERS:
            scratch.append(vmem((2,) + half_shape(order, 0, block), bf16))
            for phase, count in enumerate((2, 3, 3)):
                rest = dims_of(rest_of(order, phase)) + (block, COLS)
                scratch.append(vmem((count,) + rest, bf16))
    shapes = [(hid, width), (hid, width), (feat, width), (proj.shape[0], width), (8, 128)]
    shapes = [jax.ShapeDtypeStruct(shape, f32) for shape in shapes]
    out = pl.pallas_call(
        step_kernel,
        out_shape=shapes,
        in_specs=[VM] * 13,
        out_specs=[VM] * 5,
        scratch_shapes=scratch,
        compiler_params=pltpu.CompilerParams(
            collective_id=1, has_side_effects=True, vmem_limit_bytes=67043328
        ),
        name="step",
    )(t_up, t_down, up, down, head, proj, table, ids, t_in, t_gain, s_in, s_gain, positive)
    return pl.pallas_call(
        write_kernel,
        out_shape=shapes[:4] + [jax.ShapeDtypeStruct((1, 1), f32)],
        in_specs=[VM] * 5,
        out_specs=[VM] * 4 + [pl.BlockSpec(memory_space=pltpu.SMEM)],
        name="write",
    )(*out)


def write_kernel(*refs):
    for source, out in zip(refs[:4], refs[5:9]):
        out[...] = source[...]
    refs[9][0, 0] = jnp.max(refs[4][...])


def local(
    teacher_in,
    teacher_gain,
    teacher_up,
    teacher_down,
    student_in,
    student_gain,
    student_up,
    student_down,
    student_head,
    student_proj,
    word_table,
    caption_ids,
    positive,
):
    grad_up, grad_down, grad_head, grad_proj, loss = run_step(
        teacher_up,
        teacher_down,
        student_up.T,
        student_down,
        student_head.T,
        student_proj.T,
        word_table,
        caption_ids.T,
        teacher_in,
        teacher_gain,
        student_in,
        student_gain,
        positive,
    )
    return (loss[0, 0], grad_up.T, grad_down, grad_head.T, grad_proj.T)


def solution(mesh):
    placed = (
        P("dp", None),
        P(),
        P("dp", "grp"),
        P("dp", "grp"),
        P("dp", None),
        P(),
        P(None, ("grp", "dp")),
        P(("grp", "dp"), None),
        P(None, ("grp", "dp")),
        P(None, ("grp", "dp")),
        P(("grp", "dp"), None),
        P(),
        P(),
    )
    return jax.shard_map(
        local,
        mesh=mesh,
        in_specs=placed,
        out_specs=(
            P(),
            P(None, ("grp", "dp")),
            P(("grp", "dp"), None),
            P(None, ("grp", "dp")),
            P(None, ("grp", "dp")),
        ),
        check_vma=False,
    )
```

```python
import jax
import jax.numpy as jnp
from jax import lax
from jax.experimental import pallas as pl
from jax.experimental.pallas import tpu as pltpu
from jax.sharding import PartitionSpec as P

CAP_LEN = 77
PATCHES = 256
BLK = 16
MESH = pl.DeviceIdType.MESH
VM = pl.BlockSpec(memory_space=pltpu.VMEM)


def coords():
    grp = lax.axis_index("grp")
    dp = lax.axis_index("dp")
    x_hi = (dp // 8) % 2
    return {
        "x": 2 * x_hi + grp,
        "y": dp // 16,
        "z": (dp // 2) % 4,
        "core": dp % 2,
    }


def device(at):
    return (at["x"] % 2, at["y"] * 16 + (at["x"] // 2) * 8 + at["z"] * 2 + at["core"])


def shifted(me, axis, step):
    if axis == "core":
        return {**me, "core": 1 - me["core"]}
    return {**me, axis: (me[axis] + step) % 4}


def enter(me, axes=("x", "y", "z"), steps=(1, 2, 3)):
    barrier = pltpu.get_barrier_semaphore()
    peers = [shifted(me, "core", 1)]
    for axis in axes:
        for step in steps:
            peers.append(shifted(me, axis, step))
    for peer in peers:
        pl.semaphore_signal(barrier, inc=1, device_id=device(peer), device_id_type=MESH)
    return lambda: pl.semaphore_wait(barrier, len(peers))


class Copies:
    def __init__(self, send, recv):
        self.send, self.recv, self.count, self.open = send, recv, 0, []

    def start(self, src, dst, peer):
        copy = pltpu.make_async_remote_copy(
            src_ref=src,
            dst_ref=dst,
            send_sem=self.send.at[self.count],
            recv_sem=self.recv.at[self.count],
            device_id=device(peer),
            device_id_type=MESH,
        )
        self.count += 1
        copy.start()
        self.open.append(copy)
        return copy

    def finish(self):
        for copy in self.open:
            copy.wait_send()


def pick(ref, at, tail=()):
    x = at.get("x")
    whole = slice(None)
    index = (
        whole if x is None else x % 2,
        at.get("y", whole),
        whole if x is None else x // 2,
        at.get("z", whole),
    )
    if "core" in at:
        index += (at["core"],)
    return ref.at[index + tail]


def half(ref, side):
    if len(ref.shape) > 2:
        size = ref.shape[0] // 2
        return ref.at[pl.ds(side * size, size)]
    lanes = ref.shape[1] // 128
    cut = lanes // 2 * 128
    if side == 0:
        return ref.at[:, pl.ds(0, cut)]
    return ref.at[:, pl.ds(cut, ref.shape[1] - cut)]


def pick_teacher(ref, at, tail=()):
    whole = slice(None)
    index = (
        at.get("y", whole),
        at["x"] // 2,
        at.get("z", whole),
        at["core"],
    )
    return ref.at[index + tail]


def ring(copies, me, sibling, view, order, held, pushes):
    for axis in order:
        up, down, far = (shifted(me, axis, s) for s in (1, 3, 2))
        block = view(held)
        right = copies.start(block, block, up)
        left = copies.start(block, block, down)
        yield
        right.wait_recv()
        from_down = view({**held, axis: down[axis]})
        right2 = copies.start(half(from_down, 0), half(from_down, 0), up)
        pushes.append(copies.start(from_down, from_down, sibling))
        left.wait_recv()
        from_up = view({**held, axis: up[axis]})
        left2 = copies.start(half(from_up, 1), half(from_up, 1), down)
        pushes.append(copies.start(from_up, from_up, sibling))
        yield
        right2.wait_recv()
        left2.wait_recv()
        from_far = view({**held, axis: far[axis]})
        pushes.append(copies.start(from_far, from_far, sibling))
        held.pop(axis)


def student_chain(copies, me, sibling, ref, order):
    view = lambda at: pick(ref, at)
    own = view(me)
    pushes = [copies.start(own, own, sibling)]
    yield from ring(copies, me, sibling, view, order, dict(me), pushes)
    yield
    for copy in pushes:
        copy.wait_recv()


def teacher_chain(copies, me, sibling, ref, part, order, other):
    tail = (pl.ds(part * BLK, BLK),)
    view = lambda at: pick_teacher(ref, at, tail)
    pushes = []
    held = dict(me)
    if other:
        far = shifted(me, "x", 2)
        copy = copies.start(view(me), view(me), far)
        yield
        copy.wait_recv()
        held = dict(far)
    block = view(held)
    pushes.append(copies.start(block, block, sibling))
    yield from ring(copies, me, sibling, view, order, held, pushes)
    yield
    for copy in pushes:
        copy.wait_recv()


def caption_chain(copies, me, sibling, p_ref, out_ref, other, at_x, at_y, at_z):
    copy = copies.start(p_ref, other, sibling)
    yield
    copy.wait_recv()
    other[...] = other[...] + p_ref[...]

    def exchange(axis, source, slots):
        waits = []
        for step in (2, 1, 3):
            peer = shifted(me, axis, step)
            waits.append(copies.start(source.at[peer[axis]], slots.at[me[axis]], peer))
        slots[me[axis]] = source[me[axis]]
        return waits

    def total(waits, slots):
        for copy in waits:
            copy.wait_recv()
        return (slots[0] + slots[1]) + (slots[2] + slots[3])

    def spread(axis, view):
        return [copies.start(view, view, shifted(me, axis, step)) for step in (2, 1, 3)]

    waits = exchange("x", other, at_x)
    yield
    at_x[4] = total(waits, at_x)
    waits = exchange("y", at_x.at[4], at_y)
    yield
    at_y[4] = total(waits, at_y)
    waits = exchange("z", at_y.at[4], at_z)
    yield
    own = out_ref.at[me["x"], me["y"], me["z"]]
    own[...] = total(waits, at_z)
    for axis, view in (
        ("z", own),
        ("y", out_ref.at[me["x"], me["y"]]),
        ("x", out_ref.at[me["x"]]),
    ):
        waits = spread(axis, view)
        yield
        for copy in waits:
            copy.wait_recv()


def rows_padded(values, rows):
    short = rows - values.shape[0]
    if short == 0:
        return values
    return jnp.concatenate([values, jnp.zeros((short, values.shape[1]), values.dtype)], 0)


def image_chain(copies, me, out):
    held = dict(me)
    for axis in ("core", "x", "z", "y"):
        view = pick(out, held)
        steps = (1,) if axis == "core" else (2, 1, 3)
        waits = [copies.start(view, view, shifted(me, axis, step)) for step in steps]
        yield
        for copy in waits:
            copy.wait_recv()
        held.pop(axis)


def norm_rows(values, gain):
    center = values - jnp.mean(values, -1, keepdims=True)
    variance = jnp.mean(center * center, -1, keepdims=True)
    return (center * lax.rsqrt(variance + 1e-05) * gain).astype(jnp.bfloat16)


ORDERS = (("x", "y", "z"), ("y", "z", "x"), ("z", "x", "y"))
COLS = 256


def dims_of(axes):
    dims = []
    if "x" in axes:
        dims.append(2)
    if "y" in axes:
        dims.append(4)
    if "x" in axes:
        dims.append(2)
    if "z" in axes:
        dims.append(4)
    return tuple(dims)


def rest_of(order, phase):
    return [a for a in ("x", "y", "z") if a not in order[: phase + 1]]


def half_shape(order, phase, rows):
    shape = dims_of(rest_of(order, phase)) + (rows, COLS)
    if len(shape) == 2:
        return (rows, COLS // 2)
    return (shape[0] // 2,) + shape[1:]


def add_into(dst, srcs):
    lead = dst.shape[:-3]
    total = 1
    for size in lead:
        total *= size

    def one(index):
        value = dst[index].astype(jnp.float32)
        for src in srcs:
            value = value + src[index].astype(jnp.float32)
        dst[index] = value.astype(dst.dtype)

    if total == 1:
        one((0,) * len(lead) + (Ellipsis,))
        return

    def body(n, carry):
        index = []
        rest = n
        for size in reversed(lead):
            index.append(rest % size)
            rest = rest // size
        one(tuple(reversed(index)))
        return carry

    lax.fori_loop(0, total, body, 0)


def rows_of(view, first, count, cols=None):
    lead = (slice(None),) * (len(view.shape) - 2)
    return view.at[lead + (pl.ds(first, count), slice(None) if cols is None else cols)]


class Scatter:
    def __init__(self, copies, me, sibling, ref, accs, hold):
        self.copies, self.me, self.sibling = copies, me, sibling
        self.ref, self.accs, self.hold = ref, accs, hold
        self.opening = {}
        self.sums = [None] * 3

    def first(self, t):
        return self.hold[t * 4]

    def second(self, t, phase):
        return self.hold[t * 4 + 1 + phase]

    def source(self, t, at):
        return rows_of(pick(self.ref, at), 0, self.ref.shape[-2], pl.ds(t * COLS, COLS))

    def at(self, t, step):
        axis = ORDERS[t][0]
        return {axis: shifted(self.me, axis, step)[axis]}

    def push(self):
        for step in (2, 1, 3, 0):
            for t in range(3):
                at = self.at(t, step)
                self.opening[t, step] = self.copies.start(
                    self.source(t, {**at, "core": self.sibling["core"]}),
                    pick(self.accs[t], at),
                    self.sibling,
                )

    def opened(self, t, step):
        at = self.at(t, step)
        self.opening[t, step].wait_recv()
        add_into(pick(self.accs[t], at), [self.source(t, {**at, "core": self.me["core"]})])

    def open_phase(self, t, phase, held):
        axis = ORDERS[t][phase]
        if phase > 0:
            waits = []
            for step in (2, 1, 3):
                peer = shifted(self.me, axis, step)
                view = pick(self.accs[t], {**held, axis: peer[axis]})
                waits.append(self.copies.start(view, self.second(t, phase).at[step - 1], peer))
            return waits
        far = shifted(self.me, axis, 2)
        view = pick(self.accs[t], {**held, axis: far[axis]})
        up, down = shifted(self.me, axis, 1), shifted(self.me, axis, 3)
        return (
            self.copies.start(half(view, 0), self.first(t).at[0], up),
            self.copies.start(half(view, 1), self.first(t).at[1], down),
        )

    def chain(self):
        me, accs = self.me, self.accs
        pending = [None] * 3
        held = [dict() for _ in range(3)]
        for t in range(3):
            self.opened(t, 2)
            pending[t] = self.open_phase(t, 0, held[t])
        for step in (1, 3, 0):
            for t in range(3):
                self.opened(t, step)
        yield
        for t in range(3):
            axis = ORDERS[t][0]
            up, down = shifted(me, axis, 1), shifted(me, axis, 3)
            to_up = pick(accs[t], {axis: up[axis]})
            to_down = pick(accs[t], {axis: down[axis]})
            pending[t][0].wait_recv()
            add_into(half(to_up, 0), [self.first(t).at[0]])
            a = self.copies.start(to_up, self.second(t, 0).at[0], up)
            pending[t][1].wait_recv()
            add_into(half(to_down, 1), [self.first(t).at[1]])
            b = self.copies.start(to_down, self.second(t, 0).at[1], down)
            pending[t] = (a, b)
        for phase in range(2):
            yield
            for t in range(3):
                axis = ORDERS[t][phase]
                for copy in pending[t]:
                    copy.wait_recv()
                held[t][axis] = me[axis]
                got = self.second(t, phase)
                add_into(pick(accs[t], held[t]), [got.at[i] for i in range(len(pending[t]))])
                pending[t] = self.open_phase(t, phase + 1, held[t])
        yield
        for t in range(3):
            for copy in pending[t]:
                copy.wait_recv()
            axis = ORDERS[t][2]
            value = pick(accs[t], {**held[t], axis: me[axis]})[...].astype(jnp.float32)
            for slot in range(3):
                value = value + self.second(t, 2)[slot].astype(jnp.float32)
            self.sums[t] = value


def scalar_chain(copies, me, sibling, tile, slots):
    waits = [copies.start(tile, slots.at[0, me["core"]], sibling)]
    slots[0, me["core"]] = tile[...]
    value = None
    for phase, axis in enumerate(("x", "y", "z", None)):
        yield
        for copy in waits:
            copy.wait_recv()
        value = slots[phase, 0] + slots[phase, 1]
        if phase:
            value = value + (slots[phase, 2] + slots[phase, 3])
        if axis is None:
            break
        mine = slots.at[phase + 1, me[axis]]
        mine[...] = value
        waits = [copies.start(mine, mine, shifted(me, axis, step)) for step in (2, 1, 3)]
    slots[4, 0] = value


def gelu_tanh(values):
    return jax.nn.gelu(values, approximate=True)


def dot(a, b, da, db):
    return lax.dot_general(a, b, (((da,), (db,)), ((), ())), preferred_element_type=jnp.float32)


def exact(a, b, da, db):
    return lax.dot_general(
        a, b, (((da,), (db,)), ((), ())),
        precision=lax.Precision.HIGHEST, preferred_element_type=jnp.float32,
    )


ORDER = (
    "VHvPDQdEeCKnnnHPuUKnDQVdnHPvuUQVEKHePvUuQVEePvuUKVvEDedu",
    "UPQHuVvKUVEevhhhPhhhQhKhdDPssssEessssKESIedDIHQdDQ",
)


def step_kernel(
    t_up, t_down, up, down, head, proj, table, ids, t_in, t_gain, s_in, s_gain, positive,
    o_up, o_down, o_head, o_proj, o_loss,
    g_up, g_down, g_pack, g_head, g_proj, captions, images, gates, acts, normed, rounded, wide,
    far, near, got, t_normed, t_act, s_acc, grad_out, grad_img, d_pack, d_head, f_tile,
    words, other, at_x, at_y, at_z, s_slots, send, recv, *stores
):
    me = coords()
    grp = me["x"] % 2
    shard = grp * 64 + me["y"] * 16 + me["x"] // 2 * 8 + me["z"] * 2 + me["core"]
    sibling = shifted(me, "core", 1)
    feat, hid = head.shape[0], up.shape[0]
    width = t_in.shape[1]
    f32, bf16 = jnp.float32, jnp.bfloat16
    iota = lambda shape, axis: lax.broadcasted_iota(jnp.int32, shape, axis)

    entered = enter(me)
    pick(g_pack, me)[...] = jnp.concatenate([up[...].astype(f32), down[...].astype(f32)], 0).astype(
        bf16
    )
    pick(g_head, me)[...] = rows_padded(head[...].astype(f32), BLK).astype(bf16)
    values = proj[...].astype(f32)
    cut = values.shape[1] // 2
    pick(g_proj, me)[...] = jnp.concatenate([values[:, :cut], values[:, cut:]], 0).astype(bf16)
    for source, out in ((t_up, g_up), (t_down, g_down)):
        values = source[...].astype(f32)
        for part in range(2):
            cut = values[part * feat : (part + 1) * feat]
            pick_teacher(out, me, (pl.ds(part * BLK, BLK),))[...] = rows_padded(cut, BLK).astype(
                bf16
            )
    entered()
    copies = Copies(send, recv)

    def teacher(ref, part, other_x):
        order = ("y", "z") if part == 0 else ("z", "y")
        return teacher_chain(copies, me, sibling, ref, part, order, other_x)

    chains = {
        "P": student_chain(copies, me, sibling, g_pack, ("y", "z", "x")),
        "H": student_chain(copies, me, sibling, g_head, ("z", "y", "x")),
        "Q": student_chain(copies, me, sibling, g_proj, ("z", "y", "x")),
        "K": caption_chain(copies, me, sibling, words, captions, other, at_x, at_y, at_z),
        "I": image_chain(copies, me, images),
    }
    for part in range(2):
        chains["uU"[part]] = teacher(g_up, part, False)
        chains["vV"[part]] = teacher(g_up, part, True)
        chains["dD"[part]] = teacher(g_down, part, False)
        chains["eE"[part]] = teacher(g_down, part, True)

    own_rows = normed.shape[0]
    own = pl.ds(pl.multiple_of(grp * own_rows, own_rows), own_rows)
    partner_rows = pl.ds(pl.multiple_of((1 - grp) * own_rows, own_rows), own_rows)
    step = 256
    span = step // BLK * feat

    def count_words():
        vocab = table.shape[0]
        code = iota((vocab, ids.shape[1]), 0) + shard * vocab

        def body(j, counts):
            return counts + jnp.where(code == ids[pl.ds(j, 1), :], 1.0, 0.0)

        counts = lax.fori_loop(0, ids.shape[0], body, jnp.zeros(code.shape, f32))
        sums = dot(counts.astype(bf16), table[...], 0, 0) / CAP_LEN
        for z in range(4):
            words[:, :, z] = sums[:, z * 128 : (z + 1) * 128].reshape(4, 4, 8, 128)

    def student_norm():
        normed[...] = norm_rows(s_in[own, :].astype(f32), s_gain[...].reshape(1, -1))

    def teacher_norm():
        def body(r, carry):
            rows = pl.ds(pl.multiple_of(r * 64, 64), 64)
            t_act[rows, pl.ds(0, width)] = norm_rows(t_in[rows, :].astype(f32), t_gain[...].reshape(1, -1))
            return carry

        lax.fori_loop(0, t_in.shape[0] // 64, body, 0)

    def spread(j):
        base = span * j // 128 * 128
        size = -(-(span * j + span - base) // 128) * 128
        row = iota((size, step), 0) + base
        col = iota((size, step), 1)
        place = span * j + col // BLK * feat + col % BLK
        chosen = jnp.where((row == place) & (col % BLK < feat), 1.0, 0.0).astype(bf16)
        window = pl.ds(base, size)
        cols = pl.ds(j * step, step)
        t_normed[:, cols] = dot(t_act[:, window], chosen, 1, 0).astype(bf16)
        wide[:, cols] = dot(t_in[own, window], chosen, 1, 0).astype(bf16)

    def hidden(j):
        cols = pl.ds(j * step, step)
        weights = g_up[:, :, :, :, :, cols].reshape(-1, step)
        t_act[:, cols] = gelu_tanh(dot(t_normed[...], weights, 1, 0)).astype(bf16)

    def branch(y, rows, out):
        weights = g_down[y].reshape(-1, g_down.shape[-1])
        out[y] = dot(t_act[rows, :], weights, 1, 1).astype(bf16)

    def ups(shape):
        return iota(shape, 0) % (2 * hid) < hid

    def student(n):
        weights = g_pack[n // 4, n % 4].reshape(-1, g_pack.shape[-1])
        size = weights.shape[0]
        units = pl.ds(n * size, size)
        gate = dot(weights, normed[...], 1, 1)
        gates[units, :] = gate
        act = jnp.where(ups(gate.shape), gelu_tanh(gate), 0.0)
        act = pltpu.roll(act, hid, 0).astype(bf16)
        acts[units, :] = act
        part = dot(act, weights, 0, 0)
        s_acc[...] = part + (s_in[own, :].astype(f32) if n == 0 else s_acc[...])

    def student_end():
        value = s_acc[...]
        rounded[...] = value.astype(bf16)
        pooled = jnp.sum(value, 0, keepdims=True) / PATCHES
        lanes = [pooled[:, i * 128 : (i + 1) * 128] for i in range(pooled.shape[1] // 128)]
        tile = rows_padded(jnp.concatenate(lanes, 0), 8)
        pick(images, me)[...] = tile.astype(bf16).astype(f32)

    work = {
        "C": [count_words],
        "n": [student_norm, teacher_norm]
        + [lambda k=k: [spread(j) for j in range(k, k + 3) if j < 8] for k in (0, 3, 6)],
        "h": [lambda j=j: hidden(j) for j in range(8)],
        "s": [lambda n=n: student(n) for n in range(8)],
        "S": [student_end],
    }
    for line in ORDER:
        for name in line:
            if name in work:
                work[name].pop(0)()
            else:
                next(chains[name], None)

    partner = {**me, "x": me["x"] + 1 - 2 * grp}
    exchange = []
    for y in range(4):
        branch(y, partner_rows, far)
        exchange.append(copies.start(far.at[y], got.at[y], partner))
    next(chains["I"], None)
    branch(0, own, near)
    branch(1, own, near)
    branch(2, own, near)
    next(chains["I"], None)
    branch(3, own, near)
    images_left = chains.pop("I")
    for turn in range(8):
        for one in chains.values():
            next(one, None)

    s_acc[...] = jnp.zeros_like(s_acc)
    f_tile[...] = jnp.zeros_like(f_tile)

    def head_block(n, carry):
        weights = g_head[n // 4, n % 4].reshape(step, -1)
        cols = pl.ds(pl.multiple_of(n * step, step), step)
        lanes = pl.ds(pl.multiple_of(n % 2 * step, step), step)
        pred = dot(rounded[...], weights, 1, 1)
        added = near[n // 2, :, lanes].astype(f32) + got[n // 2, :, lanes].astype(f32)
        diff = pred - (wide[:, cols].astype(f32) + added)
        f_tile[...] = f_tile[...] + jnp.sum(diff * diff)
        grad_pred = (2.0 * diff / width).astype(bf16)
        d_head[n // 4, n % 4] = (
            dot(grad_pred, rounded[...], 0, 0).astype(bf16).reshape(d_head.shape[2:])
        )
        s_acc[...] = s_acc[...] + dot(grad_pred, weights, 1, 0)
        return carry

    def head_blocks(y):
        exchange[y].wait_recv()
        lax.fori_loop(2 * y, 2 * y + 2, head_block, 0)

    head_blocks(0)
    next(images_left, None)

    n_img = 128
    cols_dev = o_proj.shape[0]
    flat = images.reshape(n_img * 8, 128)
    pooled = [flat[pl.ds(i, n_img, stride=8), :] for i in range(g_proj.shape[-1] * 2 // 128)]
    pooled = jnp.concatenate(pooled, 1).astype(bf16)
    proj_all = g_proj[...].reshape(n_img * 8, g_proj.shape[-1])
    cut = g_proj.shape[-1]
    n_emb = proj_all.shape[0]
    low = dot(pooled[:, :cut], proj_all, 1, 1)
    high = dot(pooled[:, cut:], proj_all, 1, 1)
    real = iota(low.shape, 1) % 8 < cols_dev
    projected = jnp.where(real, low + pltpu.roll(high, n_emb - cols_dev, 1), 0.0)
    proj_norm = jnp.sqrt(jnp.sum(projected * projected, -1, keepdims=True) + 1e-06)
    image_emb = projected / proj_norm
    parts = [captions[:, :, z].reshape(n_img, 128) for z in range(4)]
    squares = sum(jnp.sum(part * part, -1, keepdims=True) for part in parts)
    size = 128 // cols_dev * 8
    row, col = iota((128, size), 0), iota((128, size), 1)
    chosen = jnp.where((row == col // 8 * cols_dev + col % 8) & (col % 8 < cols_dev), 1.0, 0.0)
    caption_all = jnp.concatenate([exact(part, chosen, 1, 0) for part in parts], 1)
    caption_all = caption_all / jnp.sqrt(squares + 1e-06)
    scores = 100.0 * exact(image_emb, caption_all, 1, 1)
    target = jnp.broadcast_to(positive[...].reshape(1, -1), (n_img, n_img))
    match = jnp.where(iota(target.shape, 0) == target, 1.0, 0.0).astype(bf16)
    row = iota(target.shape, 0)
    chosen = jnp.where(iota(target.shape, 1) == row % 64 * 2 + row // 64, 1.0, 0.0).astype(bf16)
    match = dot(chosen, match, 1, 1)

    def soft(axis):
        top = jnp.max(scores, axis, keepdims=True)
        powers = jnp.exp(scores - top)
        total = jnp.sum(powers, axis, keepdims=True)
        return jnp.sum(top + jnp.log(total)), powers / total

    log_rows, soft_rows = soft(1)
    log_cols, soft_cols = soft(0)
    contrast = log_rows + log_cols - 2.0 * jnp.sum(match * scores)
    grad_scores = soft_rows + soft_cols - 2.0 * match
    grad_image = 100.0 * exact(grad_scores, caption_all, 1, 0)
    inner = jnp.sum(image_emb * grad_image, -1, keepdims=True)
    grad_projected = ((grad_image - image_emb * inner) / proj_norm).astype(bf16)
    grad_img[...] = grad_projected.astype(f32)
    row, col = iota((n_emb, 128), 0), iota((n_emb, 128), 1)
    chosen = jnp.where((row == 8 * shard + col) & (col < cols_dev), 1.0, 0.0).astype(bf16)
    columns = dot(grad_projected, chosen, 1, 0).astype(bf16)
    o_proj[...] = dot(columns, pooled, 0, 0)[:cols_dev]
    mine = jnp.broadcast_to(grad_img[pl.ds(shard, 1), :], (8, n_emb))
    grad_low = dot(mine.astype(bf16), proj_all, 1, 0)
    grad_high = dot(pltpu.roll(mine, cols_dev, 1).astype(bf16), proj_all, 1, 0)
    grad_pooled = jnp.concatenate([grad_low, grad_high], 1)[:1]

    for y in range(1, 4):
        head_blocks(y)
    n_store = len(stores) // 2
    head_sums = Scatter(copies, me, sibling, d_head, stores[:3], stores[3:n_store])
    pack_sums = Scatter(copies, me, sibling, d_pack, stores[n_store : n_store + 3], stores[n_store + 3 :])
    head_sums.push()
    f_tile[...] = f_tile[...] / width
    ends = [head_sums.chain(), scalar_chain(copies, me, sibling, f_tile, s_slots)]
    grad_out[...] = (s_acc[...] + grad_pooled / PATCHES).astype(bf16)

    def pack_block(n, carry):
        weights = g_pack[n // 4, n % 4].reshape(-1, g_pack.shape[-1])
        size = weights.shape[0]
        units = pl.ds(pl.multiple_of(n * size, 128), size)
        grad_act = pltpu.roll(dot(weights, grad_out[...], 1, 1), size - hid, 0)
        grad_gate = jax.vjp(gelu_tanh, gates[units, :])[1](grad_act)[0]
        grad_gate = jnp.where(ups(grad_gate.shape), grad_gate, 0.0).astype(bf16)
        total = dot(grad_gate, normed[...], 1, 0) + dot(acts[units, :], grad_out[...], 1, 0)
        d_pack[n // 4, n % 4] = total.astype(bf16).reshape(d_pack.shape[2:])
        return carry

    for part in range(4):
        lax.fori_loop(2 * part, 2 * part + 2, pack_block, 0)
        for one in ends:
            next(one, None)
    pack_sums.push()
    ends.append(pack_sums.chain())
    for turn in range(8):
        for one in ends:
            next(one, None)
    for t in range(3):
        cols = pl.ds(t * COLS, COLS)
        o_up[:, cols] = pack_sums.sums[t][:hid]
        o_down[:, cols] = pack_sums.sums[t][hid:]
        o_head[:, cols] = head_sums.sums[t][:feat]
    o_loss[...] = (s_slots[4, 0] + contrast) / (n_img * PATCHES)
    copies.finish()


N_COPIES = 22 * 3 + 19 + 4 * 15 + 4 * 16 + 10 + 4 + 10 + 2 * 42


def run_step(t_up, t_down, up, down, head, proj, table, ids, t_in, t_gain, s_in, s_gain, positive):
    bf16, f32 = t_up.dtype, jnp.float32
    rows, width = t_in.shape[0], up.shape[1]
    own_rows = rows // 2
    hid, feat = up.shape[0], head.shape[0]
    whole = (2, 4, 2, 4, 2)
    tiles = (4, 4, 4, 8, 128)
    teacher = (4, 2, 4, 2, 2 * BLK, t_up.shape[1])
    n_wide = 128 * BLK
    n_pack = 128 * 2 * hid
    vmem = pltpu.VMEM
    scratch = [
        vmem(teacher, bf16),
        vmem(teacher, bf16),
        vmem(whole + (2 * hid, width), bf16),
        vmem(whole + (BLK, width), bf16),
        vmem(whole + (2 * proj.shape[0], width // 2), bf16),
        vmem(tiles, f32),
        vmem(whole + (8, 128), f32),
        vmem((n_pack, own_rows), f32),
        vmem((n_pack, own_rows), bf16),
        vmem((own_rows, width), bf16),
        vmem((own_rows, width), bf16),
        vmem((own_rows, n_wide), bf16),
        vmem((4, own_rows, n_wide // 4), bf16),
        vmem((4, own_rows, n_wide // 4), bf16),
        vmem((4, own_rows, n_wide // 4), bf16),
        vmem((rows, n_wide), bf16),
        vmem((rows, t_up.shape[1]), bf16),
        vmem((own_rows, width), f32),
        vmem((own_rows, width), bf16),
        vmem((128, 128 * 8), f32),
        vmem(whole + (2 * hid, width), bf16),
        vmem(whole + (BLK, width), bf16),
        vmem((8, 128), f32),
        vmem(tiles, f32),
        vmem(tiles, f32),
        vmem((5, 4, 4, 8, 128), f32),
        vmem((5, 4, 8, 128), f32),
        vmem((4, 8, 128), f32),
        vmem((5, 4, 8, 128), f32),
        pltpu.SemaphoreType.DMA((N_COPIES,)),
        pltpu.SemaphoreType.DMA((N_COPIES,)),
    ]
    for block in (BLK, 2 * hid):
        scratch += [vmem((2, 4, 2, 4, block, COLS), bf16) for _ in range(3)]
        for order in ORDERS:
            scratch.append(vmem((2,) + half_shape(order, 0, block), bf16))
            for phase, count in enumerate((2, 3, 3)):
                rest = dims_of(rest_of(order, phase)) + (block, COLS)
                scratch.append(vmem((count,) + rest, bf16))
    shapes = [(hid, width), (hid, width), (feat, width), (proj.shape[0], width), (8, 128)]
    shapes = [jax.ShapeDtypeStruct(shape, f32) for shape in shapes]
    out = pl.pallas_call(
        step_kernel,
        out_shape=shapes,
        in_specs=[VM] * 13,
        out_specs=[VM] * 5,
        scratch_shapes=scratch,
        compiler_params=pltpu.CompilerParams(
            collective_id=1, has_side_effects=True, vmem_limit_bytes=67043328
        ),
        name="step",
    )(t_up, t_down, up, down, head, proj, table, ids, t_in, t_gain, s_in, s_gain, positive)
    return pl.pallas_call(
        write_kernel,
        out_shape=shapes[:4] + [jax.ShapeDtypeStruct((1, 1), f32)],
        in_specs=[VM] * 5,
        out_specs=[VM] * 4 + [pl.BlockSpec(memory_space=pltpu.SMEM)],
        name="write",
    )(*out)


def write_kernel(*refs):
    for source, out in zip(refs[:4], refs[5:9]):
        out[...] = source[...]
    refs[9][0, 0] = jnp.max(refs[4][...])


def local(
    teacher_in,
    teacher_gain,
    teacher_up,
    teacher_down,
    student_in,
    student_gain,
    student_up,
    student_down,
    student_head,
    student_proj,
    word_table,
    caption_ids,
    positive,
):
    grad_up, grad_down, grad_head, grad_proj, loss = run_step(
        teacher_up,
        teacher_down,
        student_up.T,
        student_down,
        student_head.T,
        student_proj.T,
        word_table,
        caption_ids.T,
        teacher_in,
        teacher_gain,
        student_in,
        student_gain,
        positive,
    )
    return (loss[0, 0], grad_up.T, grad_down, grad_head.T, grad_proj.T)


def solution(mesh):
    placed = (
        P("dp", None),
        P(),
        P("dp", "grp"),
        P("dp", "grp"),
        P("dp", None),
        P(),
        P(None, ("grp", "dp")),
        P(("grp", "dp"), None),
        P(None, ("grp", "dp")),
        P(None, ("grp", "dp")),
        P(("grp", "dp"), None),
        P(),
        P(),
    )
    return jax.shard_map(
        local,
        mesh=mesh,
        in_specs=placed,
        out_specs=(
            P(),
            P(None, ("grp", "dp")),
            P(("grp", "dp"), None),
            P(None, ("grp", "dp")),
            P(None, ("grp", "dp")),
        ),
        check_vma=False,
    )
```

```python
import jax
import jax.numpy as jnp
from jax import lax
from jax.experimental import pallas as pl
from jax.experimental.pallas import tpu as pltpu
from jax.sharding import PartitionSpec as P

CAP_LEN = 77
PATCHES = 256
BLK = 16
MESH = pl.DeviceIdType.MESH
VM = pl.BlockSpec(memory_space=pltpu.VMEM)


def coords():
    grp = lax.axis_index("grp")
    dp = lax.axis_index("dp")
    x_hi = (dp // 8) % 2
    return {
        "x": 2 * x_hi + grp,
        "y": dp // 16,
        "z": (dp // 2) % 4,
        "core": dp % 2,
    }


def device(at):
    return (at["x"] % 2, at["y"] * 16 + (at["x"] // 2) * 8 + at["z"] * 2 + at["core"])


def shifted(me, axis, step):
    if axis == "core":
        return {**me, "core": 1 - me["core"]}
    return {**me, axis: (me[axis] + step) % 4}


def enter(me, axes=("x", "y", "z"), steps=(1, 2, 3)):
    barrier = pltpu.get_barrier_semaphore()
    peers = [shifted(me, "core", 1)]
    for axis in axes:
        for step in steps:
            peers.append(shifted(me, axis, step))
    for peer in peers:
        pl.semaphore_signal(barrier, inc=1, device_id=device(peer), device_id_type=MESH)
    return lambda: pl.semaphore_wait(barrier, len(peers))


class Copies:
    def __init__(self, send, recv):
        self.send, self.recv, self.count, self.open = send, recv, 0, []

    def start(self, src, dst, peer):
        copy = pltpu.make_async_remote_copy(
            src_ref=src,
            dst_ref=dst,
            send_sem=self.send.at[self.count],
            recv_sem=self.recv.at[self.count],
            device_id=device(peer),
            device_id_type=MESH,
        )
        self.count += 1
        copy.start()
        self.open.append(copy)
        return copy

    def finish(self):
        for copy in self.open:
            copy.wait_send()


def pick(ref, at, tail=()):
    x = at.get("x")
    whole = slice(None)
    index = (
        whole if x is None else x % 2,
        at.get("y", whole),
        whole if x is None else x // 2,
        at.get("z", whole),
    )
    if "core" in at:
        index += (at["core"],)
    return ref.at[index + tail]


def half(ref, side):
    if len(ref.shape) > 2:
        size = ref.shape[0] // 2
        return ref.at[pl.ds(side * size, size)]
    lanes = ref.shape[1] // 128
    cut = lanes // 2 * 128
    if side == 0:
        return ref.at[:, pl.ds(0, cut)]
    return ref.at[:, pl.ds(cut, ref.shape[1] - cut)]


def pick_teacher(ref, at, tail=()):
    whole = slice(None)
    index = (
        at.get("y", whole),
        at["x"] // 2,
        at.get("z", whole),
        at["core"],
    )
    return ref.at[index + tail]


def ring(copies, me, sibling, view, order, held, pushes):
    for axis in order:
        up, down, far = (shifted(me, axis, s) for s in (1, 3, 2))
        block = view(held)
        right = copies.start(block, block, up)
        left = copies.start(block, block, down)
        yield
        right.wait_recv()
        from_down = view({**held, axis: down[axis]})
        right2 = copies.start(half(from_down, 0), half(from_down, 0), up)
        pushes.append(copies.start(from_down, from_down, sibling))
        left.wait_recv()
        from_up = view({**held, axis: up[axis]})
        left2 = copies.start(half(from_up, 1), half(from_up, 1), down)
        pushes.append(copies.start(from_up, from_up, sibling))
        yield
        right2.wait_recv()
        left2.wait_recv()
        from_far = view({**held, axis: far[axis]})
        pushes.append(copies.start(from_far, from_far, sibling))
        held.pop(axis)


def student_chain(copies, me, sibling, ref, order):
    view = lambda at: pick(ref, at)
    own = view(me)
    pushes = [copies.start(own, own, sibling)]
    yield from ring(copies, me, sibling, view, order, dict(me), pushes)
    yield
    for copy in pushes:
        copy.wait_recv()


def teacher_chain(copies, me, sibling, ref, part, order, other):
    tail = (pl.ds(part * BLK, BLK),)
    view = lambda at: pick_teacher(ref, at, tail)
    pushes = []
    held = dict(me)
    if other:
        far = shifted(me, "x", 2)
        copy = copies.start(view(me), view(me), far)
        yield
        copy.wait_recv()
        held = dict(far)
    block = view(held)
    pushes.append(copies.start(block, block, sibling))
    yield from ring(copies, me, sibling, view, order, held, pushes)
    yield
    for copy in pushes:
        copy.wait_recv()


def caption_chain(copies, me, sibling, p_ref, out_ref, other, at_x, at_y, at_z):
    copy = copies.start(p_ref, other, sibling)
    yield
    copy.wait_recv()
    other[...] = other[...] + p_ref[...]

    def exchange(axis, source, slots):
        waits = []
        for step in (2, 1, 3):
            peer = shifted(me, axis, step)
            waits.append(copies.start(source.at[peer[axis]], slots.at[me[axis]], peer))
        slots[me[axis]] = source[me[axis]]
        return waits

    def total(waits, slots):
        for copy in waits:
            copy.wait_recv()
        return (slots[0] + slots[1]) + (slots[2] + slots[3])

    def spread(axis, view):
        return [copies.start(view, view, shifted(me, axis, step)) for step in (2, 1, 3)]

    waits = exchange("x", other, at_x)
    yield
    at_x[4] = total(waits, at_x)
    waits = exchange("y", at_x.at[4], at_y)
    yield
    at_y[4] = total(waits, at_y)
    waits = exchange("z", at_y.at[4], at_z)
    yield
    own = out_ref.at[me["x"], me["y"], me["z"]]
    own[...] = total(waits, at_z)
    for axis, view in (
        ("z", own),
        ("y", out_ref.at[me["x"], me["y"]]),
        ("x", out_ref.at[me["x"]]),
    ):
        waits = spread(axis, view)
        yield
        for copy in waits:
            copy.wait_recv()


def rows_padded(values, rows):
    short = rows - values.shape[0]
    if short == 0:
        return values
    return jnp.concatenate([values, jnp.zeros((short, values.shape[1]), values.dtype)], 0)


def image_chain(copies, me, out):
    held = dict(me)
    for axis in ("core", "x", "z", "y"):
        view = pick(out, held)
        steps = (1,) if axis == "core" else (2, 1, 3)
        waits = [copies.start(view, view, shifted(me, axis, step)) for step in steps]
        yield
        for copy in waits:
            copy.wait_recv()
        held.pop(axis)


def norm_rows(values, gain):
    center = values - jnp.mean(values, -1, keepdims=True)
    variance = jnp.mean(center * center, -1, keepdims=True)
    return (center * lax.rsqrt(variance + 1e-05) * gain).astype(jnp.bfloat16)


ORDERS = (("x", "y", "z"), ("y", "z", "x"), ("z", "x", "y"))
COLS = 256


def dims_of(axes):
    dims = []
    if "x" in axes:
        dims.append(2)
    if "y" in axes:
        dims.append(4)
    if "x" in axes:
        dims.append(2)
    if "z" in axes:
        dims.append(4)
    return tuple(dims)


def rest_of(order, phase):
    return [a for a in ("x", "y", "z") if a not in order[: phase + 1]]


def half_shape(order, phase, rows):
    shape = dims_of(rest_of(order, phase)) + (rows, COLS)
    if len(shape) == 2:
        return (rows, COLS // 2)
    return (shape[0] // 2,) + shape[1:]


def add_into(dst, srcs):
    lead = dst.shape[:-3]
    total = 1
    for size in lead:
        total *= size

    def one(index):
        value = dst[index].astype(jnp.float32)
        for src in srcs:
            value = value + src[index].astype(jnp.float32)
        dst[index] = value.astype(dst.dtype)

    if total == 1:
        one((0,) * len(lead) + (Ellipsis,))
        return

    def body(n, carry):
        index = []
        rest = n
        for size in reversed(lead):
            index.append(rest % size)
            rest = rest // size
        one(tuple(reversed(index)))
        return carry

    lax.fori_loop(0, total, body, 0)


def rows_of(view, first, count, cols=None):
    lead = (slice(None),) * (len(view.shape) - 2)
    return view.at[lead + (pl.ds(first, count), slice(None) if cols is None else cols)]


class Scatter:
    def __init__(self, copies, me, sibling, ref, accs, hold):
        self.copies, self.me, self.sibling = copies, me, sibling
        self.ref, self.accs, self.hold = ref, accs, hold
        self.opening = {}
        self.sums = [None] * 3

    def first(self, t):
        return self.hold[t * 4]

    def second(self, t, phase):
        return self.hold[t * 4 + 1 + phase]

    def source(self, t, at):
        return rows_of(pick(self.ref, at), 0, self.ref.shape[-2], pl.ds(t * COLS, COLS))

    def at(self, t, step):
        axis = ORDERS[t][0]
        return {axis: shifted(self.me, axis, step)[axis]}

    def push(self):
        for step in (2, 1, 3, 0):
            for t in range(3):
                at = self.at(t, step)
                self.opening[t, step] = self.copies.start(
                    self.source(t, {**at, "core": self.sibling["core"]}),
                    pick(self.accs[t], at),
                    self.sibling,
                )

    def opened(self, t, step):
        at = self.at(t, step)
        self.opening[t, step].wait_recv()
        add_into(pick(self.accs[t], at), [self.source(t, {**at, "core": self.me["core"]})])

    def open_phase(self, t, phase, held):
        axis = ORDERS[t][phase]
        if phase > 0:
            waits = []
            for step in (2, 1, 3):
                peer = shifted(self.me, axis, step)
                view = pick(self.accs[t], {**held, axis: peer[axis]})
                waits.append(self.copies.start(view, self.second(t, phase).at[step - 1], peer))
            return waits
        far = shifted(self.me, axis, 2)
        view = pick(self.accs[t], {**held, axis: far[axis]})
        up, down = shifted(self.me, axis, 1), shifted(self.me, axis, 3)
        return (
            self.copies.start(half(view, 0), self.first(t).at[0], up),
            self.copies.start(half(view, 1), self.first(t).at[1], down),
        )

    def chain(self):
        me, accs = self.me, self.accs
        pending = [None] * 3
        held = [dict() for _ in range(3)]
        for t in range(3):
            self.opened(t, 2)
            pending[t] = self.open_phase(t, 0, held[t])
        for step in (1, 3, 0):
            for t in range(3):
                self.opened(t, step)
        yield
        for t in range(3):
            axis = ORDERS[t][0]
            up, down = shifted(me, axis, 1), shifted(me, axis, 3)
            to_up = pick(accs[t], {axis: up[axis]})
            to_down = pick(accs[t], {axis: down[axis]})
            pending[t][0].wait_recv()
            add_into(half(to_up, 0), [self.first(t).at[0]])
            a = self.copies.start(to_up, self.second(t, 0).at[0], up)
            pending[t][1].wait_recv()
            add_into(half(to_down, 1), [self.first(t).at[1]])
            b = self.copies.start(to_down, self.second(t, 0).at[1], down)
            pending[t] = (a, b)
        for phase in range(2):
            yield
            for t in range(3):
                axis = ORDERS[t][phase]
                for copy in pending[t]:
                    copy.wait_recv()
                held[t][axis] = me[axis]
                got = self.second(t, phase)
                add_into(pick(accs[t], held[t]), [got.at[i] for i in range(len(pending[t]))])
                pending[t] = self.open_phase(t, phase + 1, held[t])
        yield
        for t in range(3):
            for copy in pending[t]:
                copy.wait_recv()
            axis = ORDERS[t][2]
            value = pick(accs[t], {**held[t], axis: me[axis]})[...].astype(jnp.float32)
            for slot in range(3):
                value = value + self.second(t, 2)[slot].astype(jnp.float32)
            self.sums[t] = value


def scalar_chain(copies, me, sibling, tile, slots):
    waits = [copies.start(tile, slots.at[0, me["core"]], sibling)]
    slots[0, me["core"]] = tile[...]
    value = None
    for phase, axis in enumerate(("x", "y", "z", None)):
        yield
        for copy in waits:
            copy.wait_recv()
        value = slots[phase, 0] + slots[phase, 1]
        if phase:
            value = value + (slots[phase, 2] + slots[phase, 3])
        if axis is None:
            break
        mine = slots.at[phase + 1, me[axis]]
        mine[...] = value
        waits = [copies.start(mine, mine, shifted(me, axis, step)) for step in (2, 1, 3)]
    slots[4, 0] = value


def gelu_tanh(values):
    return jax.nn.gelu(values, approximate=True)


def dot(a, b, da, db):
    return lax.dot_general(a, b, (((da,), (db,)), ((), ())), preferred_element_type=jnp.float32)


def exact(a, b, da, db):
    return lax.dot_general(
        a, b, (((da,), (db,)), ((), ())),
        precision=lax.Precision.HIGHEST, preferred_element_type=jnp.float32,
    )


ORDER = (
    "VHvPDQdEeCKnnnHPuUKnDQVdnHPvuUQVEKHePvUuQVEePvuUKVvEDedu",
    "UPQHuVvKUVEevhhhPhhhQhKhdDPssssEessssKESIedDIHQdDQ",
)


def step_kernel(
    t_up, t_down, up, down, head, proj, table, ids, t_in, t_gain, s_in, s_gain, positive,
    o_up, o_down, o_head, o_proj, o_loss,
    g_up, g_down, g_pack, g_head, g_proj, captions, images, gates, acts, normed, rounded, wide,
    far, near, got, t_normed, t_act, s_acc, grad_out, grad_img, d_pack, d_head, f_tile,
    words, other, at_x, at_y, at_z, s_slots, send, recv, *stores
):
    me = coords()
    grp = me["x"] % 2
    shard = grp * 64 + me["y"] * 16 + me["x"] // 2 * 8 + me["z"] * 2 + me["core"]
    sibling = shifted(me, "core", 1)
    feat, hid = head.shape[0], up.shape[0]
    width = t_in.shape[1]
    f32, bf16 = jnp.float32, jnp.bfloat16
    iota = lambda shape, axis: lax.broadcasted_iota(jnp.int32, shape, axis)

    entered = enter(me)
    pick(g_pack, me)[...] = jnp.concatenate([up[...].astype(f32), down[...].astype(f32)], 0).astype(
        bf16
    )
    pick(g_head, me)[...] = rows_padded(head[...].astype(f32), BLK).astype(bf16)
    values = proj[...].astype(f32)
    cut = values.shape[1] // 2
    pick(g_proj, me)[...] = jnp.concatenate([values[:, :cut], values[:, cut:]], 0).astype(bf16)
    for source, out in ((t_up, g_up), (t_down, g_down)):
        values = source[...].astype(f32)
        for part in range(2):
            cut = values[part * feat : (part + 1) * feat]
            pick_teacher(out, me, (pl.ds(part * BLK, BLK),))[...] = rows_padded(cut, BLK).astype(
                bf16
            )
    entered()
    copies = Copies(send, recv)

    def teacher(ref, part, other_x):
        order = ("y", "z") if part == 0 else ("z", "y")
        return teacher_chain(copies, me, sibling, ref, part, order, other_x)

    chains = {
        "P": student_chain(copies, me, sibling, g_pack, ("y", "z", "x")),
        "H": student_chain(copies, me, sibling, g_head, ("z", "y", "x")),
        "Q": student_chain(copies, me, sibling, g_proj, ("z", "y", "x")),
        "K": caption_chain(copies, me, sibling, words, captions, other, at_x, at_y, at_z),
        "I": image_chain(copies, me, images),
    }
    for part in range(2):
        chains["uU"[part]] = teacher(g_up, part, False)
        chains["vV"[part]] = teacher(g_up, part, True)
        chains["dD"[part]] = teacher(g_down, part, False)
        chains["eE"[part]] = teacher(g_down, part, True)

    own_rows = normed.shape[0]
    own = pl.ds(pl.multiple_of(grp * own_rows, own_rows), own_rows)
    partner_rows = pl.ds(pl.multiple_of((1 - grp) * own_rows, own_rows), own_rows)
    step = 256
    span = step // BLK * feat

    def count_words():
        vocab = table.shape[0]
        code = iota((vocab, ids.shape[1]), 0) + shard * vocab

        def body(j, counts):
            return counts + jnp.where(code == ids[pl.ds(j, 1), :], 1.0, 0.0)

        counts = lax.fori_loop(0, ids.shape[0], body, jnp.zeros(code.shape, f32))
        sums = dot(counts.astype(bf16), table[...], 0, 0) / CAP_LEN
        for z in range(4):
            words[:, :, z] = sums[:, z * 128 : (z + 1) * 128].reshape(4, 4, 8, 128)

    def student_norm():
        normed[...] = norm_rows(s_in[own, :].astype(f32), s_gain[...].reshape(1, -1))

    def teacher_norm():
        def body(r, carry):
            rows = pl.ds(pl.multiple_of(r * 64, 64), 64)
            t_act[rows, pl.ds(0, width)] = norm_rows(t_in[rows, :].astype(f32), t_gain[...].reshape(1, -1))
            return carry

        lax.fori_loop(0, t_in.shape[0] // 64, body, 0)

    def spread(j):
        base = span * j // 128 * 128
        size = -(-(span * j + span - base) // 128) * 128
        row = iota((size, step), 0) + base
        col = iota((size, step), 1)
        place = span * j + col // BLK * feat + col % BLK
        chosen = jnp.where((row == place) & (col % BLK < feat), 1.0, 0.0).astype(bf16)
        window = pl.ds(base, size)
        cols = pl.ds(j * step, step)
        t_normed[:, cols] = dot(t_act[:, window], chosen, 1, 0).astype(bf16)
        wide[:, cols] = dot(t_in[own, window], chosen, 1, 0).astype(bf16)

    def hidden(j):
        cols = pl.ds(j * step, step)
        weights = g_up[:, :, :, :, :, cols].reshape(-1, step)
        t_act[:, cols] = gelu_tanh(dot(t_normed[...], weights, 1, 0)).astype(bf16)

    def branch(y, rows, out):
        weights = g_down[y].reshape(-1, g_down.shape[-1])
        out[y] = dot(t_act[rows, :], weights, 1, 1).astype(bf16)

    def ups(shape):
        return iota(shape, 0) % (2 * hid) < hid

    def student(n):
        weights = g_pack[n // 4, n % 4].reshape(-1, g_pack.shape[-1])
        size = weights.shape[0]
        units = pl.ds(n * size, size)
        gate = dot(weights, normed[...], 1, 1)
        gates[units, :] = gate
        act = jnp.where(ups(gate.shape), gelu_tanh(gate), 0.0)
        act = pltpu.roll(act, hid, 0).astype(bf16)
        acts[units, :] = act
        part = dot(act, weights, 0, 0)
        s_acc[...] = part + (s_in[own, :].astype(f32) if n == 0 else s_acc[...])

    def student_end():
        value = s_acc[...]
        rounded[...] = value.astype(bf16)
        pooled = jnp.sum(value, 0, keepdims=True) / PATCHES
        lanes = [pooled[:, i * 128 : (i + 1) * 128] for i in range(pooled.shape[1] // 128)]
        tile = rows_padded(jnp.concatenate(lanes, 0), 8)
        pick(images, me)[...] = tile.astype(bf16).astype(f32)

    work = {
        "C": [count_words],
        "n": [student_norm, teacher_norm]
        + [lambda k=k: [spread(j) for j in range(k, k + 3) if j < 8] for k in (0, 3, 6)],
        "h": [lambda j=j: hidden(j) for j in range(8)],
        "s": [lambda n=n: student(n) for n in range(8)],
        "S": [student_end],
    }
    for line in ORDER:
        for name in line:
            if name in work:
                work[name].pop(0)()
            else:
                next(chains[name], None)

    partner = {**me, "x": me["x"] + 1 - 2 * grp}
    exchange = []
    for y in range(4):
        branch(y, partner_rows, far)
        exchange.append(copies.start(far.at[y], got.at[y], partner))
    next(chains["I"], None)
    branch(0, own, near)
    branch(1, own, near)
    branch(2, own, near)
    next(chains["I"], None)
    branch(3, own, near)
    images_left = chains.pop("I")
    for turn in range(8):
        for one in chains.values():
            next(one, None)

    s_acc[...] = jnp.zeros_like(s_acc)
    f_tile[...] = jnp.zeros_like(f_tile)

    def head_block(n, carry):
        weights = g_head[n // 4, n % 4].reshape(step, -1)
        cols = pl.ds(pl.multiple_of(n * step, step), step)
        lanes = pl.ds(pl.multiple_of(n % 2 * step, step), step)
        pred = dot(rounded[...], weights, 1, 1)
        added = near[n // 2, :, lanes].astype(f32) + got[n // 2, :, lanes].astype(f32)
        diff = pred - (wide[:, cols].astype(f32) + added)
        f_tile[...] = f_tile[...] + jnp.sum(diff * diff)
        grad_pred = (2.0 * diff / width).astype(bf16)
        d_head[n // 4, n % 4] = (
            dot(grad_pred, rounded[...], 0, 0).astype(bf16).reshape(d_head.shape[2:])
        )
        s_acc[...] = s_acc[...] + dot(grad_pred, weights, 1, 0)
        return carry

    def head_blocks(y):
        exchange[y].wait_recv()
        lax.fori_loop(2 * y, 2 * y + 2, head_block, 0)

    head_blocks(0)
    next(images_left, None)

    n_img = 128
    cols_dev = o_proj.shape[0]
    flat = images.reshape(n_img * 8, 128)
    pooled = [flat[pl.ds(i, n_img, stride=8), :] for i in range(g_proj.shape[-1] * 2 // 128)]
    pooled = jnp.concatenate(pooled, 1).astype(bf16)
    proj_all = g_proj[...].reshape(n_img * 8, g_proj.shape[-1])
    cut = g_proj.shape[-1]
    n_emb = proj_all.shape[0]
    low = dot(pooled[:, :cut], proj_all, 1, 1)
    high = dot(pooled[:, cut:], proj_all, 1, 1)
    real = iota(low.shape, 1) % 8 < cols_dev
    projected = jnp.where(real, low + pltpu.roll(high, n_emb - cols_dev, 1), 0.0)
    proj_norm = jnp.sqrt(jnp.sum(projected * projected, -1, keepdims=True) + 1e-06)
    image_emb = projected / proj_norm
    parts = [captions[:, :, z].reshape(n_img, 128) for z in range(4)]
    squares = sum(jnp.sum(part * part, -1, keepdims=True) for part in parts)
    size = 128 // cols_dev * 8
    row, col = iota((128, size), 0), iota((128, size), 1)
    chosen = jnp.where((row == col // 8 * cols_dev + col % 8) & (col % 8 < cols_dev), 1.0, 0.0)
    caption_all = jnp.concatenate([exact(part, chosen, 1, 0) for part in parts], 1)
    caption_all = caption_all / jnp.sqrt(squares + 1e-06)
    scores = 100.0 * exact(image_emb, caption_all, 1, 1)
    target = jnp.broadcast_to(positive[...].reshape(1, -1), (n_img, n_img))
    match = jnp.where(iota(target.shape, 0) == target, 1.0, 0.0).astype(bf16)
    row = iota(target.shape, 0)
    chosen = jnp.where(iota(target.shape, 1) == row % 64 * 2 + row // 64, 1.0, 0.0).astype(bf16)
    match = dot(chosen, match, 1, 1)

    def soft(axis):
        top = jnp.max(scores, axis, keepdims=True)
        powers = jnp.exp(scores - top)
        total = jnp.sum(powers, axis, keepdims=True)
        return jnp.sum(top + jnp.log(total)), powers / total

    log_rows, soft_rows = soft(1)
    log_cols, soft_cols = soft(0)
    contrast = log_rows + log_cols - 2.0 * jnp.sum(match * scores)
    grad_scores = soft_rows + soft_cols - 2.0 * match
    grad_image = 100.0 * exact(grad_scores, caption_all, 1, 0)
    inner = jnp.sum(image_emb * grad_image, -1, keepdims=True)
    grad_projected = ((grad_image - image_emb * inner) / proj_norm).astype(bf16)
    grad_img[...] = grad_projected.astype(f32)
    row, col = iota((n_emb, 128), 0), iota((n_emb, 128), 1)
    chosen = jnp.where((row == 8 * shard + col) & (col < cols_dev), 1.0, 0.0).astype(bf16)
    columns = dot(grad_projected, chosen, 1, 0).astype(bf16)
    o_proj[...] = dot(columns, pooled, 0, 0)[:cols_dev]
    mine = jnp.broadcast_to(grad_img[pl.ds(shard, 1), :], (8, n_emb))
    grad_low = dot(mine.astype(bf16), proj_all, 1, 0)
    grad_high = dot(pltpu.roll(mine, cols_dev, 1).astype(bf16), proj_all, 1, 0)
    grad_pooled = jnp.concatenate([grad_low, grad_high], 1)[:1]

    for y in range(1, 4):
        head_blocks(y)
    n_store = len(stores) // 2
    head_sums = Scatter(copies, me, sibling, d_head, stores[:3], stores[3:n_store])
    pack_sums = Scatter(copies, me, sibling, d_pack, stores[n_store : n_store + 3], stores[n_store + 3 :])
    head_sums.push()
    f_tile[...] = f_tile[...] / width
    ends = [head_sums.chain(), scalar_chain(copies, me, sibling, f_tile, s_slots)]
    grad_out[...] = (s_acc[...] + grad_pooled / PATCHES).astype(bf16)

    def pack_block(n, carry):
        weights = g_pack[n // 4, n % 4].reshape(-1, g_pack.shape[-1])
        size = weights.shape[0]
        units = pl.ds(pl.multiple_of(n * size, 128), size)
        grad_act = pltpu.roll(dot(weights, grad_out[...], 1, 1), size - hid, 0)
        grad_gate = jax.vjp(gelu_tanh, gates[units, :])[1](grad_act)[0]
        grad_gate = jnp.where(ups(grad_gate.shape), grad_gate, 0.0).astype(bf16)
        total = dot(grad_gate, normed[...], 1, 0) + dot(acts[units, :], grad_out[...], 1, 0)
        d_pack[n // 4, n % 4] = total.astype(bf16).reshape(d_pack.shape[2:])
        return carry

    for part in range(4):
        lax.fori_loop(2 * part, 2 * part + 2, pack_block, 0)
        if part % 2:
            for one in ends:
                next(one, None)
    pack_sums.push()
    ends.append(pack_sums.chain())
    for turn in range(8):
        for one in ends:
            next(one, None)
    for t in range(3):
        cols = pl.ds(t * COLS, COLS)
        o_up[:, cols] = pack_sums.sums[t][:hid]
        o_down[:, cols] = pack_sums.sums[t][hid:]
        o_head[:, cols] = head_sums.sums[t][:feat]
    o_loss[...] = (s_slots[4, 0] + contrast) / (n_img * PATCHES)
    copies.finish()


N_COPIES = 22 * 3 + 19 + 4 * 15 + 4 * 16 + 10 + 4 + 10 + 2 * 42


def run_step(t_up, t_down, up, down, head, proj, table, ids, t_in, t_gain, s_in, s_gain, positive):
    bf16, f32 = t_up.dtype, jnp.float32
    rows, width = t_in.shape[0], up.shape[1]
    own_rows = rows // 2
    hid, feat = up.shape[0], head.shape[0]
    whole = (2, 4, 2, 4, 2)
    tiles = (4, 4, 4, 8, 128)
    teacher = (4, 2, 4, 2, 2 * BLK, t_up.shape[1])
    n_wide = 128 * BLK
    n_pack = 128 * 2 * hid
    vmem = pltpu.VMEM
    scratch = [
        vmem(teacher, bf16),
        vmem(teacher, bf16),
        vmem(whole + (2 * hid, width), bf16),
        vmem(whole + (BLK, width), bf16),
        vmem(whole + (2 * proj.shape[0], width // 2), bf16),
        vmem(tiles, f32),
        vmem(whole + (8, 128), f32),
        vmem((n_pack, own_rows), f32),
        vmem((n_pack, own_rows), bf16),
        vmem((own_rows, width), bf16),
        vmem((own_rows, width), bf16),
        vmem((own_rows, n_wide), bf16),
        vmem((4, own_rows, n_wide // 4), bf16),
        vmem((4, own_rows, n_wide // 4), bf16),
        vmem((4, own_rows, n_wide // 4), bf16),
        vmem((rows, n_wide), bf16),
        vmem((rows, t_up.shape[1]), bf16),
        vmem((own_rows, width), f32),
        vmem((own_rows, width), bf16),
        vmem((128, 128 * 8), f32),
        vmem(whole + (2 * hid, width), bf16),
        vmem(whole + (BLK, width), bf16),
        vmem((8, 128), f32),
        vmem(tiles, f32),
        vmem(tiles, f32),
        vmem((5, 4, 4, 8, 128), f32),
        vmem((5, 4, 8, 128), f32),
        vmem((4, 8, 128), f32),
        vmem((5, 4, 8, 128), f32),
        pltpu.SemaphoreType.DMA((N_COPIES,)),
        pltpu.SemaphoreType.DMA((N_COPIES,)),
    ]
    for block in (BLK, 2 * hid):
        scratch += [vmem((2, 4, 2, 4, block, COLS), bf16) for _ in range(3)]
        for order in ORDERS:
            scratch.append(vmem((2,) + half_shape(order, 0, block), bf16))
            for phase, count in enumerate((2, 3, 3)):
                rest = dims_of(rest_of(order, phase)) + (block, COLS)
                scratch.append(vmem((count,) + rest, bf16))
    shapes = [(hid, width), (hid, width), (feat, width), (proj.shape[0], width), (8, 128)]
    shapes = [jax.ShapeDtypeStruct(shape, f32) for shape in shapes]
    out = pl.pallas_call(
        step_kernel,
        out_shape=shapes,
        in_specs=[VM] * 13,
        out_specs=[VM] * 5,
        scratch_shapes=scratch,
        compiler_params=pltpu.CompilerParams(
            collective_id=1, has_side_effects=True, vmem_limit_bytes=67043328
        ),
        name="step",
    )(t_up, t_down, up, down, head, proj, table, ids, t_in, t_gain, s_in, s_gain, positive)
    return pl.pallas_call(
        write_kernel,
        out_shape=shapes[:4] + [jax.ShapeDtypeStruct((1, 1), f32)],
        in_specs=[VM] * 5,
        out_specs=[VM] * 4 + [pl.BlockSpec(memory_space=pltpu.SMEM)],
        name="write",
    )(*out)


def write_kernel(*refs):
    for source, out in zip(refs[:4], refs[5:9]):
        out[...] = source[...]
    refs[9][0, 0] = jnp.max(refs[4][...])


def local(
    teacher_in,
    teacher_gain,
    teacher_up,
    teacher_down,
    student_in,
    student_gain,
    student_up,
    student_down,
    student_head,
    student_proj,
    word_table,
    caption_ids,
    positive,
):
    grad_up, grad_down, grad_head, grad_proj, loss = run_step(
        teacher_up,
        teacher_down,
        student_up.T,
        student_down,
        student_head.T,
        student_proj.T,
        word_table,
        caption_ids.T,
        teacher_in,
        teacher_gain,
        student_in,
        student_gain,
        positive,
    )
    return (loss[0, 0], grad_up.T, grad_down, grad_head.T, grad_proj.T)


def solution(mesh):
    placed = (
        P("dp", None),
        P(),
        P("dp", "grp"),
        P("dp", "grp"),
        P("dp", None),
        P(),
        P(None, ("grp", "dp")),
        P(("grp", "dp"), None),
        P(None, ("grp", "dp")),
        P(None, ("grp", "dp")),
        P(("grp", "dp"), None),
        P(),
        P(),
    )
    return jax.shard_map(
        local,
        mesh=mesh,
        in_specs=placed,
        out_specs=(
            P(),
            P(None, ("grp", "dp")),
            P(("grp", "dp"), None),
            P(None, ("grp", "dp")),
            P(None, ("grp", "dp")),
        ),
        check_vma=False,
    )
```
